128 devices in a mesh: gx: 16 (over x, z), gy: 8 (over y, core).
Axes of the slice: x: 4, y: 4, z: 4, core: 2. Of those that a mesh axis runs over, the one named last changes fastest.
Arguments:
- base_state: float32 [4, 8, 1024, 1024], P(None, None, 'gx', 'gy'), may hold values from -6 to 6
- base_old: float32 [4, 8, 1024, 1024], P(None, None, 'gx', 'gy'), may hold values from -6 to 6
- fine_state: float32 [4, 8, 16, 264, 264], P(None, None, 'gx', 'gy'), may hold values from -6 to 6
- fine_old: float32 [4, 8, 16, 264, 264], P(None, None, 'gx', 'gy'), may hold values from -6 to 6
- coupling: float32 [4, 4], replicated, may hold values from -12 to 12
- patch_offsets: int32 [16, 2], replicated, may hold values from 1 to 935, as said below
- patch_group: int32 [16], replicated, may hold values from 0 to 15, each once
Outputs:
- base_residual: float32 [4, 8, 1024, 1024], P(None, None, 'gx', 'gy')
- fine_residual: float32 [4, 8, 16, 264, 264], P(None, None, 'gx', 'gy')
- residual_norm: float32 [], replicated
The draws below stay inside these ranges and needn't reach their ends.
Inputs may be any that keep to these rules, and one draw needn't show every extreme that they name: `patch_offsets`: with the cycle of one base cell around it, each patch lies inside the grid, and no two patches or cycles share a cell. `patch_group`: every group owns exactly one patch.
All inputs are finite; a program needn't handle non-finite values.
Results may differ from the reference program's by a relative error of at most 0.0003.
Values sent between devices are 32-bit elements; how exact they have to be, the bound alone decides.
A program may use at most 128 MiB of HBM per device.

```python
import jax
import jax.numpy as jnp
from jax import lax

FIELDS = 4
NZ = 8
PC = 88
RATIO = 3
NX = 1024
NY = 1024
PATCHES = 16
FP = 264


def draw_patch_offsets(key, part):
    across = PATCHES // 4
    tile_x = NX // across
    tile_y = NY // 4
    index = jnp.arange(PATCHES, dtype=jnp.int32)
    shift_x = jax.random.randint(jax.random.fold_in(key, 11), (PATCHES,), 0, tile_x - PC - 1)
    shift_y = jax.random.randint(jax.random.fold_in(key, 23), (PATCHES,), 0, tile_y - PC - 1)
    start_x = index % across * tile_x + 1 + shift_x
    start_y = index // across * tile_y + 1 + shift_y
    order = jax.random.permutation(jax.random.fold_in(key, 37), PATCHES)
    return jnp.stack([start_x, start_y], axis=1)[order].astype(jnp.int32)


def block_scale(stream_key, shape, pieces, smallest, largest):
    factor_of = 1.0
    for dim, shards_of in pieces:
        draws = jax.random.uniform(jax.random.fold_in(jax.random.fold_in(stream_key, 6), dim), (shards_of,), jnp.float32, smallest / len(pieces), largest / len(pieces))
        factor_of = factor_of * jnp.repeat(jnp.exp(draws), shape[dim] // shards_of).reshape((-1,) + (1,) * (len(shape) - 1 - dim))
    return factor_of


def gaussian(key, shape, scale, limit, shards=(), kind=jnp.bfloat16):
    drawn = jax.random.normal(key, shape, jnp.float32) * scale
    if len(shards) > 0:
        drawn = block_scale(key, shape, shards, -0.22, 0.18) * drawn
    return jnp.clip(drawn, min=-limit, max=limit).astype(kind)


def setup_inputs(seed: int = 0) -> dict:
    key_list = jax.random.split(jax.random.key(seed), 8)
    return {
        "base_state": gaussian(key_list[0], (FIELDS, NZ, NX, NY), 1.0, 6.0, ((2, 16), (3, 8)), jnp.float32),
        "base_old": gaussian(key_list[1], (FIELDS, NZ, NX, NY), 1.0, 6.0, ((2, 16), (3, 8)), jnp.float32),
        "fine_state": gaussian(key_list[2], (FIELDS, NZ, PATCHES, FP, FP), 1.0, 6.0, ((2, 16), (3, 8)), jnp.float32),
        "fine_old": gaussian(key_list[3], (FIELDS, NZ, PATCHES, FP, FP), 1.0, 6.0, ((2, 16), (3, 8)), jnp.float32),
        "coupling": gaussian(key_list[4], (FIELDS, FIELDS), 2.0, 12.0, (), jnp.float32),
        "patch_offsets": draw_patch_offsets(jax.random.fold_in(key_list[7], 71), 0),
        "patch_group": jax.random.permutation(key_list[6], PATCHES).astype(jnp.int32),
    }


time_step = 0.1
viscosity = 0.2
vertical_mix = 0.5

def tendency(padded, state, former, coupling, inverse):
    north = padded[:, :, 2:, 1:-1]
    south = padded[:, :, :-2, 1:-1]
    east = padded[:, :, 1:-1, 2:]
    west = padded[:, :, 1:-1, :-2]
    advect = (state[0:1] * (north - south) + state[1:2] * (east - west)) * (0.5 * inverse)
    laplace = (north + south + east + west - 4.0 * state) * (inverse * inverse)
    zero_level = jnp.zeros_like(state[:, :1])
    upper = jnp.concatenate([state[:, 1:], zero_level], axis=1)
    lower = jnp.concatenate([zero_level, state[:, :-1]], axis=1)
    vertical = 2.0 * state - upper - lower
    coupled = coupling[:, 0, None, None, None] * state[0:1]
    for source in range(1, state.shape[0]):
        coupled = coupled + coupling[:, source, None, None, None] * state[source:source + 1]
    return state - former + time_step * (advect - viscosity * laplace + vertical_mix * vertical + coupled)

def reference(base_state, base_old, fine_state, fine_old, coupling, patch_offsets, patch_group):
    fields = base_state.shape[0]
    levels = base_state.shape[1]
    padded = jnp.pad(base_state, ((0, 0), (0, 0), (1, 1), (1, 1)))
    base_tend = tendency(padded, base_state, base_old, coupling, 1.0)
    owner = (patch_group[None, :] == jnp.arange(PATCHES, dtype=jnp.int32)[:, None]).astype(jnp.int32)
    placed = lax.optimization_barrier(jnp.sum(owner[:, :, None] * patch_offsets[None, :, :], axis=1)).astype(jnp.int32)
    zero = jnp.zeros((), jnp.int32)

    def one_patch(group):
        start_x = placed[group, 0]
        start_y = placed[group, 1]
        top = lax.dynamic_slice(base_state, (zero, zero, start_x - 1, start_y), (fields, levels, 1, PC))
        bottom = lax.dynamic_slice(base_state, (zero, zero, start_x + PC, start_y), (fields, levels, 1, PC))
        left = lax.dynamic_slice(base_state, (zero, zero, start_x, start_y - 1), (fields, levels, PC, 1))
        right = lax.dynamic_slice(base_state, (zero, zero, start_x, start_y + PC), (fields, levels, PC, 1))
        top = jnp.repeat(top, RATIO, axis=3)
        bottom = jnp.repeat(bottom, RATIO, axis=3)
        left = jnp.repeat(left, RATIO, axis=2)
        right = jnp.repeat(right, RATIO, axis=2)
        state = lax.dynamic_index_in_dim(fine_state, group, 2, keepdims=False)
        former = lax.dynamic_index_in_dim(fine_old, group, 2, keepdims=False)
        corner = jnp.zeros((fields, levels, 1, 1), jnp.float32)
        top_row = jnp.concatenate([corner, top, corner], axis=3)
        bottom_row = jnp.concatenate([corner, bottom, corner], axis=3)
        middle = jnp.concatenate([left, state, right], axis=3)
        padded_fine = jnp.concatenate([top_row, middle, bottom_row], axis=2)
        result = tendency(padded_fine, state, former, coupling, float(RATIO))
        coarse = result.reshape(fields, levels, PC, RATIO, PC, RATIO).mean(axis=(3, 5))
        return (result, coarse)
    fine_res, restricted = lax.map(one_patch, jnp.arange(PATCHES, dtype=jnp.int32))
    fine_res = jnp.moveaxis(fine_res, 0, 2)

    def place(group, carry):
        merged, covered = carry
        start = (zero, zero, placed[group, 0], placed[group, 1])
        merged = lax.dynamic_update_slice(merged, restricted[group], start)
        covered = lax.dynamic_update_slice(covered, jnp.ones((1, 1, PC, PC), jnp.float32), start)
        return (merged, covered)
    covered_init = jnp.zeros((1, 1, base_state.shape[2], base_state.shape[3]), jnp.float32)
    merged, covered = lax.fori_loop(0, PATCHES, place, (base_tend, covered_init))
    base_sq = jnp.sum(jnp.where(covered > 0.5, 0.0, base_tend * base_tend))
    fine_sq = jnp.sum(fine_res * fine_res) / (RATIO * RATIO)
    residual_norm = jnp.sqrt(base_sq + fine_sq)
    return (merged, fine_res, residual_norm)
```

```python
import functools

import jax
import jax.numpy as jnp
from jax import lax
from jax.experimental import pallas as pl
from jax.experimental.pallas import tpu as pltpu
from jax.sharding import PartitionSpec as P

PC = 88
NG, NM = 16, 8
BX, BY = 64, 128
FR, FC = 33, 264
MESH = pl.DeviceIdType.MESH
VM = pltpu.VMEM
F32 = jnp.float32
HI = lax.Precision.HIGHEST


def vspec():
    return pl.BlockSpec(memory_space=pltpu.VMEM)


def sspec():
    return pl.BlockSpec(memory_space=pltpu.SMEM)


def shape(*dims):
    return jax.ShapeDtypeStruct(dims, F32)


def iota(dims, axis):
    return lax.broadcasted_iota(jnp.int32, dims, axis)


def extract_kernel(off, pg, base, fine, pxy, s1, hr, hc, fh, trans):
    r = lax.axis_index("gx")
    c = lax.axis_index("gy")
    for p in range(NG):
        g = pg[p]
        pxy[0, g] = off[p, 0]
        pxy[1, g] = off[p, 1]
    for q in range(16):
        trans[pl.ds(q, 128, stride=16), :] = base[pl.ds(128 * q, 128), :].T
    hr[0] = base[pl.ds(0, 32, stride=BX), :]
    hr[1] = base[pl.ds(BX - 1, 32, stride=BX), :]
    hc[0] = trans[pl.ds(0, 16), :]
    hc[1] = trans[pl.ds(127 * 16, 16), :]
    zero = jnp.zeros((32, 384 - FC), F32)
    fh[0] = jnp.concatenate([fine[:, 0, :], zero], axis=1)
    fh[1] = jnp.concatenate([fine[:, FR - 1, :], zero], axis=1)

    def body(g, _):
        x = pxy[0, g]
        y = pxy[1, g]
        lo = x - 1 - r * BX
        hi = x + PC - r * BX
        loc = jnp.where((lo >= 0) & (lo < BX), lo, jnp.clip(hi, 0, BX - 1))
        s1[g, 0:32, :] = base[pl.ds(loc, 32, stride=BX), :]
        y0 = jnp.clip(y - 1 - c * BY, 0, BY - 1)
        s1[g, 32:48, :] = trans[pl.ds(pl.multiple_of(y0 * 16, 16), 16), :]
        y1 = jnp.clip(y + PC - c * BY, 0, BY - 1)
        s1[g, 48:64, :] = trans[pl.ds(pl.multiple_of(y1 * 16, 16), 16), :]
        return 0

    lax.fori_loop(0, NG, body, 0)


def extract(off, pg, base, fine):
    return pl.pallas_call(
        extract_kernel,
        out_shape=(
            jax.ShapeDtypeStruct((2, NG), jnp.int32),
            shape(NG, 64, 128),
            shape(2, 32, 128),
            shape(2, 16, 128),
            shape(2, 32, 384),
        ),
        in_specs=[sspec(), sspec(), vspec(), vspec()],
        out_specs=(sspec(), vspec(), vspec(), vspec(), vspec()),
        scratch_shapes=[VM((2048, 128), F32)],
    )(off, pg, base, fine)


def wrap(v, n):
    return jnp.where(v >= n, v - n, v)


def here():
    return lax.axis_index("gx"), lax.axis_index("gy")


def gx_peers(gx):
    x = gx // 4
    z = gx - 4 * x
    out = []
    for dx, dz in ((2, 2), (1, 2), (2, 1), (3, 2), (2, 3), (1, 1), (3, 3), (1, 3), (3, 1), (2, 0), (0, 2), (1, 0), (0, 1), (3, 0), (0, 3)):
        out.append(wrap(x + dx, 4) * 4 + wrap(z + dz, 4))
    return out


def gy_peers(gy):
    return [wrap(gy + d, NM) for d in range(1, NM)]


def remote(src, dst, send, recv, a, b):
    return pltpu.make_async_remote_copy(
        src_ref=src, dst_ref=dst, send_sem=send, recv_sem=recv, device_id=(a, b), device_id_type=MESH
    )


def wait_bytes(ref, sem):
    pltpu.make_async_copy(ref, ref, sem).wait()


def cycle_kernel(pxy, s1, hr, hc, fh, gr, tr, br, hrn, hcn, fhn, r1, gs, tb, sa, sb, sc, lsem):
    gx, gy = here()
    bar = pltpu.get_barrier_semaphore()
    ga = gx_peers(gx)
    gb = gy_peers(gy)
    for a in ga:
        pl.semaphore_signal(bar, inc=1, device_id=(a, gy), device_id_type=MESH)
    for b in gb:
        pl.semaphore_signal(bar, inc=1, device_id=(gx, b), device_id_type=MESH)
    own = pltpu.make_async_copy(s1.at[gx], r1.at[gx], lsem.at[0])
    own.start()
    pl.semaphore_wait(bar, len(ga) + len(gb))
    for a in ga:
        remote(s1.at[a], r1.at[gx], sa.at[0], sa.at[1], a, gy).start()
    up, down = wrap(gx + 1, NG), wrap(gx + NG - 1, NG)
    right, left = wrap(gy + 1, NM), wrap(gy + NM - 1, NM)
    halos = [
        remote(hr.at[1], hrn.at[0], sb.at[0], sb.at[1], up, gy),
        remote(hr.at[0], hrn.at[1], sb.at[2], sb.at[3], down, gy),
        remote(hc.at[1], hcn.at[0], sb.at[4], sb.at[5], gx, right),
        remote(hc.at[0], hcn.at[1], sb.at[6], sb.at[7], gx, left),
        remote(fh.at[1], fhn.at[0], sb.at[8], sb.at[9], gx, right),
        remote(fh.at[0], fhn.at[1], sb.at[10], sb.at[11], gx, left),
    ]
    for h in halos:
        h.start()
    own.wait()
    wait_bytes(r1.at[pl.ds(0, NG - 1)], sa.at[1])
    x = pxy[0, gx]
    tb[0] = r1[jnp.maximum(x - 1, 0) // BX, 0:32, :]
    tb[1] = r1[(x + PC) // BX, 0:32, :]
    for j in range(NM):
        a = (x + 11 * j) // BX
        b = jnp.minimum(a + 1, NG - 1)
        gs[j, 0:32, :] = r1[a, 32:64, :]
        gs[j, 32:64, :] = r1[b, 32:64, :]
    for b in gb:
        remote(gs.at[b], gr.at[gy], sc.at[0], sc.at[1], gx, b).start()
    mine = pltpu.make_async_copy(gs.at[gy], gr.at[gy], lsem.at[1])
    mine.start()
    for k, (ref, target) in enumerate(((tr, 0), (br, NM - 1))):
        far = remote(tb.at[k], ref.at[gy], sc.at[2 + 2 * k], sc.at[3 + 2 * k], gx, target)
        near = pltpu.make_async_copy(tb.at[k], ref.at[gy], lsem.at[2])

        @pl.when(gy != target)
        def _():
            far.start()
            far.wait_send()

        @pl.when(gy == target)
        def _():
            near.start()
            near.wait()
            wait_bytes(ref.at[pl.ds(0, NM - 1)], sc.at[3 + 2 * k])

    mine.wait()
    for h in halos:
        h.wait()
    wait_bytes(gr.at[pl.ds(0, NM - 1)], sc.at[1])
    wait_bytes(gr.at[pl.ds(0, NM - 1)], sc.at[0])
    wait_bytes(r1.at[pl.ds(0, NG - 1)], sa.at[0])


def cycle(pxy, s1, hr, hc, fh):
    return pl.pallas_call(
        cycle_kernel,
        out_shape=(
            shape(NM, 64, 128),
            shape(NM, 32, 128),
            shape(NM, 32, 128),
            shape(2, 32, 128),
            shape(2, 16, 128),
            shape(2, 32, 384),
        ),
        in_specs=[sspec()] + [vspec()] * 4,
        out_specs=(vspec(),) * 6,
        scratch_shapes=[
            VM((NG, 64, 128), F32),
            VM((NM, 64, 128), F32),
            VM((2, 32, 128), F32),
            pltpu.SemaphoreType.DMA((2,)),
            pltpu.SemaphoreType.DMA((12,)),
            pltpu.SemaphoreType.DMA((6,)),
            pltpu.SemaphoreType.DMA((3,)),
        ],
        compiler_params=pltpu.CompilerParams(collective_id=0, has_side_effects=True),
    )(pxy, s1, hr, hc, fh)


def stencil(q, north, south, east, west, above, below, old, cpl, a0m, a0p, a1m, a1p, own, f):
    total = own * q[f] - old
    total += north * a0m - south * a0p
    total += east * a1m - west * a1p
    total -= 0.05 * (above + below)
    for g in range(4):
        total += cpl[f][g] * q[g]
    return total


def couplings(cp):
    return [[0.1 * cp[f, g] for g in range(4)] for f in range(4)]


def base_kernel(pxy, cp, base, old, hrn, hcn, tend, psum, hz):
    r = lax.axis_index("gx")
    c = lax.axis_index("gy")
    cpl = couplings(cp)
    keep = [
        jnp.where(r > 0, 1.0, 0.0),
        jnp.where(r < NG - 1, 1.0, 0.0),
        jnp.where(c > 0, 1.0, 0.0),
        jnp.where(c < NM - 1, 1.0, 0.0),
    ]
    hz[0] = hrn[0] * keep[0]
    hz[1] = hrn[1] * keep[1]
    zeros = jnp.zeros((112, 128), F32)
    westc = jnp.concatenate([hcn[0] * keep[2], zeros], axis=0).T
    eastc = jnp.concatenate([hcn[1] * keep[3], zeros], axis=0).T
    row = iota((BX, BY), 0)
    lane = iota((BX, BY), 1)
    open_ = jnp.ones((BX, BY), F32)
    for g in range(NG):
        x = pxy[0, g] - r * BX
        y = pxy[1, g] - c * BY
        inside = (row >= x) & (row < x + PC) & (lane >= y) & (lane < y + PC)
        open_ = jnp.where(inside, 0.0, open_)
    k = 0.02
    own = 1.0 + 4 * k + 0.1
    acc = jnp.zeros((BX, BY), F32)
    for l in range(8):
        q = [base[f * 8 + l] for f in range(4)]
        a0 = 0.05 * q[0]
        a1 = 0.05 * q[1]
        for f in range(4):
            p = f * 8 + l
            pair, par = p // 2, p % 2
            north = jnp.where(row == BX - 1, hz[1, p : p + 1, :], pltpu.roll(q[f], BX - 1, 0))
            south = jnp.where(row == 0, hz[0, p : p + 1, :], pltpu.roll(q[f], 1, 0))
            ecol = pltpu.roll(eastc[par * 64 : par * 64 + 64], 127 - pair, 1)
            wcol = pltpu.roll(westc[par * 64 : par * 64 + 64], (128 - pair) % 128, 1)
            east = jnp.where(lane == BY - 1, ecol, pltpu.roll(q[f], BY - 1, 1))
            west = jnp.where(lane == 0, wcol, pltpu.roll(q[f], 1, 1))
            above = base[p + 1] if l < 7 else jnp.zeros((BX, BY), F32)
            below = base[p - 1] if l > 0 else jnp.zeros((BX, BY), F32)
            total = stencil(
                q, north, south, east, west, above, below, old[p], cpl, a0 - k, a0 + k, a1 - k, a1 + k, own, f
            )
            tend[p] = total
            acc = acc + open_ * (total * total)
    psum[...] = acc.reshape(8, 8, 128).sum(axis=0)


def base_tendency(pxy, cp, base, old, hrn, hcn):
    return pl.pallas_call(
        base_kernel,
        out_shape=(shape(32, BX, BY), shape(8, 128)),
        in_specs=[sspec(), sspec()] + [vspec()] * 4,
        out_specs=(vspec(), vspec()),
        scratch_shapes=[VM((2, 32, 128), F32)],
    )(pxy, cp, base, old, hrn, hcn)


def fine_kernel(pxy, cp, fine, old, fhn, gr, tr, br, bsum, out, ro, pad, hrow, res, mm):
    g = lax.axis_index("gx")
    j = lax.axis_index("gy")
    x = pxy[0, g]
    y = pxy[1, g]
    cpl = couplings(cp)
    first = lax.rem(x + 11 * j, BX)
    cl = (y - 1) // BY
    cr = (y + PC) // BY
    blank = jnp.zeros((96, 128), F32)
    va = jnp.concatenate([gr[cl, 0:16, :], gr[cr, 16:32, :], blank], axis=0)
    vb = jnp.concatenate([gr[cl, 32:48, :], gr[cr, 48:64, :], blank], axis=0)
    want = first + iota((40, 128), 0) // 3
    lane40 = iota((40, 128), 1)
    cols = []
    for par in range(2):
        at = lane40 - 64 * par
        good = (at >= 0) & (at < 64)
        pa = jnp.where(good & (at == want), 1.0, 0.0)
        pb = jnp.where(good & (at + 64 == want), 1.0, 0.0)
        dims = (((1,), (1,)), ((), ()))
        cols.append(
            lax.dot_general(pa, va, dims, precision=HI, preferred_element_type=F32)
            + lax.dot_general(pb, vb, dims, precision=HI, preferred_element_type=F32)
        )
    hrow[0] = fhn[0]
    hrow[1] = fhn[1]

    def spread(cells):
        c0 = y // BY
        c1 = jnp.minimum(c0 + 1, NM - 1)
        b = iota((128, 384), 0)
        jf = iota((128, 384), 1)
        cell = y + jf // 3 - c0 * BY
        good = jf < FC
        p0 = jnp.where(good & (b == cell), 1.0, 0.0)
        p1 = jnp.where(good & (b + BY == cell), 1.0, 0.0)
        return jnp.dot(cells[c0], p0, precision=HI, preferred_element_type=F32) + jnp.dot(
            cells[c1], p1, precision=HI, preferred_element_type=F32
        )

    @pl.when(j == 0)
    def _():
        hrow[0] = spread(tr)

    @pl.when(j == NM - 1)
    def _():
        hrow[1] = spread(br)

    lane33 = iota((FR, 128), 1)
    for f in range(4):
        pad[f * 10] = jnp.zeros((56, 384), F32)
        pad[f * 10 + 9] = jnp.zeros((56, 384), F32)

    def fill(pair, _):
        for par in range(2):
            p = 2 * pair + par
            dst = p + 2 * (p // 8) + 1
            pad[dst, 8 : 8 + FR, 0:256] = fine[p, :, 0:256]
            t = jnp.concatenate([fine[p, :, 256:FC], jnp.zeros((FR, 120), F32)], axis=1)
            cv = cols[par][:FR]
            t = jnp.where(lane33 == 127, pltpu.roll(cv, 127 - pair, 1), t)
            t = jnp.where(lane33 == 8, pltpu.roll(cv, 120 - pair, 1), t)
            pad[dst, 8 : 8 + FR, 256:384] = t
            pad[dst, 7:8, :] = hrow[0, pl.ds(p, 1), :]
            pad[dst, 8 + FR : 9 + FR, :] = hrow[1, pl.ds(p, 1), :]
        return 0

    lax.fori_loop(0, 16, fill, 0)
    k = 0.02 * 9
    own = 1.0 + 4 * k + 0.1

    def level(l, acc):
        for start, n in ((0, 8), (8, 8), (16, 8), (24, 8), (32, 1)):
            s = 8 + start
            q = [pad[f * 10 + 1 + l, s : s + n, :] for f in range(4)]
            a0 = 0.15 * q[0]
            a1 = 0.15 * q[1]
            keep = iota((n, 384), 1) < FC
            for f in range(4):
                z = f * 10 + 1 + l
                north = pad[z, s + 1 : s + 1 + n, :]
                south = pad[z, s - 1 : s - 1 + n, :]
                east = pltpu.roll(q[f], 383, 1)
                west = pltpu.roll(q[f], 1, 1)
                p = f * 8 + l
                before = old[p, start : start + n, :]
                before = jnp.concatenate([before, jnp.zeros((n, 384 - FC), F32)], axis=1)
                total = stencil(
                    q, north, south, east, west, pad[z + 1, s : s + n, :], pad[z - 1, s : s + n, :],
                    before, cpl, a0 - k, a0 + k, a1 - k, a1 + k, own, f,
                )
                out[p, start : start + n, :] = total[:, :FC]
                total = jnp.where(keep, total, 0.0)
                for t in range(3):
                    part = total[:, 128 * t : 128 * t + 128]
                    res[f, t, start : start + n, :] = part
                    sq = part * part
                    if n == 1:
                        sq = jnp.where(iota((8, 128), 0) == 0, jnp.broadcast_to(sq, (8, 128)), 0.0)
                    acc = acc + sq
        for f in range(4):
            for t in range(3):
                rows = [res[f, t, pl.ds(d, 11, stride=3), :] for d in range(3)]
                mm[t, f * 8 + l, 0:11, :] = rows[0] + rows[1] + rows[2]
        return acc

    for t in range(3):
        mm[t, :, 8:16, :] = jnp.zeros((32, 8, 128), F32)
    acc = lax.fori_loop(0, 8, level, jnp.zeros((8, 128), F32))
    total = 0.0
    for t in range(3):
        comb = jnp.where((iota((128, 128), 0) + 128 * t) // 3 == iota((128, 128), 1), 1.0, 0.0)
        total = total + jnp.dot(mm[t].reshape(512, 128), comb, precision=HI, preferred_element_type=F32)
    total = (total * (1.0 / 9.0)).reshape(32, 16, 128)
    norm = bsum[...] + acc * (1.0 / 9.0)
    norm = jnp.sum(norm, axis=0, keepdims=True)
    for i in range(16):
        ro[i, 0:11, :] = total[2 * i, 0:11, :]
        ro[i, 11:22, :] = total[2 * i + 1, 0:11, :]
        ro[i, 22:23, :] = norm
        ro[i, 23:24, :] = norm


def fine_residual(pxy, cp, fine, old, fhn, gr, tr, br, bsum):
    return pl.pallas_call(
        fine_kernel,
        out_shape=(shape(32, FR, FC), shape(NG, 24, 128)),
        in_specs=[sspec(), sspec()] + [vspec()] * 7,
        out_specs=(vspec(), vspec()),
        scratch_shapes=[
            VM((40, 56, 384), F32),
            VM((2, 32, 384), F32),
            VM((4, 3, 40, 128), F32),
            VM((3, 32, 16, 128), F32),
        ],
    )(pxy, cp, fine, old, fhn, gr, tr, br, bsum)


def spray_kernel(ro, ri, send, recv, lsem):
    gx, gy = here()
    bar = pltpu.get_barrier_semaphore()
    ga = gx_peers(gx)
    for a in ga:
        pl.semaphore_signal(bar, inc=1, device_id=(a, gy), device_id_type=MESH)
    own = pltpu.make_async_copy(ro.at[gx], ri.at[gx], lsem)
    own.start()
    pl.semaphore_wait(bar, len(ga))
    for a in ga:
        remote(ro.at[a], ri.at[gx], send, recv, a, gy).start()
    own.wait()
    wait_bytes(ri.at[pl.ds(0, NG - 1)], send)
    wait_bytes(ri.at[pl.ds(0, NG - 1)], recv)


def spray(ro):
    return pl.pallas_call(
        spray_kernel,
        out_shape=shape(NG, 24, 128),
        in_specs=[vspec()],
        out_specs=vspec(),
        scratch_shapes=[pltpu.SemaphoreType.DMA] * 3,
        compiler_params=pltpu.CompilerParams(collective_id=1, has_side_effects=True),
    )(ro)


def place_kernel(pxy, ri, so):
    j = lax.axis_index("gy")
    norm = ri[0, 22:23, :]
    for g in range(1, NG):
        norm = norm + ri[g, 22:23, :]
    fill = jnp.broadcast_to(norm, (24, 128))

    def clear(d, _):
        so[d] = fill
        return 0

    lax.fori_loop(0, NG * NM, clear, 0, unroll=8)
    lane = iota((24, 128), 1)
    body = iota((24, 128), 0) < 22

    def patch(g, _):
        x = pxy[0, g] + 11 * j
        y = pxy[1, g]
        ra = x // BX
        rb = (x + 10) // BX
        c0 = y // BY
        shift = y - c0 * BY
        c1 = jnp.minimum(c0 + 1, NM - 1)
        v = pltpu.roll(ri[g], shift, 1)
        m0 = body & (lane >= shift) & (lane < shift + PC)
        m1 = body & (lane < shift + PC - BY)
        for r in (ra, rb):
            for c, m in ((c0, m0), (c1, m1)):
                so[r * NM + c] = jnp.where(m, v, so[r * NM + c])
        return 0

    lax.fori_loop(0, NG, patch, 0)


def place(pxy, ri):
    return pl.pallas_call(
        place_kernel,
        out_shape=shape(NG * NM, 24, 128),
        in_specs=[sspec(), vspec()],
        out_specs=vspec(),
    )(pxy, ri)


def all_peers(gx, gy):
    x = gx // 4
    z = gx - 4 * x
    y = gy // 2
    c = gy - 2 * y
    offs = [(a, b, d, e) for a in range(4) for b in range(4) for d in range(4) for e in range(2)][1:]
    offs.sort(key=lambda o: -sum(min(v, 4 - v) for v in o[:3]))
    xs = [wrap(x + d, 4) for d in range(4)]
    ys = [wrap(y + d, 4) for d in range(4)]
    zs = [wrap(z + d, 4) for d in range(4)]
    cs = [c, 1 - c]
    return [(xs[a] * 4 + zs[d], ys[b] * 2 + cs[e]) for a, b, d, e in offs]


def scatter_kernel(so, ri, send, recv, lsem):
    gx, gy = here()
    me = gx * NM + gy
    bar = pltpu.get_barrier_semaphore()
    peers = all_peers(gx, gy)
    for a, b in peers:
        pl.semaphore_signal(bar, inc=1, device_id=(a, b), device_id_type=MESH)
    own = pltpu.make_async_copy(so.at[me], ri.at[me], lsem)
    own.start()
    pl.semaphore_wait(bar, len(peers))
    for a, b in peers:
        remote(so.at[a * NM + b], ri.at[me], send, recv, a, b).start()
    own.wait()
    wait_bytes(ri.at[pl.ds(0, NG * NM - 1)], send)
    wait_bytes(ri.at[pl.ds(0, NG * NM - 1)], recv)


def scatter(so):
    return pl.pallas_call(
        scatter_kernel,
        out_shape=shape(NG * NM, 24, 128),
        in_specs=[pl.BlockSpec(memory_space=pl.ANY)],
        out_specs=pl.BlockSpec(memory_space=pl.ANY),
        scratch_shapes=[pltpu.SemaphoreType.DMA] * 3,
        compiler_params=pltpu.CompilerParams(collective_id=2, has_side_effects=True),
    )(so)


def merge_kernel(pxy, tend, ri, out, norm, cells):
    r = lax.axis_index("gx")
    c = lax.axis_index("gy")
    for i in range(16):
        for j in range(NM):
            for par in range(2):
                at = 64 + 11 * j
                cells[2 * i + par, at : at + 11, :] = ri[i * NM + j, 11 * par : 11 * par + 11, :]
    out[...] = tend[...]
    row = iota((BX, BY), 0)
    lane = iota((BX, BY), 1)

    def patch(g, _):
        x = pxy[0, g] - r * BX
        y = pxy[1, g] - c * BY

        @pl.when((x < BX) & (x + PC > 0) & (y < BY) & (y + PC > 0))
        def _():
            inside = (row >= x) & (row < x + PC) & (lane >= y) & (lane < y + PC)
            start = 64 - x

            def plane(p, _):
                out[p] = jnp.where(inside, cells[p, pl.ds(start, BX), :], out[p])
                return 0

            lax.fori_loop(0, 32, plane, 0)

        return 0

    lax.fori_loop(0, NG, patch, 0)
    total = ri[0, 22:23, :]
    for j in range(1, NM):
        total = total + ri[j, 22:23, :]
    norm[...] = jnp.sqrt(jnp.sum(total, axis=1, keepdims=True))


def merge(pxy, tend, ri):
    return pl.pallas_call(
        merge_kernel,
        out_shape=(shape(32, BX, BY), shape(1, 1)),
        in_specs=[sspec(), vspec(), vspec()],
        out_specs=(vspec(), vspec()),
        scratch_shapes=[VM((32, 216, 128), F32)],
    )(pxy, tend, ri)


def local(base_state, base_old, fine_state, fine_old, coupling, patch_offsets, patch_group):
    base = base_state.reshape(32, BX, BY)
    old = base_old.reshape(32, BX, BY)
    fine = fine_state.reshape(32, FR, FC)
    fold = fine_old.reshape(32, FR, FC)
    pxy, s1, hr, hc, fh = extract(patch_offsets, patch_group, base.reshape(2048, 128), fine)
    gr, tr, br, hrn, hcn, fhn = cycle(pxy, s1, hr, hc, fh)
    tend, bsum = base_tendency(pxy, coupling, base, old, hrn, hcn)
    fres, ro = fine_residual(pxy, coupling, fine, fold, fhn, gr, tr, br, bsum)
    ri = spray(ro)
    so = place(pxy, ri)
    r2 = scatter(so)
    bout, norm = merge(pxy, tend, r2)
    return (
        bout.reshape(4, 8, BX, BY),
        fres.reshape(4, 8, 1, FR, FC),
        norm.reshape(()),
    )


def solution(mesh):
    placed = (
        P(None, None, "gx", "gy"),
        P(None, None, "gx", "gy"),
        P(None, None, "gx", "gy", None),
        P(None, None, "gx", "gy", None),
        P(),
        P(),
        P(),
    )
    return jax.shard_map(
        local,
        mesh=mesh,
        in_specs=placed,
        out_specs=(P(None, None, "gx", "gy"), P(None, None, "gx", "gy", None), P()),
        check_vma=False,
    )
```

```python
import functools

import jax
import jax.numpy as jnp
from jax import lax
from jax.experimental import pallas as pl
from jax.experimental.pallas import tpu as pltpu
from jax.sharding import PartitionSpec as P

PC = 88
NG, NM = 16, 8
BX, BY = 64, 128
FR, FC = 33, 264
MESH = pl.DeviceIdType.MESH
VM = pltpu.VMEM
F32 = jnp.float32
HI = lax.Precision.HIGHEST


def vspec():
    return pl.BlockSpec(memory_space=pltpu.VMEM)


def sspec():
    return pl.BlockSpec(memory_space=pltpu.SMEM)


def shape(*dims):
    return jax.ShapeDtypeStruct(dims, F32)


def iota(dims, axis):
    return lax.broadcasted_iota(jnp.int32, dims, axis)


def wrap(v, n):
    return jnp.where(v >= n, v - n, v)


def gx_peers(gx):
    x = gx // 4
    z = gx - 4 * x
    out = []
    for dx, dz in GX_OFFSETS:
        out.append(wrap(x + dx, 4) * 4 + wrap(z + dz, 4))
    return out


GX_OFFSETS = (
    (2, 2), (1, 2), (2, 1), (3, 2), (2, 3), (1, 1), (3, 3), (1, 3), (3, 1), (2, 0), (0, 2), (1, 0), (0, 1), (3, 0), (0, 3),
)


def gy_peers(gy):
    return [wrap(gy + d, NM) for d in range(1, NM)]


def all_peers(gx, gy):
    x = gx // 4
    z = gx - 4 * x
    y = gy // 2
    c = gy - 2 * y
    offs = [(a, b, d, e) for a in range(4) for b in range(4) for d in range(4) for e in range(2)][1:]
    offs.sort(key=lambda o: -sum(min(v, 4 - v) for v in o[:3]))
    xs = [wrap(x + d, 4) for d in range(4)]
    ys = [wrap(y + d, 4) for d in range(4)]
    zs = [wrap(z + d, 4) for d in range(4)]
    cs = [c, 1 - c]
    return [(xs[a] * 4 + zs[d], ys[b] * 2 + cs[e]) for a, b, d, e in offs]


def remote(src, dst, send, recv, a, b):
    return pltpu.make_async_remote_copy(
        src_ref=src, dst_ref=dst, send_sem=send, recv_sem=recv, device_id=(a, b), device_id_type=MESH
    )


def wait_bytes(ref, sem):
    pltpu.make_async_copy(ref, ref, sem).wait()


def slot(d, n, size=None):
    return pl.ds(pl.multiple_of(d * n, n), size or n)


def stencil(q, north, south, east, west, above, below, old, cpl, a0m, a0p, a1m, a1p, own, f):
    total = own * q[f] - old
    total += north * a0m - south * a0p
    total += east * a1m - west * a1p
    total -= 0.05 * (above + below)
    for g in range(4):
        total += cpl[f][g] * q[g]
    return total


def couplings(cp):
    return [[0.1 * cp[f, g] for g in range(4)] for f in range(4)]


KB = 0.02
KF = 0.02 * 9


def place_patches(off, pg, pxy):
    for g in range(NG):
        x = jnp.int32(0)
        y = jnp.int32(0)
        for p in range(NG):
            hit = pg[p] == g
            x = x + jnp.where(hit, off[0, p], 0)
            y = y + jnp.where(hit, off[1, p], 0)
        pxy[0, g] = x
        pxy[1, g] = y


def extract_base(r, c, pxy, base, trans, hr, hc, s1):
    flat = trans.reshape(2048, 128)
    for q in range(16):
        flat[pl.ds(q, 128, stride=16), :] = base[2 * q : 2 * q + 2].reshape(128, 128).T
    hr[0] = base[:, 0, :]
    hr[1] = base[:, BX - 1, :]
    hc[0] = trans[0]
    hc[1] = trans[127]

    def body(g, _):
        x = pxy[0, g]
        y = pxy[1, g]
        lo = x - 1 - r * BX
        hi = x + PC - r * BX
        loc = jnp.where((lo >= 0) & (lo < BX), lo, jnp.clip(hi, 0, BX - 1))
        s1[g, 0:32, :] = base[:, loc, :]
        y0 = jnp.clip(y - 1 - c * BY, 0, BY - 1)
        s1[g, 32:48, :] = trans[y0]
        y1 = jnp.clip(y + PC - c * BY, 0, BY - 1)
        s1[g, 48:64, :] = trans[y1]
        return 0

    lax.fori_loop(0, NG, body, 0)


def base_tendency(r, c, pxy, cpl, base, old, hrn, hcn, hz, tend):
    keep = [
        jnp.where(r > 0, 1.0, 0.0),
        jnp.where(r < NG - 1, 1.0, 0.0),
        jnp.where(c > 0, 1.0, 0.0),
        jnp.where(c < NM - 1, 1.0, 0.0),
    ]
    hz[0] = hrn[0] * keep[0]
    hz[1] = hrn[1] * keep[1]
    zeros = jnp.zeros((112, 128), F32)
    westc = jnp.concatenate([hcn[0] * keep[2], zeros], axis=0).T
    eastc = jnp.concatenate([hcn[1] * keep[3], zeros], axis=0).T
    row = iota((BX, BY), 0)
    lane = iota((BX, BY), 1)
    open_ = open_cells(r, c, pxy)
    own = 1.0 + 4 * KB + 0.1
    acc = jnp.zeros((BX, BY), F32)
    for l in range(8):
        q = [base[f * 8 + l] for f in range(4)]
        a0 = 0.05 * q[0]
        a1 = 0.05 * q[1]
        for f in range(4):
            p = f * 8 + l
            pair, par = p // 2, p % 2
            north = jnp.where(row == BX - 1, hz[1, p : p + 1, :], pltpu.roll(q[f], BX - 1, 0))
            south = jnp.where(row == 0, hz[0, p : p + 1, :], pltpu.roll(q[f], 1, 0))
            ecol = pltpu.roll(eastc[par * 64 : par * 64 + 64], 127 - pair, 1)
            wcol = pltpu.roll(westc[par * 64 : par * 64 + 64], (128 - pair) % 128, 1)
            east = jnp.where(lane == BY - 1, ecol, pltpu.roll(q[f], BY - 1, 1))
            west = jnp.where(lane == 0, wcol, pltpu.roll(q[f], 1, 1))
            none = jnp.zeros((BX, BY), F32)
            above = base[p + 1] if l < 7 else none
            below = base[p - 1] if l > 0 else none
            total = stencil(
                q, north, south, east, west, above, below, old[p], cpl,
                a0 - KB, a0 + KB, a1 - KB, a1 + KB, own, f,
            )
            tend[p] = total
            acc = acc + open_ * (total * total)
    return acc.reshape(8, 8, 128).sum(axis=0)


def open_cells(r, c, pxy):
    row = iota((BX, BY), 0)
    lane = iota((BX, BY), 1)
    cells = jnp.ones((BX, BY), F32)
    for g in range(NG):
        x = pxy[0, g] - r * BX
        y = pxy[1, g] - c * BY
        inside = (row >= x) & (row < x + PC) & (lane >= y) & (lane < y + PC)
        cells = jnp.where(inside, 0.0, cells)
    return cells


def fine_interior(cpl, fine, old, pad, res):
    for f in range(4):
        pad[f * 10] = jnp.zeros((56, 384), F32)
        pad[f * 10 + 9] = jnp.zeros((56, 384), F32)

    def fill(p, _):
        dst = p + 2 * (p // 8) + 1
        pad[dst, 0:8, :] = jnp.zeros((8, 384), F32)
        pad[dst, 8 : 8 + FR, 0:256] = fine[p, :, 0:256]
        pad[dst, 8 : 8 + FR, 256:384] = jnp.concatenate([fine[p, :, 256:FC], jnp.zeros((FR, 120), F32)], axis=1)
        pad[dst, 8 + FR : 9 + FR, :] = jnp.zeros((1, 384), F32)
        return 0

    lax.fori_loop(0, 32, fill, 0)
    own = 1.0 + 4 * KF + 0.1

    def level(l, acc):
        for start, n in ((0, 8), (8, 8), (16, 8), (24, 8), (32, 1)):
            s = 8 + start
            q = [pad[f * 10 + 1 + l, s : s + n, :] for f in range(4)]
            a0 = 0.15 * q[0]
            a1 = 0.15 * q[1]
            keep = iota((n, 384), 1) < FC
            for f in range(4):
                z = f * 10 + 1 + l
                north = pad[z, s + 1 : s + 1 + n, :]
                south = pad[z, s - 1 : s - 1 + n, :]
                east = pltpu.roll(q[f], 383, 1)
                west = pltpu.roll(q[f], 1, 1)
                p = f * 8 + l
                before = old[p, start : start + n, :]
                before = jnp.concatenate([before, jnp.zeros((n, 384 - FC), F32)], axis=1)
                total = stencil(
                    q, north, south, east, west, pad[z + 1, s : s + n, :], pad[z - 1, s : s + n, :],
                    before, cpl, a0 - KF, a0 + KF, a1 - KF, a1 + KF, own, f,
                )
                total = jnp.where(keep, total, 0.0)
                for t in range(3):
                    part = total[:, 128 * t : 128 * t + 128]
                    res[pl.ds((t * 32 + p) * 40 + start, n), :] = part
                    sq = part * part
                    if n == 1:
                        sq = jnp.where(iota((8, 128), 0) == 0, jnp.broadcast_to(sq, (8, 128)), 0.0)
                    acc = acc + sq
        return acc

    return lax.fori_loop(0, 8, level, jnp.zeros((8, 128), F32))


def edge_columns(x, y, j, gr):
    first = lax.rem(x + 11 * j, BX)
    cl = jnp.maximum(y - 1, 0) // BY
    cr = (y + PC) // BY
    blank = jnp.zeros((96, 128), F32)
    va = jnp.concatenate([gr[cl, 0:16, :], gr[cr, 16:32, :], blank], axis=0)
    vb = jnp.concatenate([gr[cl, 32:48, :], gr[cr, 48:64, :], blank], axis=0)
    want = first + iota((40, 128), 0) // 3
    lane40 = iota((40, 128), 1)
    cols = []
    for par in range(2):
        at = lane40 - 64 * par
        good = (at >= 0) & (at < 64)
        pa = jnp.where(good & (at == want), 1.0, 0.0)
        pb = jnp.where(good & (at + 64 == want), 1.0, 0.0)
        dims = (((1,), (1,)), ((), ()))
        cols.append(
            lax.dot_general(pa, va, dims, precision=HI, preferred_element_type=F32)
            + lax.dot_general(pb, vb, dims, precision=HI, preferred_element_type=F32)
        )
    return cols


def edge_row(y, cells):
    c0 = y // BY
    c1 = jnp.minimum(c0 + 1, NM - 1)
    b = iota((128, 384), 0)
    jf = iota((128, 384), 1)
    cell = y + jf // 3 - c0 * BY
    good = jf < FC
    p0 = jnp.where(good & (b == cell), 1.0, 0.0)
    p1 = jnp.where(good & (b + BY == cell), 1.0, 0.0)
    return jnp.dot(cells[c0], p0, precision=HI, preferred_element_type=F32) + jnp.dot(
        cells[c1], p1, precision=HI, preferred_element_type=F32
    )


def fine_edges(cols, hrow, fh, fine, res):
    change = jnp.zeros((8, 128), F32)
    for t in range(3):
        for row, side in ((0, 0), (FR - 1, 1)):
            a0 = 0.15 * fh[side, 0:8, 128 * t : 128 * t + 128]
            factor = a0 - KF if side else -(a0 + KF)
            factor = jnp.concatenate([factor] * 4, axis=0)
            at = pl.ds(t * 32 * 40 + row, 32, stride=40)
            was = res[at, :]
            now = was + hrow[side, :, 128 * t : 128 * t + 128] * factor
            res[at, :] = now
            for f in range(4):
                change = change + (now[8 * f : 8 * f + 8] * now[8 * f : 8 * f + 8])
                change = change - (was[8 * f : 8 * f + 8] * was[8 * f : 8 * f + 8])
    lane = iota((FR, 128), 1)
    for l in range(8):
        q1 = fine[8 + l, :, 0:128]
        lo = -(0.15 * q1 + KF)
        q1 = jnp.concatenate([fine[8 + l, :, 256:FC], jnp.zeros((FR, 120), F32)], axis=1)
        hi = 0.15 * q1 - KF
        for f in range(4):
            p = f * 8 + l
            pair, par = p // 2, p % 2
            cv = cols[par][:FR]
            for t, factor, spot, turn in ((0, lo, 0, (128 - pair) % 128), (2, hi, 7, 119 - pair)):
                at = pl.ds((t * 32 + p) * 40, FR)
                was = res[at, :]
                now = jnp.where(lane == spot, was + pltpu.roll(cv, turn, 1) * factor, was)
                res[at, :] = now
                delta = now * now - was * was
                change = change + delta[0:8] + delta[8:16] + delta[16:24] + delta[24:32]
                change = change + jnp.where(iota((8, 128), 0) == 0, jnp.broadcast_to(delta[32:33], (8, 128)), 0.0)
    return change


def restrict(x, j, norm, res, mm, cells, ss):
    for t in range(3):
        mm[t, :, 8:16, :] = jnp.zeros((32, 8, 128), F32)

    def rows(pair, _):
        for par in range(2):
            for t in range(3):
                at = (t * 32 + 2 * pair + par) * 40
                part = [res[pl.ds(at + d, 11, stride=3), :] for d in range(3)]
                mm[t, par * 16 + pair, 0:11, :] = part[0] + part[1] + part[2]
        return 0

    lax.fori_loop(0, 16, rows, 0, unroll=2)
    total = 0.0
    for t in range(3):
        comb = jnp.where((iota((128, 128), 0) + 128 * t) // 3 == iota((128, 128), 1), 1.0, 0.0)
        total = total + jnp.dot(mm[t].reshape(512, 128), comb, precision=HI, preferred_element_type=F32)
    cells[...] = (total * (1.0 / 9.0)).reshape(32, 16, 128)
    lane = iota((16, 128), 1)
    for k in range(NM):
        first = lax.rem(k - x - 11 * j + 2048, 8)
        for par in range(2):
            for h in range(2):
                v = cells[pl.ds(par * 16, 16), first + 8 * h, :]
                if par == 0 and h == 0:
                    v = jnp.where(lane == 127, norm, v)
                ss[pl.ds(k * 8 + par * 2 + h, 16, stride=64), :] = v


def compose(j, pxy, rs, so):
    n = iota((1, 512), 1)
    e = n // 128
    g = (n - e * 128) // 8
    k = n - (n // 8) * 8
    x = jnp.zeros((1, 512), jnp.int32)
    for i in range(NG):
        x = jnp.where(g == i, pxy[0, i], x)
    start = x + 11 * k
    away = j - start + 2048
    first = away - (away // 8) * 8
    h = e - (e // 2) * 2
    row = first + 8 * h
    octet = jnp.where(row <= 10, (start + row - j) // 8, -1)
    take = iota((256, 512), 0)
    par = take // 128
    take = jnp.where((take - par * 128 == octet) & (par == e // 2), 1.0, 0.0)
    lane = iota((8, 128), 1)
    rolled = []
    for i in range(NG):
        y = pxy[1, i]
        shift = lax.rem(y, BY)
        v = [rs[pl.ds(i * 64 + q, 8, stride=8), :] for q in range(4)]
        shift = jnp.broadcast_to(shift, (8, 128))
        for bit in range(7):
            shift, odd = shift // 2, shift - 2 * (shift // 2) == 1
            v = [jnp.where(odd, pltpu.roll(u, 1 << bit, 1), u) for u in v]
        rolled.append(v)
    for c in range(NM):
        parts = [[], [], [], []]
        for i in range(NG):
            at = lane + c * BY - pxy[1, i]
            inside = (at >= 0) & (at < PC)
            for q in range(4):
                parts[q].append(jnp.where(inside, rolled[i][q], 0.0))
        b = jnp.concatenate(parts[0] + parts[1] + parts[2] + parts[3], axis=0)
        got = jnp.dot(take, b, precision=HI, preferred_element_type=F32)
        for r in range(NG):
            for q in range(2):
                so[pl.ds((r * NM + c) * 16 + 8 * q, 8), :] = got[q * 128 + 8 * r : q * 128 + 8 * r + 8]


def main_kernel(
    pxy, cp, base_h, old_h, fine_h, fold_h,
    tend_h, fout_h, norm_h, r2,
    base, old, fine, fold, tend, trans, s1, hr, hc, fh, r1, hrn, hcn, fhn, gs, tb, gr, tr, br, hz,
    pad, hrow, res, mm, cells, ss, rs, so, nv, fout,
    la, sa, sb, sc, sd, se, lb,
):
    gx = lax.axis_index("gx")
    gy = lax.axis_index("gy")
    me = gx * NM + gy
    ga = gx_peers(gx)
    gb = gy_peers(gy)
    peers = all_peers(gx, gy)
    loads = [
        pltpu.make_async_copy(base_h, base, la.at[0]),
        pltpu.make_async_copy(fine_h.at[:, :, 0, :], fine, la.at[1]),
        pltpu.make_async_copy(fold_h.at[:, :, 0, :], fold, la.at[2]),
        pltpu.make_async_copy(old_h, old, la.at[3]),
    ]
    for load in loads:
        load.start()
    bar = pltpu.get_barrier_semaphore()
    for a, b in peers:
        pl.semaphore_signal(bar, inc=1, device_id=(a, b), device_id_type=MESH)
    cpl = couplings(cp)
    loads[0].wait()
    extract_base(gx, gy, pxy, base, trans, hr, hc, s1)
    loads[1].wait()
    blank = jnp.zeros((32, 384 - FC), F32)
    fh[0] = jnp.concatenate([fine[:, 0, :], blank], axis=1)
    fh[1] = jnp.concatenate([fine[:, FR - 1, :], blank], axis=1)
    own = pltpu.make_async_copy(s1.at[gx], r1.at[gx], lb.at[0])
    own.start()
    pl.semaphore_wait(bar, len(peers))

    up, down = wrap(gx + 1, NG), wrap(gx + NG - 1, NG)
    right, left = wrap(gy + 1, NM), wrap(gy + NM - 1, NM)
    halos = [
        remote(hr.at[1], hrn.at[0], sb.at[0], sb.at[1], up, gy),
        remote(hr.at[0], hrn.at[1], sb.at[2], sb.at[3], down, gy),
        remote(hc.at[1], hcn.at[0], sb.at[4], sb.at[5], gx, right),
        remote(hc.at[0], hcn.at[1], sb.at[6], sb.at[7], gx, left),
        remote(fh.at[1], fhn.at[0], sb.at[8], sb.at[9], gx, right),
        remote(fh.at[0], fhn.at[1], sb.at[10], sb.at[11], gx, left),
    ]
    for a in ga:
        remote(s1.at[a], r1.at[gx], sa.at[0], sa.at[1], a, gy).start()
    for h in halos:
        h.start()

    loads[2].wait()
    acc = fine_interior(cpl, fine, fold, pad, res)

    own.wait()
    wait_bytes(r1.at[pl.ds(0, NG - 1)], sa.at[1])
    x = pxy[0, gx]
    y = pxy[1, gx]
    tb[0] = r1[jnp.maximum(x - 1, 0) // BX, 0:32, :]
    tb[1] = r1[(x + PC) // BX, 0:32, :]
    for j in range(NM):
        a = (x + 11 * j) // BX
        b = jnp.minimum(a + 1, NG - 1)
        gs[j, 0:32, :] = r1[a, 32:64, :]
        gs[j, 32:64, :] = r1[b, 32:64, :]
    for b in gb:
        remote(gs.at[b], gr.at[gy], sc.at[0], sc.at[1], gx, b).start()
    mine = pltpu.make_async_copy(gs.at[gy], gr.at[gy], lb.at[1])
    mine.start()
    ends = ((tr, 0, 0), (br, NM - 1, 1))
    for ref, target, k in ends:
        far = remote(tb.at[k], ref.at[gy], sc.at[2 + 2 * k], sc.at[3 + 2 * k], gx, target)
        near = pltpu.make_async_copy(tb.at[k], ref.at[gy], lb.at[2])

        @pl.when(gy != target)
        def _():
            far.start()

        @pl.when(gy == target)
        def _():
            near.start()

    for h in halos:
        h.wait()
    loads[3].wait()
    hrow[0] = fhn[0]
    hrow[1] = fhn[1]
    bsum = base_tendency(gx, gy, pxy, cpl, base, old, hrn, hcn, hz, tend)
    tput = pltpu.make_async_copy(tend, tend_h, lb.at[3])
    tput.start()

    mine.wait()
    wait_bytes(gr.at[pl.ds(0, NM - 1)], sc.at[1])
    for ref, target, k in ends:
        far = remote(tb.at[k], ref.at[gy], sc.at[2 + 2 * k], sc.at[3 + 2 * k], gx, target)
        near = pltpu.make_async_copy(tb.at[k], ref.at[gy], lb.at[2])

        @pl.when(gy != target)
        def _():
            far.wait_send()

        @pl.when(gy == target)
        def _():
            near.wait()
            wait_bytes(ref.at[pl.ds(0, NM - 1)], sc.at[3 + 2 * k])
            hrow[k] = edge_row(y, ref)

    cols = edge_columns(x, y, gy, gr)
    acc = acc + fine_edges(cols, hrow, fh, fine, res)
    norm = jnp.sum(bsum + acc * (1.0 / 9.0), axis=(0, 1), keepdims=True)
    restrict(x, gy, norm, res, mm, cells, ss)
    rs[slot(me, 8), :] = ss[slot(me, 8), :]
    for a, b in peers:
        remote(ss.at[slot(a * NM + b, 8, 4), :], rs.at[slot(me, 8, 4), :], sd.at[0], sd.at[1], a, b).start()

    def write(p, _):
        for t in range(2):
            fout[p, :, 128 * t : 128 * t + 128] = res[pl.ds((t * 32 + p) * 40, FR), :]
        fout[p, :, 256:FC] = res[pl.ds((64 + p) * 40, FR), :][:, 0 : FC - 256]
        return 0

    lax.fori_loop(0, 32, write, 0)
    fput = pltpu.make_async_copy(fout, fout_h, lb.at[4])
    fput.start()

    n = NG * NM - 1
    wait_bytes(rs.at[pl.ds(0, 4 * n), :], sd.at[1])
    compose(gy, pxy, rs, so)
    for a, b in peers:
        remote(so.at[slot(a * NM + b, 16), :], r2.at[slot(me, 16), :], se.at[0], se.at[1], a, b).start()
    keep = pltpu.make_async_copy(so.at[slot(me, 16), :], r2.at[slot(me, 16), :], lb.at[5])
    keep.start()
    total = jnp.sum(rs[pl.ds(0, 128, stride=8), :], axis=0, keepdims=True)
    nv[...] = jnp.broadcast_to(jnp.sqrt(total[:, 127:128]), (8, 128))
    nput = pltpu.make_async_copy(nv, norm_h, lb.at[6])
    nput.start()
    nput.wait()
    keep.wait()
    tput.wait()
    fput.wait()
    wait_bytes(r1.at[pl.ds(0, NG - 1)], sa.at[0])
    wait_bytes(gr.at[pl.ds(0, NM - 1)], sc.at[0])
    wait_bytes(rs.at[pl.ds(0, 4 * n), :], sd.at[0])
    wait_bytes(so.at[pl.ds(0, 16 * n), :], se.at[0])
    wait_bytes(so.at[pl.ds(0, 16 * n), :], se.at[1])


def main(pxy, cp, base, old, fine, fold):
    hbm = pl.BlockSpec(memory_space=pl.ANY)
    dma = pltpu.SemaphoreType.DMA
    return pl.pallas_call(
        main_kernel,
        out_shape=(shape(32, BX, BY), shape(32, FR, FC), shape(8, 128), shape(2048, 128)),
        in_specs=[sspec()] * 2 + [hbm] * 4,
        out_specs=(hbm,) * 4,
        scratch_shapes=[
            VM((32, BX, BY), F32),
            VM((32, BX, BY), F32),
            VM((32, FR, FC), F32),
            VM((32, FR, FC), F32),
            VM((32, BX, BY), F32),
            VM((128, 16, 128), F32),
            VM((NG, 64, 128), F32),
            VM((2, 32, 128), F32),
            VM((2, 16, 128), F32),
            VM((2, 32, 384), F32),
            VM((NG, 64, 128), F32),
            VM((2, 32, 128), F32),
            VM((2, 16, 128), F32),
            VM((2, 32, 384), F32),
            VM((NM, 64, 128), F32),
            VM((2, 32, 128), F32),
            VM((NM, 64, 128), F32),
            VM((NM, 32, 128), F32),
            VM((NM, 32, 128), F32),
            VM((2, 32, 128), F32),
            VM((40, 56, 384), F32),
            VM((2, 32, 384), F32),
            VM((3 * 32 * 40, 128), F32),
            VM((3, 32, 16, 128), F32),
            VM((32, 16, 128), F32),
            VM((1024, 128), F32),
            VM((1024, 128), F32),
            VM((2048, 128), F32),
            VM((8, 128), F32),
            VM((32, FR, FC), F32),
            dma((4,)),
            dma((2,)),
            dma((12,)),
            dma((6,)),
            dma((2,)),
            dma((2,)),
            dma((7,)),
        ],
        compiler_params=pltpu.CompilerParams(collective_id=0, has_side_effects=True),
    )(pxy, cp, base, old, fine, fold)


def merge_kernel(off, tend, ri, fout, nv, out, fres, norm, sem):
    r = lax.axis_index("gx")
    c = lax.axis_index("gy")
    put = pltpu.make_async_copy(fout, fres.at[:, :, 0, :], sem)
    put.start()
    row = iota((8, BY), 0)
    lane = iota((8, BY), 1)
    for t in range(8):
        inside = jnp.zeros((8, BY), jnp.bool_)
        for g in range(NG):
            x = off[0, g] - r * BX - 8 * t
            y = off[1, g] - c * BY
            inside = inside | ((row >= x) & (row < x + PC) & (lane >= y) & (lane < y + PC))
        for p in range(32):
            got = ri[pl.ds((p // 2) * 128 + (p % 2) * 8 + t, 8, stride=16), :]
            out[p, 8 * t : 8 * t + 8, :] = jnp.where(inside, got, tend[p, 8 * t : 8 * t + 8, :])
    norm[...] = nv[0:1, 0:1]
    put.wait()


def merge(off, tend, ri, fout, nv):
    return pl.pallas_call(
        merge_kernel,
        out_shape=(shape(32, BX, BY), shape(32, FR, 1, FC), shape(1, 1)),
        in_specs=[sspec()] + [vspec()] * 4,
        out_specs=(vspec(), pl.BlockSpec(memory_space=pl.ANY), vspec()),
        scratch_shapes=[pltpu.SemaphoreType.DMA],
    )(off, tend, ri, fout, nv)


def local(base_state, base_old, fine_state, fine_old, coupling, patch_offsets, patch_group):
    base = base_state.reshape(32, BX, BY)
    old = base_old.reshape(32, BX, BY)
    fine = fine_state.reshape(32, FR, 1, FC)
    fold = fine_old.reshape(32, FR, 1, FC)
    off = patch_offsets.T
    owner = patch_group[None, :] == jnp.arange(NG, dtype=jnp.int32)[:, None]
    pxy = jnp.sum(jnp.where(owner[None], off[:, None, :], 0), axis=2)
    tend, fout, nv, r2 = main(pxy, coupling, base, old, fine, fold)
    bout, fres, norm = merge(off, tend, r2, fout, nv)
    return (
        bout.reshape(4, 8, BX, BY),
        fres.reshape(4, 8, 1, FR, FC),
        norm.reshape(()),
    )


def solution(mesh):
    placed = (
        P(None, None, "gx", "gy"),
        P(None, None, "gx", "gy"),
        P(None, None, "gx", "gy", None),
        P(None, None, "gx", "gy", None),
        P(),
        P(),
        P(),
    )
    return jax.shard_map(
        local,
        mesh=mesh,
        in_specs=placed,
        out_specs=(P(None, None, "gx", "gy"), P(None, None, "gx", "gy", None), P()),
        check_vma=False,
    )
```

```python
import functools

import jax
import jax.numpy as jnp
from jax import lax
from jax.experimental import pallas as pl
from jax.experimental.pallas import tpu as pltpu
from jax.sharding import PartitionSpec as P

PC = 88
NG, NM = 16, 8
BX, BY = 64, 128
FR, FC = 33, 264
MESH = pl.DeviceIdType.MESH
VM = pltpu.VMEM
F32 = jnp.float32
HI = lax.Precision.HIGHEST


def vspec():
    return pl.BlockSpec(memory_space=pltpu.VMEM)


def sspec():
    return pl.BlockSpec(memory_space=pltpu.SMEM)


def shape(*dims):
    return jax.ShapeDtypeStruct(dims, F32)


def iota(dims, axis):
    return lax.broadcasted_iota(jnp.int32, dims, axis)


def wrap(v, n):
    return jnp.where(v >= n, v - n, v)


def gx_peers(gx):
    x = gx // 4
    z = gx - 4 * x
    out = []
    for dx, dz in GX_OFFSETS:
        out.append(wrap(x + dx, 4) * 4 + wrap(z + dz, 4))
    return out


GX_OFFSETS = (
    (2, 2), (1, 2), (2, 1), (3, 2), (2, 3), (1, 1), (3, 3), (1, 3), (3, 1), (2, 0), (0, 2), (1, 0), (0, 1), (3, 0), (0, 3),
)


def gy_peers(gy):
    return [wrap(gy + d, NM) for d in range(1, NM)]


def all_peers(gx, gy):
    x = gx // 4
    z = gx - 4 * x
    y = gy // 2
    c = gy - 2 * y
    offs = [(a, b, d, e) for a in range(4) for b in range(4) for d in range(4) for e in range(2)][1:]
    offs.sort(key=lambda o: -sum(min(v, 4 - v) for v in o[:3]))
    xs = [wrap(x + d, 4) for d in range(4)]
    ys = [wrap(y + d, 4) for d in range(4)]
    zs = [wrap(z + d, 4) for d in range(4)]
    cs = [c, 1 - c]
    return [(xs[a] * 4 + zs[d], ys[b] * 2 + cs[e]) for a, b, d, e in offs]


def remote(src, dst, send, recv, a, b):
    return pltpu.make_async_remote_copy(
        src_ref=src, dst_ref=dst, send_sem=send, recv_sem=recv, device_id=(a, b), device_id_type=MESH
    )


def wait_bytes(ref, sem):
    pltpu.make_async_copy(ref, ref, sem).wait()


def slot(d, n, size=None):
    return pl.ds(pl.multiple_of(d * n, n), size or n)


def stencil(q, north, south, east, west, above, below, old, cpl, a0m, a0p, a1m, a1p, own, f):
    total = own * q[f] - old
    total += north * a0m - south * a0p
    total += east * a1m - west * a1p
    total -= 0.05 * (above + below)
    for g in range(4):
        total += cpl[f][g] * q[g]
    return total


def couplings(cp):
    return [[0.1 * cp[f, g] for g in range(4)] for f in range(4)]


KB = 0.02
KF = 0.02 * 9


def place_patches(off, pg, pxy):
    for g in range(NG):
        x = jnp.int32(0)
        y = jnp.int32(0)
        for p in range(NG):
            hit = pg[p] == g
            x = x + jnp.where(hit, off[0, p], 0)
            y = y + jnp.where(hit, off[1, p], 0)
        pxy[0, g] = x
        pxy[1, g] = y


def extract_base(r, c, pxy, base, trans, hr, hc, s1):
    flat = trans.reshape(2048, 128)
    for q in range(16):
        flat[pl.ds(q, 128, stride=16), :] = base[2 * q : 2 * q + 2].reshape(128, 128).T
    hr[0] = base[:, 0, :]
    hr[1] = base[:, BX - 1, :]
    hc[0] = trans[0]
    hc[1] = trans[127]

    def body(g, _):
        x = pxy[0, g]
        y = pxy[1, g]
        lo = x - 1 - r * BX
        hi = x + PC - r * BX
        loc = jnp.where((lo >= 0) & (lo < BX), lo, jnp.clip(hi, 0, BX - 1))
        s1[g, 0:32, :] = base[:, loc, :]
        y0 = jnp.clip(y - 1 - c * BY, 0, BY - 1)
        s1[g, 32:48, :] = trans[y0]
        y1 = jnp.clip(y + PC - c * BY, 0, BY - 1)
        s1[g, 48:64, :] = trans[y1]
        return 0

    lax.fori_loop(0, NG, body, 0)


def base_tendency(r, c, pxy, cpl, base, old, hrn, hcn, hz, tend):
    keep = [
        jnp.where(r > 0, 1.0, 0.0),
        jnp.where(r < NG - 1, 1.0, 0.0),
        jnp.where(c > 0, 1.0, 0.0),
        jnp.where(c < NM - 1, 1.0, 0.0),
    ]
    hz[0] = hrn[0] * keep[0]
    hz[1] = hrn[1] * keep[1]
    zeros = jnp.zeros((112, 128), F32)
    westc = jnp.concatenate([hcn[0] * keep[2], zeros], axis=0).T
    eastc = jnp.concatenate([hcn[1] * keep[3], zeros], axis=0).T
    row = iota((BX, BY), 0)
    lane = iota((BX, BY), 1)
    open_ = open_cells(r, c, pxy)
    own = 1.0 + 4 * KB + 0.1
    acc = jnp.zeros((BX, BY), F32)
    for l in range(8):
        q = [base[f * 8 + l] for f in range(4)]
        a0 = 0.05 * q[0]
        a1 = 0.05 * q[1]
        for f in range(4):
            p = f * 8 + l
            pair, par = p // 2, p % 2
            north = jnp.where(row == BX - 1, hz[1, p : p + 1, :], pltpu.roll(q[f], BX - 1, 0))
            south = jnp.where(row == 0, hz[0, p : p + 1, :], pltpu.roll(q[f], 1, 0))
            ecol = pltpu.roll(eastc[par * 64 : par * 64 + 64], 127 - pair, 1)
            wcol = pltpu.roll(westc[par * 64 : par * 64 + 64], (128 - pair) % 128, 1)
            east = jnp.where(lane == BY - 1, ecol, pltpu.roll(q[f], BY - 1, 1))
            west = jnp.where(lane == 0, wcol, pltpu.roll(q[f], 1, 1))
            none = jnp.zeros((BX, BY), F32)
            above = base[p + 1] if l < 7 else none
            below = base[p - 1] if l > 0 else none
            total = stencil(
                q, north, south, east, west, above, below, old[p], cpl,
                a0 - KB, a0 + KB, a1 - KB, a1 + KB, own, f,
            )
            tend[p] = total
            acc = acc + open_ * (total * total)
    return acc.reshape(8, 8, 128).sum(axis=0)


def open_cells(r, c, pxy):
    row = iota((BX, BY), 0)
    lane = iota((BX, BY), 1)
    cells = jnp.ones((BX, BY), F32)
    for g in range(NG):
        x = pxy[0, g] - r * BX
        y = pxy[1, g] - c * BY
        inside = (row >= x) & (row < x + PC) & (lane >= y) & (lane < y + PC)
        cells = jnp.where(inside, 0.0, cells)
    return cells


def fine_interior(cpl, fine, old, pad, res):
    for f in range(4):
        pad[f * 10] = jnp.zeros((56, 384), F32)
        pad[f * 10 + 9] = jnp.zeros((56, 384), F32)

    def fill(p, _):
        dst = p + 2 * (p // 8) + 1
        pad[dst, 0:8, :] = jnp.zeros((8, 384), F32)
        pad[dst, 8 : 8 + FR, 0:256] = fine[p, :, 0:256]
        pad[dst, 8 : 8 + FR, 256:384] = jnp.concatenate([fine[p, :, 256:FC], jnp.zeros((FR, 120), F32)], axis=1)
        pad[dst, 8 + FR : 9 + FR, :] = jnp.zeros((1, 384), F32)
        return 0

    lax.fori_loop(0, 32, fill, 0)
    own = 1.0 + 4 * KF + 0.1

    def level(l, acc):
        for start, n in ((0, 8), (8, 8), (16, 8), (24, 8), (32, 1)):
            s = 8 + start
            q = [pad[f * 10 + 1 + l, s : s + n, :] for f in range(4)]
            a0 = 0.15 * q[0]
            a1 = 0.15 * q[1]
            keep = iota((n, 384), 1) < FC
            for f in range(4):
                z = f * 10 + 1 + l
                north = pad[z, s + 1 : s + 1 + n, :]
                south = pad[z, s - 1 : s - 1 + n, :]
                east = pltpu.roll(q[f], 383, 1)
                west = pltpu.roll(q[f], 1, 1)
                p = f * 8 + l
                before = old[p, start : start + n, :]
                before = jnp.concatenate([before, jnp.zeros((n, 384 - FC), F32)], axis=1)
                total = stencil(
                    q, north, south, east, west, pad[z + 1, s : s + n, :], pad[z - 1, s : s + n, :],
                    before, cpl, a0 - KF, a0 + KF, a1 - KF, a1 + KF, own, f,
                )
                total = jnp.where(keep, total, 0.0)
                for t in range(3):
                    part = total[:, 128 * t : 128 * t + 128]
                    res[pl.ds((t * 32 + p) * 40 + start, n), :] = part
                    sq = part * part
                    if n == 1:
                        sq = jnp.where(iota((8, 128), 0) == 0, jnp.broadcast_to(sq, (8, 128)), 0.0)
                    acc = acc + sq
        return acc

    return lax.fori_loop(0, 8, level, jnp.zeros((8, 128), F32))


def edge_columns(x, y, j, gr):
    first = lax.rem(x + 11 * j, BX)
    cl = jnp.maximum(y - 1, 0) // BY
    cr = (y + PC) // BY
    blank = jnp.zeros((96, 128), F32)
    va = jnp.concatenate([gr[cl, 0:16, :], gr[cr, 16:32, :], blank], axis=0)
    vb = jnp.concatenate([gr[cl, 32:48, :], gr[cr, 48:64, :], blank], axis=0)
    want = first + iota((40, 128), 0) // 3
    lane40 = iota((40, 128), 1)
    cols = []
    for par in range(2):
        at = lane40 - 64 * par
        good = (at >= 0) & (at < 64)
        pa = jnp.where(good & (at == want), 1.0, 0.0)
        pb = jnp.where(good & (at + 64 == want), 1.0, 0.0)
        dims = (((1,), (1,)), ((), ()))
        cols.append(
            lax.dot_general(pa, va, dims, precision=HI, preferred_element_type=F32)
            + lax.dot_general(pb, vb, dims, precision=HI, preferred_element_type=F32)
        )
    return cols


def edge_row(y, cells):
    c0 = y // BY
    c1 = jnp.minimum(c0 + 1, NM - 1)
    b = iota((128, 384), 0)
    jf = iota((128, 384), 1)
    cell = y + jf // 3 - c0 * BY
    good = jf < FC
    p0 = jnp.where(good & (b == cell), 1.0, 0.0)
    p1 = jnp.where(good & (b + BY == cell), 1.0, 0.0)
    return jnp.dot(cells[c0], p0, precision=HI, preferred_element_type=F32) + jnp.dot(
        cells[c1], p1, precision=HI, preferred_element_type=F32
    )


def fine_edges(cols, hrow, fh, fine, res):
    change = jnp.zeros((8, 128), F32)
    for t in range(3):
        for row, side in ((0, 0), (FR - 1, 1)):
            a0 = 0.15 * fh[side, 0:8, 128 * t : 128 * t + 128]
            factor = a0 - KF if side else -(a0 + KF)
            factor = jnp.concatenate([factor] * 4, axis=0)
            at = pl.ds(t * 32 * 40 + row, 32, stride=40)
            was = res[at, :]
            now = was + hrow[side, :, 128 * t : 128 * t + 128] * factor
            res[at, :] = now
            for f in range(4):
                change = change + (now[8 * f : 8 * f + 8] * now[8 * f : 8 * f + 8])
                change = change - (was[8 * f : 8 * f + 8] * was[8 * f : 8 * f + 8])
    lane = iota((FR, 128), 1)
    for l in range(8):
        q1 = fine[8 + l, :, 0:128]
        lo = -(0.15 * q1 + KF)
        q1 = jnp.concatenate([fine[8 + l, :, 256:FC], jnp.zeros((FR, 120), F32)], axis=1)
        hi = 0.15 * q1 - KF
        for f in range(4):
            p = f * 8 + l
            pair, par = p // 2, p % 2
            cv = cols[par][:FR]
            for t, factor, spot, turn in ((0, lo, 0, (128 - pair) % 128), (2, hi, 7, 119 - pair)):
                at = pl.ds((t * 32 + p) * 40, FR)
                was = res[at, :]
                now = jnp.where(lane == spot, was + pltpu.roll(cv, turn, 1) * factor, was)
                res[at, :] = now
                delta = now * now - was * was
                change = change + delta[0:8] + delta[8:16] + delta[16:24] + delta[24:32]
                change = change + jnp.where(iota((8, 128), 0) == 0, jnp.broadcast_to(delta[32:33], (8, 128)), 0.0)
    return change


def restrict(x, j, norm, res, mm, cells, ss):
    for t in range(3):
        mm[t, :, 8:16, :] = jnp.zeros((32, 8, 128), F32)

    def rows(pair, _):
        for par in range(2):
            for t in range(3):
                at = (t * 32 + 2 * pair + par) * 40
                part = [res[pl.ds(at + d, 11, stride=3), :] for d in range(3)]
                mm[t, par * 16 + pair, 0:11, :] = part[0] + part[1] + part[2]
        return 0

    lax.fori_loop(0, 16, rows, 0, unroll=2)
    total = 0.0
    for t in range(3):
        comb = jnp.where((iota((128, 128), 0) + 128 * t) // 3 == iota((128, 128), 1), 1.0, 0.0)
        total = total + jnp.dot(mm[t].reshape(512, 128), comb, precision=HI, preferred_element_type=F32)
    cells[...] = (total * (1.0 / 9.0)).reshape(32, 16, 128)
    lane = iota((16, 128), 1)
    for k in range(NM):
        first = lax.rem(k - x - 11 * j + 2048, 8)
        for par in range(2):
            for h in range(2):
                v = cells[pl.ds(par * 16, 16), first + 8 * h, :]
                if par == 0 and h == 0:
                    v = jnp.where(lane == 127, norm, v)
                ss[pl.ds(k * 8 + par * 2 + h, 16, stride=64), :] = v


def split3(v):
    hi = v.astype(jnp.bfloat16)
    rest = v - hi.astype(F32)
    mid = rest.astype(jnp.bfloat16)
    return hi, mid, (rest - mid.astype(F32)).astype(jnp.bfloat16)


def compose_send(gx, gy, pxy, rs, so, rolled, take, r2, sems):
    n = iota((1, 256), 1)
    h = n // 128
    g = (n - h * 128) // 8
    k = n - (n // 8) * 8
    x = jnp.zeros((1, 256), jnp.int32)
    for i in range(NG):
        x = jnp.where(g == i, pxy[0, i], x)
    start = x + 11 * k
    away = gy - start + 2048
    row = away - (away // 8) * 8 + 8 * h
    octet = jnp.where(row <= 10, (start + row - gy) // 8, -1)
    take[...] = jnp.where(iota((128, 256), 0) == octet, 1.0, 0.0).astype(jnp.bfloat16)
    for i in range(NG):
        v = [rs[pl.ds(i * 64 + q, 8, stride=8), :] for q in range(4)]
        shift = jnp.broadcast_to(lax.rem(pxy[1, i], BY), (8, 128))
        for bit in range(7):
            shift, odd = shift // 2, shift - 2 * (shift // 2) == 1
            v = [jnp.where(odd, pltpu.roll(u, 1 << bit, 1), u) for u in v]
        for q in range(4):
            rolled[q, 8 * i : 8 * i + 8, :] = v[q]
    lane = iota((8, 128), 1)
    x4 = gx // 4
    z4 = gx - 4 * x4

    def column(step, _):
        c = wrap(gy + step, NM)
        inside = []
        for i in range(NG):
            at = lane + c * BY - pxy[1, i]
            inside.append((at >= 0) & (at < PC))
        for par in range(2):
            rows = []
            for q in (2 * par, 2 * par + 1):
                for i in range(NG):
                    rows.append(jnp.where(inside[i], rolled[q, 8 * i : 8 * i + 8, :], 0.0))
            b = jnp.concatenate(split3(jnp.concatenate(rows, axis=0)), axis=1)
            got = jnp.dot(take[...], b, preferred_element_type=F32)
            got = got[:, 0:128] + (got[:, 128:256] + got[:, 256:384])
            for r in range(NG):
                at = pl.multiple_of((r * NM + c) * 16 + 8 * par, 8)
                so[pl.ds(at, 8), :] = got[8 * r : 8 * r + 8]

        for dx, dz in GX_OFFSETS + ((0, 0),):
            a = wrap(x4 + dx, 4) * 4 + wrap(z4 + dz, 4)
            send = remote(
                so.at[slot(a * NM + c, 16), :], r2.at[slot(gx * NM + gy, 16), :], sems.at[0], sems.at[1], a, c
            )
            if (dx, dz) == (0, 0):
                pl.when(step > 0)(send.start)
            else:
                send.start()
        return 0

    lax.fori_loop(0, NM, column, 0)


def main_kernel(
    off, pg, cp, base_h, old_h, fine_h, fold_h,
    tend_h, fout_h, norm_h, r2,
    pxy, base, old, fine, fold, tend, trans, s1, hr, hc, fh, r1, hrn, hcn, fhn, gs, tb, gr, tr, br, hz,
    pad, hrow, res, mm, cells, ss, rs, so, rolled, take, nv, fout,
    la, sa, sb, sc, sd, se, lb,
):
    gx = lax.axis_index("gx")
    gy = lax.axis_index("gy")
    me = gx * NM + gy
    ga = gx_peers(gx)
    gb = gy_peers(gy)
    peers = all_peers(gx, gy)
    loads = [
        pltpu.make_async_copy(base_h, base, la.at[0]),
        pltpu.make_async_copy(fine_h.at[:, :, 0, :], fine, la.at[1]),
        pltpu.make_async_copy(fold_h.at[:, :, 0, :], fold, la.at[2]),
        pltpu.make_async_copy(old_h, old, la.at[3]),
    ]
    for load in loads:
        load.start()
    bar = pltpu.get_barrier_semaphore()
    for a in ga:
        pl.semaphore_signal(bar, inc=1, device_id=(a, gy), device_id_type=MESH)
    for b in gb:
        pl.semaphore_signal(bar, inc=1, device_id=(gx, b), device_id_type=MESH)
    cpl = couplings(cp)
    place_patches(off, pg, pxy)
    loads[0].wait()
    extract_base(gx, gy, pxy, base, trans, hr, hc, s1)
    loads[1].wait()
    blank = jnp.zeros((32, 384 - FC), F32)
    fh[0] = jnp.concatenate([fine[:, 0, :], blank], axis=1)
    fh[1] = jnp.concatenate([fine[:, FR - 1, :], blank], axis=1)
    own = pltpu.make_async_copy(s1.at[gx], r1.at[gx], lb.at[0])
    own.start()
    pl.semaphore_wait(bar, len(ga) + len(gb))

    up, down = wrap(gx + 1, NG), wrap(gx + NG - 1, NG)
    right, left = wrap(gy + 1, NM), wrap(gy + NM - 1, NM)
    halos = [
        remote(hr.at[1], hrn.at[0], sb.at[0], sb.at[1], up, gy),
        remote(hr.at[0], hrn.at[1], sb.at[2], sb.at[3], down, gy),
        remote(hc.at[1], hcn.at[0], sb.at[4], sb.at[5], gx, right),
        remote(hc.at[0], hcn.at[1], sb.at[6], sb.at[7], gx, left),
        remote(fh.at[1], fhn.at[0], sb.at[8], sb.at[9], gx, right),
        remote(fh.at[0], fhn.at[1], sb.at[10], sb.at[11], gx, left),
    ]
    for a in ga:
        remote(s1.at[a], r1.at[gx], sa.at[0], sa.at[1], a, gy).start()
    for h in halos:
        h.start()

    loads[2].wait()
    acc = fine_interior(cpl, fine, fold, pad, res)

    own.wait()
    wait_bytes(r1.at[pl.ds(0, NG - 1)], sa.at[1])
    x = pxy[0, gx]
    y = pxy[1, gx]
    tb[0] = r1[jnp.maximum(x - 1, 0) // BX, 0:32, :]
    tb[1] = r1[(x + PC) // BX, 0:32, :]
    for j in range(NM):
        a = (x + 11 * j) // BX
        b = jnp.minimum(a + 1, NG - 1)
        gs[j, 0:32, :] = r1[a, 32:64, :]
        gs[j, 32:64, :] = r1[b, 32:64, :]
    for b in gb:
        remote(gs.at[b], gr.at[gy], sc.at[0], sc.at[1], gx, b).start()
    mine = pltpu.make_async_copy(gs.at[gy], gr.at[gy], lb.at[1])
    mine.start()
    ends = ((tr, 0, 0), (br, NM - 1, 1))
    for ref, target, k in ends:
        far = remote(tb.at[k], ref.at[gy], sc.at[2 + 2 * k], sc.at[3 + 2 * k], gx, target)
        near = pltpu.make_async_copy(tb.at[k], ref.at[gy], lb.at[2])

        @pl.when(gy != target)
        def _():
            far.start()

        @pl.when(gy == target)
        def _():
            near.start()

    for h in halos:
        h.wait()
    loads[3].wait()
    hrow[0] = fhn[0]
    hrow[1] = fhn[1]
    bsum = base_tendency(gx, gy, pxy, cpl, base, old, hrn, hcn, hz, tend)
    tput = pltpu.make_async_copy(tend, tend_h, lb.at[3])
    tput.start()

    mine.wait()
    wait_bytes(gr.at[pl.ds(0, NM - 1)], sc.at[1])
    for ref, target, k in ends:
        far = remote(tb.at[k], ref.at[gy], sc.at[2 + 2 * k], sc.at[3 + 2 * k], gx, target)
        near = pltpu.make_async_copy(tb.at[k], ref.at[gy], lb.at[2])

        @pl.when(gy != target)
        def _():
            far.wait_send()

        @pl.when(gy == target)
        def _():
            near.wait()
            wait_bytes(ref.at[pl.ds(0, NM - 1)], sc.at[3 + 2 * k])
            hrow[k] = edge_row(y, ref)

    cols = edge_columns(x, y, gy, gr)
    acc = acc + fine_edges(cols, hrow, fh, fine, res)
    norm = jnp.sum(bsum + acc * (1.0 / 9.0), axis=(0, 1), keepdims=True)
    restrict(x, gy, norm, res, mm, cells, ss)
    rs[slot(me, 8), :] = ss[slot(me, 8), :]
    for a, b in peers:
        remote(ss.at[slot(a * NM + b, 8, 4), :], rs.at[slot(me, 8, 4), :], sd.at[0], sd.at[1], a, b).start()

    def write(p, _):
        for t in range(2):
            fout[p, :, 128 * t : 128 * t + 128] = res[pl.ds((t * 32 + p) * 40, FR), :]
        fout[p, :, 256:FC] = res[pl.ds((64 + p) * 40, FR), :][:, 0 : FC - 256]
        return 0

    lax.fori_loop(0, 32, write, 0)
    fput = pltpu.make_async_copy(fout, fout_h, lb.at[4])
    fput.start()

    n = NG * NM - 1
    wait_bytes(rs.at[pl.ds(0, 4 * n), :], sd.at[1])
    compose_send(gx, gy, pxy, rs, so, rolled, take, r2, se)
    keep = pltpu.make_async_copy(so.at[slot(me, 16), :], r2.at[slot(me, 16), :], lb.at[5])
    keep.start()
    total = jnp.sum(rs[pl.ds(0, 128, stride=8), :], axis=0, keepdims=True)
    nv[...] = jnp.broadcast_to(jnp.sqrt(total[:, 127:128]), (8, 128))
    nput = pltpu.make_async_copy(nv, norm_h, lb.at[6])
    nput.start()
    nput.wait()
    keep.wait()
    tput.wait()
    fput.wait()
    wait_bytes(r1.at[pl.ds(0, NG - 1)], sa.at[0])
    wait_bytes(gr.at[pl.ds(0, NM - 1)], sc.at[0])
    wait_bytes(rs.at[pl.ds(0, 4 * n), :], sd.at[0])
    wait_bytes(so.at[pl.ds(0, 16 * n), :], se.at[0])
    wait_bytes(so.at[pl.ds(0, 16 * n), :], se.at[1])


def main(off, pg, cp, base, old, fine, fold):
    hbm = pl.BlockSpec(memory_space=pl.ANY)
    dma = pltpu.SemaphoreType.DMA
    return pl.pallas_call(
        main_kernel,
        out_shape=(shape(32, BX, BY), shape(32, FR, FC), shape(8, 128), shape(2048, 128)),
        in_specs=[sspec()] * 3 + [hbm] * 4,
        out_specs=(hbm,) * 4,
        scratch_shapes=[
            pltpu.SMEM((2, NG), jnp.int32),
            VM((32, BX, BY), F32),
            VM((32, BX, BY), F32),
            VM((32, FR, FC), F32),
            VM((32, FR, FC), F32),
            VM((32, BX, BY), F32),
            VM((128, 16, 128), F32),
            VM((NG, 64, 128), F32),
            VM((2, 32, 128), F32),
            VM((2, 16, 128), F32),
            VM((2, 32, 384), F32),
            VM((NG, 64, 128), F32),
            VM((2, 32, 128), F32),
            VM((2, 16, 128), F32),
            VM((2, 32, 384), F32),
            VM((NM, 64, 128), F32),
            VM((2, 32, 128), F32),
            VM((NM, 64, 128), F32),
            VM((NM, 32, 128), F32),
            VM((NM, 32, 128), F32),
            VM((2, 32, 128), F32),
            VM((40, 56, 384), F32),
            VM((2, 32, 384), F32),
            VM((3 * 32 * 40, 128), F32),
            VM((3, 32, 16, 128), F32),
            VM((32, 16, 128), F32),
            VM((1024, 128), F32),
            VM((1024, 128), F32),
            VM((2048, 128), F32),
            VM((4, 128, 128), F32),
            VM((128, 256), jnp.bfloat16),
            VM((8, 128), F32),
            VM((32, FR, FC), F32),
            dma((4,)),
            dma((2,)),
            dma((12,)),
            dma((6,)),
            dma((2,)),
            dma((2,)),
            dma((7,)),
        ],
        compiler_params=pltpu.CompilerParams(collective_id=0, has_side_effects=True),
    )(off, pg, cp, base, old, fine, fold)


PARTS = 4


def merge_kernel(off, tend, ri, fout, nv, out, fres, norm, covered, fine, sem):
    step = pl.program_id(0)
    piece = 32 // PARTS
    ins = [
        pltpu.make_async_copy(fout.at[pl.ds(piece * k, piece)], fine.at[pl.ds(piece * k, piece)], sem.at[k])
        for k in range(PARTS)
    ]
    outs = [
        pltpu.make_async_copy(fine.at[pl.ds(piece * k, piece)], fres.at[pl.ds(piece * k, piece), :, 0, :], sem.at[PARTS + k])
        for k in range(PARTS)
    ]

    @pl.when(step == 0)
    def _():
        for copy in ins:
            copy.start()
        r = lax.axis_index("gx")
        c = lax.axis_index("gy")
        row = iota((BX, BY), 0)
        lane = iota((BX, BY), 1)
        inside = jnp.zeros((BX, BY), F32)
        for g in range(NG):
            x = off[0, g] - r * BX
            y = off[1, g] - c * BY
            inside = jnp.where((row >= x) & (row < x + PC) & (lane >= y) & (lane < y + PC), 1.0, inside)
        covered[...] = inside
        norm[...] = nv[0:1, 0:1]

    for t in range(8):
        inside = covered[8 * t : 8 * t + 8, :] > 0.5
        for p in range(piece):
            got = ri[pl.ds((p // 2) * 128 + (p % 2) * 8 + t, 8, stride=16), :]
            out[p, 8 * t : 8 * t + 8, :] = jnp.where(inside, got, tend[p, 8 * t : 8 * t + 8, :])

    for k in range(PARTS):

        @pl.when(step == k)
        def _():
            ins[k].wait()
            outs[k].start()

    @pl.when(step == PARTS - 1)
    def _():
        for copy in outs:
            copy.wait()


def merge(off, tend, ri, fout, nv):
    hbm = pl.BlockSpec(memory_space=pl.ANY)
    piece = 32 // PARTS
    return pl.pallas_call(
        merge_kernel,
        grid=(PARTS,),
        out_shape=(shape(32, BX, BY), shape(32, FR, 1, FC), shape(1, 1)),
        in_specs=[
            sspec(),
            pl.BlockSpec((piece, BX, BY), lambda i: (i, 0, 0)),
            pl.BlockSpec((piece * 64, 128), lambda i: (i, 0)),
            hbm,
            pl.BlockSpec((8, 128), lambda i: (0, 0)),
        ],
        out_specs=(
            pl.BlockSpec((piece, BX, BY), lambda i: (i, 0, 0)),
            hbm,
            pl.BlockSpec((1, 1), lambda i: (0, 0)),
        ),
        scratch_shapes=[VM((BX, BY), F32), VM((32, FR, FC), F32), pltpu.SemaphoreType.DMA((2 * PARTS,))],
    )(off, tend, ri, fout, nv)


def local(base_state, base_old, fine_state, fine_old, coupling, patch_offsets, patch_group):
    base = base_state.reshape(32, BX, BY)
    old = base_old.reshape(32, BX, BY)
    fine = fine_state.reshape(32, FR, 1, FC)
    fold = fine_old.reshape(32, FR, 1, FC)
    off = patch_offsets.T
    tend, fout, nv, r2 = main(off, patch_group, coupling, base, old, fine, fold)
    bout, fres, norm = merge(off, tend, r2, fout, nv)
    return (
        bout.reshape(4, 8, BX, BY),
        fres.reshape(4, 8, 1, FR, FC),
        norm.reshape(()),
    )


def solution(mesh):
    placed = (
        P(None, None, "gx", "gy"),
        P(None, None, "gx", "gy"),
        P(None, None, "gx", "gy", None),
        P(None, None, "gx", "gy", None),
        P(),
        P(),
        P(),
    )
    return jax.shard_map(
        local,
        mesh=mesh,
        in_specs=placed,
        out_specs=(P(None, None, "gx", "gy"), P(None, None, "gx", "gy", None), P()),
        check_vma=False,
    )
```

```python
import functools

import jax
import jax.numpy as jnp
from jax import lax
from jax.experimental import pallas as pl
from jax.experimental.pallas import tpu as pltpu
from jax.sharding import PartitionSpec as P

PC = 88
NG, NM = 16, 8
BX, BY = 64, 128
FR, FC = 33, 264
MESH = pl.DeviceIdType.MESH
VM = pltpu.VMEM
F32 = jnp.float32
HI = lax.Precision.HIGHEST


def vspec():
    return pl.BlockSpec(memory_space=pltpu.VMEM)


def sspec():
    return pl.BlockSpec(memory_space=pltpu.SMEM)


def shape(*dims):
    return jax.ShapeDtypeStruct(dims, F32)


def iota(dims, axis):
    return lax.broadcasted_iota(jnp.int32, dims, axis)


def wrap(v, n):
    return jnp.where(v >= n, v - n, v)


def gx_peers(gx):
    x = gx // 4
    z = gx - 4 * x
    out = []
    for dx, dz in GX_OFFSETS:
        out.append(wrap(x + dx, 4) * 4 + wrap(z + dz, 4))
    return out


GX_OFFSETS = (
    (2, 2), (1, 2), (2, 1), (3, 2), (2, 3), (1, 1), (3, 3), (1, 3), (3, 1), (2, 0), (0, 2), (1, 0), (0, 1), (3, 0), (0, 3),
)


def gy_peers(gy):
    return [wrap(gy + d, NM) for d in range(1, NM)]


def all_peers(gx, gy):
    x = gx // 4
    z = gx - 4 * x
    y = gy // 2
    c = gy - 2 * y
    offs = [(a, b, d, e) for a in range(4) for b in range(4) for d in range(4) for e in range(2)][1:]
    offs.sort(key=lambda o: -sum(min(v, 4 - v) for v in o[:3]))
    xs = [wrap(x + d, 4) for d in range(4)]
    ys = [wrap(y + d, 4) for d in range(4)]
    zs = [wrap(z + d, 4) for d in range(4)]
    cs = [c, 1 - c]
    return [(xs[a] * 4 + zs[d], ys[b] * 2 + cs[e]) for a, b, d, e in offs]


def remote(src, dst, send, recv, a, b):
    return pltpu.make_async_remote_copy(
        src_ref=src, dst_ref=dst, send_sem=send, recv_sem=recv, device_id=(a, b), device_id_type=MESH
    )


def wait_bytes(ref, sem):
    pltpu.make_async_copy(ref, ref, sem).wait()


def slot(d, n, size=None):
    return pl.ds(pl.multiple_of(d * n, n), size or n)


def stencil(q, north, south, east, west, above, below, old, cpl, a0m, a0p, a1m, a1p, own, f):
    total = own * q[f] - old
    total += north * a0m - south * a0p
    total += east * a1m - west * a1p
    total -= 0.05 * (above + below)
    for g in range(4):
        total += cpl[f][g] * q[g]
    return total


def couplings(cp):
    return [[0.1 * cp[f, g] for g in range(4)] for f in range(4)]


PITCH = 24
USED = 19
KB = 0.02
KF = 0.02 * 9


def place_patches(off, pg, pxy):
    for g in range(NG):
        x = jnp.int32(0)
        y = jnp.int32(0)
        for p in range(NG):
            hit = pg[p] == g
            x = x + jnp.where(hit, off[0, p], 0)
            y = y + jnp.where(hit, off[1, p], 0)
        pxy[0, g] = x
        pxy[1, g] = y


def extract_base(r, c, pxy, base, trans, hr, hc, s1):
    flat = trans.reshape(2048, 128)
    for q in range(16):
        flat[pl.ds(q, 128, stride=16), :] = base[2 * q : 2 * q + 2].reshape(128, 128).T
    hr[0] = base[:, 0, :]
    hr[1] = base[:, BX - 1, :]
    hc[0] = trans[0]
    hc[1] = trans[127]

    def body(g, _):
        x = pxy[0, g]
        y = pxy[1, g]
        lo = x - 1 - r * BX
        hi = x + PC - r * BX
        loc = jnp.where((lo >= 0) & (lo < BX), lo, jnp.clip(hi, 0, BX - 1))
        s1[g, 0:32, :] = base[:, loc, :]
        y0 = jnp.clip(y - 1 - c * BY, 0, BY - 1)
        s1[g, 32:48, :] = trans[y0]
        y1 = jnp.clip(y + PC - c * BY, 0, BY - 1)
        s1[g, 48:64, :] = trans[y1]
        return 0

    lax.fori_loop(0, NG, body, 0)


def base_tendency(r, c, pxy, cpl, base, old, hrn, hcn, hz, ring, tend, d0, d1):
    keep = [
        jnp.where(r > 0, 1.0, 0.0),
        jnp.where(r < NG - 1, 1.0, 0.0),
        jnp.where(c > 0, 1.0, 0.0),
        jnp.where(c < NM - 1, 1.0, 0.0),
    ]
    hz[0] = hrn[0] * keep[0]
    hz[1] = hrn[1] * keep[1]
    zeros = jnp.zeros((112, 128), F32)
    westc = jnp.concatenate([hcn[0] * keep[2], zeros], axis=0).T
    eastc = jnp.concatenate([hcn[1] * keep[3], zeros], axis=0).T
    row = iota((BX, BY), 0)
    lane = iota((BX, BY), 1)
    open_ = ring_masks(r, c, pxy, ring)
    own = 1.0 + 4 * KB + 0.1
    acc = jnp.zeros((BX, BY), F32)
    for l in range(8):
        q = [base[f * 8 + l] for f in range(4)]
        a0 = 0.05 * q[0]
        a1 = 0.05 * q[1]
        for f in range(4):
            p = f * 8 + l
            pair, par = p // 2, p % 2
            north = jnp.where(row == BX - 1, hz[1, p : p + 1, :], pltpu.roll(q[f], BX - 1, 0))
            south = jnp.where(row == 0, hz[0, p : p + 1, :], pltpu.roll(q[f], 1, 0))
            ecol = pltpu.roll(eastc[par * 64 : par * 64 + 64], 127 - pair, 1)
            wcol = pltpu.roll(westc[par * 64 : par * 64 + 64], (128 - pair) % 128, 1)
            east = jnp.where(lane == BY - 1, ecol, pltpu.roll(q[f], BY - 1, 1))
            west = jnp.where(lane == 0, wcol, pltpu.roll(q[f], 1, 1))
            none = jnp.zeros((BX, BY), F32)
            above = base[p + 1] if l < 7 else none
            below = base[p - 1] if l > 0 else none
            total = stencil(
                q, north, south, east, west, above, below, old[p], cpl,
                a0 - KB, a0 + KB, a1 - KB, a1 + KB, own, f,
            )
            after = ring[1] * north
            before = ring[0] * south
            d0[p] = after - before
            both = after + before
            after = ring[3] * east
            before = ring[2] * west
            d1[p] = after - before
            tend[p] = open_ * total - (3 * KF / 9) * (both + after + before)
            acc = acc + open_ * (total * total)
    return acc.reshape(8, 8, 128).sum(axis=0)


def ring_masks(r, c, pxy, ring):
    row = iota((BX, BY), 0)
    lane = iota((BX, BY), 1)
    cells = jnp.ones((BX, BY), F32)
    sides = [jnp.zeros((BX, BY), F32)] * 4
    for g in range(NG):
        x = pxy[0, g] - r * BX
        y = pxy[1, g] - c * BY
        inside = (row >= x) & (row < x + PC) & (lane >= y) & (lane < y + PC)
        cells = jnp.where(inside, 0.0, cells)
        lines = (row == x, row == x + PC - 1, lane == y, lane == y + PC - 1)
        sides = [jnp.where(inside & line, 1.0, side) for line, side in zip(lines, sides)]
    for k in range(4):
        ring[k] = sides[k]
    return cells


def fine_interior(cpl, fine, old, pad, res):
    for f in range(4):
        pad[f * 10] = jnp.zeros((56, 384), F32)
        pad[f * 10 + 9] = jnp.zeros((56, 384), F32)

    def fill(p, _):
        dst = p + 2 * (p // 8) + 1
        pad[dst, 0:8, :] = jnp.zeros((8, 384), F32)
        pad[dst, 8 : 8 + FR, 0:256] = fine[p, :, 0:256]
        pad[dst, 8 : 8 + FR, 256:384] = jnp.concatenate([fine[p, :, 256:FC], jnp.zeros((FR, 120), F32)], axis=1)
        pad[dst, 8 + FR : 9 + FR, :] = jnp.zeros((1, 384), F32)
        return 0

    lax.fori_loop(0, 32, fill, 0)
    own = 1.0 + 4 * KF + 0.1

    def level(l, acc):
        for start, n in ((0, 8), (8, 8), (16, 8), (24, 8), (32, 1)):
            s = 8 + start
            q = [pad[f * 10 + 1 + l, s : s + n, :] for f in range(4)]
            a0 = 0.15 * q[0]
            a1 = 0.15 * q[1]
            keep = iota((n, 384), 1) < FC
            for f in range(4):
                z = f * 10 + 1 + l
                north = pad[z, s + 1 : s + 1 + n, :]
                south = pad[z, s - 1 : s - 1 + n, :]
                east = pltpu.roll(q[f], 383, 1)
                west = pltpu.roll(q[f], 1, 1)
                p = f * 8 + l
                before = old[p, start : start + n, :]
                before = jnp.concatenate([before, jnp.zeros((n, 384 - FC), F32)], axis=1)
                total = stencil(
                    q, north, south, east, west, pad[z + 1, s : s + n, :], pad[z - 1, s : s + n, :],
                    before, cpl, a0 - KF, a0 + KF, a1 - KF, a1 + KF, own, f,
                )
                total = jnp.where(keep, total, 0.0)
                for t in range(3):
                    part = total[:, 128 * t : 128 * t + 128]
                    res[pl.ds((t * 32 + p) * 40 + start, n), :] = part
                    sq = part * part
                    if n == 1:
                        sq = jnp.where(iota((8, 128), 0) == 0, jnp.broadcast_to(sq, (8, 128)), 0.0)
                    acc = acc + sq
        return acc

    return lax.fori_loop(0, 8, level, jnp.zeros((8, 128), F32))


def edge_columns(x, y, j, gr):
    first = lax.rem(x + 11 * j, BX)
    cl = jnp.maximum(y - 1, 0) // BY
    cr = (y + PC) // BY
    blank = jnp.zeros((96, 128), F32)
    va = jnp.concatenate([gr[cl, 0:16, :], gr[cr, 16:32, :], blank], axis=0)
    vb = jnp.concatenate([gr[cl, 32:48, :], gr[cr, 48:64, :], blank], axis=0)
    want = first + iota((40, 128), 0) // 3
    lane40 = iota((40, 128), 1)
    cols = []
    for par in range(2):
        at = lane40 - 64 * par
        good = (at >= 0) & (at < 64)
        pa = jnp.where(good & (at == want), 1.0, 0.0)
        pb = jnp.where(good & (at + 64 == want), 1.0, 0.0)
        dims = (((1,), (1,)), ((), ()))
        cols.append(
            lax.dot_general(pa, va, dims, precision=HI, preferred_element_type=F32)
            + lax.dot_general(pb, vb, dims, precision=HI, preferred_element_type=F32)
        )
    return cols


def edge_row(y, cells):
    c0 = y // BY
    c1 = jnp.minimum(c0 + 1, NM - 1)
    b = iota((128, 384), 0)
    jf = iota((128, 384), 1)
    cell = y + jf // 3 - c0 * BY
    good = jf < FC
    p0 = jnp.where(good & (b == cell), 1.0, 0.0)
    p1 = jnp.where(good & (b + BY == cell), 1.0, 0.0)
    return jnp.dot(cells[c0], p0, precision=HI, preferred_element_type=F32) + jnp.dot(
        cells[c1], p1, precision=HI, preferred_element_type=F32
    )


def fine_rows(hrow, fh, res):
    change = jnp.zeros((8, 128), F32)
    for t in range(3):
        for row, side in ((0, 0), (FR - 1, 1)):
            a0 = 0.15 * fh[side, 0:8, 128 * t : 128 * t + 128]
            factor = a0 - KF if side else -(a0 + KF)
            factor = jnp.concatenate([factor] * 4, axis=0)
            at = pl.ds(t * 32 * 40 + row, 32, stride=40)
            was = res[at, :]
            now = was + hrow[side, :, 128 * t : 128 * t + 128] * factor
            res[at, :] = now
            for f in range(4):
                change = change + (now[8 * f : 8 * f + 8] * now[8 * f : 8 * f + 8])
                change = change - (was[8 * f : 8 * f + 8] * was[8 * f : 8 * f + 8])
    return change


def fine_columns(cols, fine, res):
    change = jnp.zeros((8, 128), F32)
    lane = iota((FR, 128), 1)
    for l in range(8):
        q1 = fine[8 + l, :, 0:128]
        lo = -(0.15 * q1 + KF)
        q1 = jnp.concatenate([fine[8 + l, :, 256:FC], jnp.zeros((FR, 120), F32)], axis=1)
        hi = 0.15 * q1 - KF
        for f in range(4):
            p = f * 8 + l
            pair, par = p // 2, p % 2
            cv = cols[par][:FR]
            for t, factor, spot, turn in ((0, lo, 0, (128 - pair) % 128), (2, hi, 7, 119 - pair)):
                at = pl.ds((t * 32 + p) * 40, FR)
                was = res[at, :]
                now = jnp.where(lane == spot, was + pltpu.roll(cv, turn, 1) * factor, was)
                res[at, :] = now
                delta = now * now - was * was
                change = change + delta[0:8] + delta[8:16] + delta[16:24] + delta[24:32]
                change = change + jnp.where(iota((8, 128), 0) == 0, jnp.broadcast_to(delta[32:33], (8, 128)), 0.0)
    return change


def restrict(x, j, fine, fh, qs, res, mm, cells, ss):
    for t in range(3):
        mm[t, :, 8:16, :] = jnp.zeros((32, 8, 128), F32)

    def rows(pair, _):
        for par in range(2):
            for t in range(3):
                at = (t * 32 + 2 * pair + par) * 40
                part = [res[pl.ds(at + d, 11, stride=3), :] for d in range(3)]
                mm[t, par * 16 + pair, 0:11, :] = part[0] + part[1] + part[2]
        return 0

    lax.fori_loop(0, 16, rows, 0, unroll=2)
    total = 0.0
    ends = [0.0, 0.0]
    for t in range(3):
        comb = jnp.where((iota((128, 128), 0) + 128 * t) // 3 == iota((128, 128), 1), 1.0, 0.0)
        total = total + jnp.dot(mm[t].reshape(512, 128), comb, precision=HI, preferred_element_type=F32)
        for side in range(2):
            row = fh[side, 0:8, 128 * t : 128 * t + 128]
            ends[side] = ends[side] + jnp.dot(row, comb, precision=HI, preferred_element_type=F32)
    cells[...] = (total * (1.0 / 9.0)).reshape(32, 16, 128)
    for l in range(8):
        qs[pl.ds(l * 40, FR), :] = fine[8 + l, :, 0:128]
        qs[pl.ds((8 + l) * 40, FR), :] = jnp.concatenate([fine[8 + l, :, 256:FC], jnp.zeros((FR, 120), F32)], axis=1)
    lane = iota((11, 128), 1)
    for l in range(8):
        for side, turn in ((0, 88), (1, 81)):
            at = (side * 8 + l) * 40
            part = [qs[pl.ds(at + d, 11, stride=3), :] for d in range(3)]
            edge = pltpu.roll(part[0] + part[1] + part[2], turn, 1)
            cells[2 * l + side, 0:11, :] = jnp.where(lane == 88, edge, cells[2 * l + side, 0:11, :])
    for k in range(NM):
        first = lax.rem(k - x - 11 * j + 2048, 8)
        for par in range(2):
            for h in range(2):
                v = cells[pl.ds(par * 16, 16), first + 8 * h, :]
                ss[pl.ds(k * 8 + par * 2 + h, 16, stride=64), :] = v
        for side in range(2):
            ss[pl.ds((side * 8 + k) * 8 + 4, 8, stride=128), :] = ends[side]


def split3(v):
    hi = v.astype(jnp.bfloat16)
    rest = v - hi.astype(F32)
    mid = rest.astype(jnp.bfloat16)
    return hi, mid, (rest - mid.astype(F32)).astype(jnp.bfloat16)


def compose_send(gx, gy, pxy, rs, so, rolled, take, turned, r2, sems):
    n = iota((1, 256), 1)
    h = n // 128
    g = (n - h * 128) // 8
    k = n - (n // 8) * 8
    x = jnp.zeros((1, 256), jnp.int32)
    for i in range(NG):
        x = jnp.where(g == i, pxy[0, i], x)
    start = x + 11 * k
    away = gy - start + 2048
    row = away - (away // 8) * 8 + 8 * h
    octet = jnp.where(row <= 10, (start + row - gy) // 8, -1)
    take[...] = jnp.where(iota((128, 256), 0) == octet, 1.0, 0.0).astype(jnp.bfloat16)
    for i in range(NG):
        v = [rs[pl.ds(i * 64 + q, 8, stride=8), :] for q in range(4)]
        shift = jnp.broadcast_to(lax.rem(pxy[1, i], BY), (8, 128))
        for bit in range(7):
            shift, odd = shift // 2, shift - 2 * (shift // 2) == 1
            v = [jnp.where(odd, pltpu.roll(u, 1 << bit, 1), u) for u in v]
        for q in range(4):
            rolled[q, 8 * i : 8 * i + 8, :] = v[q]
    lane = iota((8, 128), 1)
    x4 = gx // 4
    z4 = gx - 4 * x4
    side = gx - 2 * (gx // 2)
    rank = iota((NG, 128), 0)
    yy = jnp.zeros((NG, 128), jnp.int32)
    for i in range(NG):
        yy = jnp.where(rank == i, pxy[1, i], yy)
    ends = rs[pl.ds(side * (NM - 1) * 8 + 4, NG, stride=64), :]
    shift = yy - (yy // BY) * BY
    for bit in range(7):
        shift, odd = shift // 2, shift - 2 * (shift // 2) == 1
        ends = jnp.where(odd, pltpu.roll(ends, 1 << bit, 1), ends)
    spots = []
    for i in range(NG):
        spots.append(jnp.where(lane == (pxy[1, i] + side * (PC - 1)) // 64, 1.0, 0.0))
    spots = jnp.concatenate(spots, axis=0)
    sums = []
    for h_ in range(2):
        v = rs[pl.ds(h_, 128, stride=8), :]
        sums.append(jnp.broadcast_to(v[:, 88:89], (128, 128)) * spots)
    b = jnp.concatenate(split3(jnp.concatenate(sums, axis=0)), axis=1)
    b = jnp.dot(take[...], b, preferred_element_type=F32)
    turned[...] = (b[:, 0:128] + (b[:, 128:256] + b[:, 256:384])).T

    def column(step, _):
        c = wrap(gy + step, NM)
        inside = []
        for i in range(NG):
            at = lane + c * BY - pxy[1, i]
            inside.append((at >= 0) & (at < PC))
        for par in range(2):
            rows = []
            for q in (2 * par, 2 * par + 1):
                for i in range(NG):
                    rows.append(jnp.where(inside[i], rolled[q, 8 * i : 8 * i + 8, :], 0.0))
            b = jnp.concatenate(split3(jnp.concatenate(rows, axis=0)), axis=1)
            got = jnp.dot(take[...], b, preferred_element_type=F32)
            got = got[:, 0:128] + (got[:, 128:256] + got[:, 256:384])
            for r in range(NG):
                at = pl.multiple_of((r * NM + c) * PITCH + 8 * par, 8)
                so[pl.ds(at, 8), :] = got[8 * r : 8 * r + 8]
        across = iota((NG, 128), 1) + c * BY - yy
        mine = jnp.where((across >= 0) & (across < PC), ends, 0.0)
        out = jnp.zeros((NG, 128), F32)
        for i in range(NG):
            line = pxy[0, i] + side * (PC - 1)
            hit = (rank == line // BX) & (line - (line // 8) * 8 == gy)
            out = jnp.where(hit, out + jnp.broadcast_to(mine[i : i + 1], (NG, 128)), out)
        so[pl.ds(c * PITCH + 16, NG, stride=NM * PITCH), :] = out
        for w in range(2):
            so[pl.ds(c * PITCH + 17 + w, NG, stride=NM * PITCH), :] = jnp.broadcast_to(
                turned[pl.ds(2 * c + w, 1), :], (NG, 128)
            )

        for dx, dz in GX_OFFSETS + ((0, 0),):
            a = wrap(x4 + dx, 4) * 4 + wrap(z4 + dz, 4)
            send = remote(
                so.at[slot(a * NM + c, PITCH, USED), :], r2.at[slot(gx * NM + gy, PITCH, USED), :],
                sems.at[0], sems.at[1], a, c,
            )
            if (dx, dz) == (0, 0):
                pl.when(step > 0)(send.start)
            else:
                send.start()
        return 0

    lax.fori_loop(0, NM, column, 0)


def main_kernel(
    off, pg, cp, base_h, old_h, fine_h, fold_h,
    tend_h, d0_h, d1_h, fout_h, norm_h, r2,
    pxy, base, old, fine, fold, tend, d0, d1, ring, trans, s1, hr, hc, fh, r1, hrn, hcn, fhn, gs, tb, gr, tr, br, hz,
    pad, hrow, res, mm, qs, cells, ss, rs, so, rolled, take, turned, nv, nr, fout,
    la, sa, sb, sc, sd, se, sf, lb, known,
):
    gx = lax.axis_index("gx")
    gy = lax.axis_index("gy")
    me = gx * NM + gy
    ga = gx_peers(gx)
    gb = gy_peers(gy)
    peers = all_peers(gx, gy)
    n = NG * NM - 1
    loads = [
        pltpu.make_async_copy(base_h, base, la.at[0]),
        pltpu.make_async_copy(fine_h.at[:, :, 0, :], fine, la.at[1]),
        pltpu.make_async_copy(fold_h.at[:, :, 0, :], fold, la.at[2]),
        pltpu.make_async_copy(old_h, old, la.at[3]),
    ]
    for load in loads:
        load.start()
    bar = pltpu.get_barrier_semaphore()
    for a in ga:
        pl.semaphore_signal(bar, inc=1, device_id=(a, gy), device_id_type=MESH)
    for b in gb:
        pl.semaphore_signal(bar, inc=1, device_id=(gx, b), device_id_type=MESH)
    cpl = couplings(cp)
    place_patches(off, pg, pxy)
    loads[0].wait()
    extract_base(gx, gy, pxy, base, trans, hr, hc, s1)
    loads[1].wait()
    blank = jnp.zeros((32, 384 - FC), F32)
    fh[0] = jnp.concatenate([fine[:, 0, :], blank], axis=1)
    fh[1] = jnp.concatenate([fine[:, FR - 1, :], blank], axis=1)
    own = pltpu.make_async_copy(s1.at[gx], r1.at[gx], lb.at[0])
    own.start()
    pl.semaphore_wait(bar, len(ga) + len(gb))
    for a in ga:
        pl.semaphore_signal(known, inc=1, device_id=(a, gy), device_id_type=MESH)

    up, down = wrap(gx + 1, NG), wrap(gx + NG - 1, NG)
    right, left = wrap(gy + 1, NM), wrap(gy + NM - 1, NM)
    halos = [
        remote(fh.at[1], fhn.at[0], sb.at[8], sb.at[9], gx, right),
        remote(fh.at[0], fhn.at[1], sb.at[10], sb.at[11], gx, left),
        remote(hr.at[1], hrn.at[0], sb.at[0], sb.at[1], up, gy),
        remote(hr.at[0], hrn.at[1], sb.at[2], sb.at[3], down, gy),
        remote(hc.at[1], hcn.at[0], sb.at[4], sb.at[5], gx, right),
        remote(hc.at[0], hcn.at[1], sb.at[6], sb.at[7], gx, left),
    ]
    for h in halos:
        h.start()
    for a in ga:
        remote(s1.at[a], r1.at[gx], sa.at[0], sa.at[1], a, gy).start()

    loads[2].wait()
    acc = fine_interior(cpl, fine, fold, pad, res)
    halos[0].wait()
    halos[1].wait()
    hrow[0] = fhn[0] * jnp.where(gy > 0, 1.0, 0.0)
    hrow[1] = fhn[1] * jnp.where(gy < NM - 1, 1.0, 0.0)
    acc = acc + fine_rows(hrow, fh, res)
    x = pxy[0, gx]
    y = pxy[1, gx]
    restrict(x, gy, fine, fh, qs, res, mm, cells, ss)
    rs[slot(me, 8), :] = ss[slot(me, 8), :]
    pl.semaphore_wait(known, len(ga))
    for a, b in peers:
        remote(ss.at[slot(a * NM + b, 8, 5), :], rs.at[slot(me, 8, 5), :], sd.at[0], sd.at[1], a, b).start()

    for h in halos[2:]:
        h.wait()
    loads[3].wait()
    bsum = base_tendency(gx, gy, pxy, cpl, base, old, hrn, hcn, hz, ring, tend, d0, d1)
    puts = [
        pltpu.make_async_copy(tend, tend_h, lb.at[3]),
        pltpu.make_async_copy(d0, d0_h, lb.at[4]),
        pltpu.make_async_copy(d1, d1_h, lb.at[5]),
        pltpu.make_async_copy(fout, fout_h, lb.at[6]),
        pltpu.make_async_copy(so.at[slot(me, PITCH), :], r2.at[slot(me, PITCH), :], lb.at[7]),
        pltpu.make_async_copy(nv, norm_h, lb.at[8]),
    ]
    for k in range(3):
        puts[k].start()

    own.wait()
    wait_bytes(r1.at[pl.ds(0, NG - 1)], sa.at[1])
    tb[0] = r1[jnp.maximum(x - 1, 0) // BX, 0:32, :]
    tb[1] = r1[(x + PC) // BX, 0:32, :]
    for j in range(NM):
        a = (x + 11 * j) // BX
        b = jnp.minimum(a + 1, NG - 1)
        gs[j, 0:32, :] = r1[a, 32:64, :]
        gs[j, 32:64, :] = r1[b, 32:64, :]
    for b in gb:
        remote(gs.at[b], gr.at[gy], sc.at[0], sc.at[1], gx, b).start()
    mine = pltpu.make_async_copy(gs.at[gy], gr.at[gy], lb.at[1])
    mine.start()
    ends = ((tr, 0, 0), (br, NM - 1, 1))
    for ref, target, k in ends:
        far = remote(tb.at[k], ref.at[gy], sc.at[2 + 2 * k], sc.at[3 + 2 * k], gx, target)
        near = pltpu.make_async_copy(tb.at[k], ref.at[gy], lb.at[2])

        @pl.when(gy != target)
        def _():
            far.start()

        @pl.when(gy == target)
        def _():
            near.start()

    wait_bytes(rs.at[pl.ds(0, 5 * n), :], sd.at[1])
    compose_send(gx, gy, pxy, rs, so, rolled, take, turned, r2, se)
    puts[4].start()

    mine.wait()
    wait_bytes(gr.at[pl.ds(0, NM - 1)], sc.at[1])
    hrow[...] = jnp.zeros((2, 32, 384), F32)
    for ref, target, k in ends:
        far = remote(tb.at[k], ref.at[gy], sc.at[2 + 2 * k], sc.at[3 + 2 * k], gx, target)
        near = pltpu.make_async_copy(tb.at[k], ref.at[gy], lb.at[2])

        @pl.when(gy != target)
        def _():
            far.wait_send()

        @pl.when(gy == target)
        def _():
            near.wait()
            wait_bytes(ref.at[pl.ds(0, NM - 1)], sc.at[3 + 2 * k])
            hrow[k] = edge_row(y, ref)

    cols = edge_columns(x, y, gy, gr)
    acc = acc + fine_rows(hrow, fh, res)
    acc = acc + fine_columns(cols, fine, res)
    norm = jnp.sum(bsum + acc * (1.0 / 9.0), axis=(0, 1), keepdims=True)
    nv[...] = jnp.broadcast_to(norm, (8, 128))
    nr[slot(me, 8), :] = jnp.broadcast_to(norm, (8, 128))
    for a, b in peers:
        remote(nv.at[pl.ds(0, 1), :], nr.at[slot(me, 8, 1), :], sf.at[0], sf.at[1], a, b).start()

    def write(p, _):
        for t in range(2):
            fout[p, :, 128 * t : 128 * t + 128] = res[pl.ds((t * 32 + p) * 40, FR), :]
        fout[p, :, 256:FC] = res[pl.ds((64 + p) * 40, FR), :][:, 0 : FC - 256]
        return 0

    lax.fori_loop(0, 32, write, 0)
    puts[3].start()
    wait_bytes(nr.at[pl.ds(0, n), :], sf.at[1])
    wait_bytes(nr.at[pl.ds(0, n), :], sf.at[0])
    total = jnp.sum(nr[pl.ds(0, 128, stride=8), :], axis=0, keepdims=True)
    nv[...] = jnp.broadcast_to(jnp.sqrt(total), (8, 128))
    puts[5].start()
    for put in puts:
        put.wait()
    wait_bytes(r1.at[pl.ds(0, NG - 1)], sa.at[0])
    wait_bytes(gr.at[pl.ds(0, NM - 1)], sc.at[0])
    wait_bytes(rs.at[pl.ds(0, 5 * n), :], sd.at[0])
    wait_bytes(so.at[pl.ds(0, USED * n), :], se.at[0])
    wait_bytes(so.at[pl.ds(0, USED * n), :], se.at[1])


def main(off, pg, cp, base, old, fine, fold):
    hbm = pl.BlockSpec(memory_space=pl.ANY)
    dma = pltpu.SemaphoreType.DMA
    return pl.pallas_call(
        main_kernel,
        out_shape=(shape(32, BX, BY),) * 3 + (shape(32, FR, FC), shape(8, 128), shape(NG * NM * PITCH, 128)),
        in_specs=[sspec()] * 3 + [hbm] * 4,
        out_specs=(hbm,) * 6,
        scratch_shapes=[
            pltpu.SMEM((2, NG), jnp.int32),
            VM((32, BX, BY), F32),
            VM((32, BX, BY), F32),
            VM((32, FR, FC), F32),
            VM((32, FR, FC), F32),
            VM((32, BX, BY), F32),
            VM((32, BX, BY), F32),
            VM((32, BX, BY), F32),
            VM((4, BX, BY), F32),
            VM((128, 16, 128), F32),
            VM((NG, 64, 128), F32),
            VM((2, 32, 128), F32),
            VM((2, 16, 128), F32),
            VM((2, 32, 384), F32),
            VM((NG, 64, 128), F32),
            VM((2, 32, 128), F32),
            VM((2, 16, 128), F32),
            VM((2, 32, 384), F32),
            VM((NM, 64, 128), F32),
            VM((2, 32, 128), F32),
            VM((NM, 64, 128), F32),
            VM((NM, 32, 128), F32),
            VM((NM, 32, 128), F32),
            VM((2, 32, 128), F32),
            VM((40, 56, 384), F32),
            VM((2, 32, 384), F32),
            VM((3 * 32 * 40, 128), F32),
            VM((3, 32, 16, 128), F32),
            VM((16 * 40, 128), F32),
            VM((32, 16, 128), F32),
            VM((1024, 128), F32),
            VM((1024, 128), F32),
            VM((NG * NM * PITCH, 128), F32),
            VM((4, 128, 128), F32),
            VM((128, 256), jnp.bfloat16),
            VM((128, 128), F32),
            VM((8, 128), F32),
            VM((1024, 128), F32),
            VM((32, FR, FC), F32),
            dma((4,)),
            dma((2,)),
            dma((12,)),
            dma((6,)),
            dma((2,)),
            dma((2,)),
            dma((2,)),
            dma((9,)),
            pltpu.SemaphoreType.REGULAR,
        ],
        compiler_params=pltpu.CompilerParams(collective_id=0, has_side_effects=True),
    )(off, pg, cp, base, old, fine, fold)


PARTS = 4


def merge_kernel(off, tend_h, d0_h, d1_h, r2, fout, nv, out_h, fres, norm, tend, d0, d1, ri, fine, sem):
    r = lax.axis_index("gx")
    c = lax.axis_index("gy")
    slots = [pl.ds(128 // PARTS * k, 128 // PARTS) for k in range(PARTS)]
    levels = 8 // PARTS

    def copies(pairs, at):
        return [[pltpu.make_async_copy(a, b, sem.at[at + k]) for a, b in pairs(k)] for k in range(PARTS)]

    def planes(k):
        return [pl.ds(8 * f + levels * k, levels) for f in range(4)]

    piece = 32 // PARTS
    here = [pl.ds(piece * k, piece) for k in range(PARTS)]
    got = [pltpu.make_async_copy(r2, ri, sem.at[0])]
    had = [
        [pltpu.make_async_copy(a.at[s], b.at[s], sem.at[1 + k]) for a, b in ((tend_h, tend), (d0_h, d0), (d1_h, d1)) for s in planes(k)]
        for k in range(PARTS)
    ]
    give = [[pltpu.make_async_copy(tend.at[s], out_h.at[s], sem.at[1 + PARTS + k]) for s in planes(k)] for k in range(PARTS)]
    take = [pltpu.make_async_copy(fout.at[here[k]], fine.at[here[k]], sem.at[1 + 2 * PARTS + k]) for k in range(PARTS)]
    put = [pltpu.make_async_copy(fine.at[here[k]], fres.at[here[k], :, 0, :], sem.at[1 + 3 * PARTS + k]) for k in range(PARTS)]
    got[0].start()
    for k in range(PARTS):
        for copy in had[k]:
            copy.start()
    for k in range(PARTS):
        take[k].start()
    row = iota((8, BY), 0)
    lane = iota((8, BY), 1)
    last = [jnp.zeros((8, BY), F32) for t in range(8)]
    east = [jnp.zeros((8, BY), F32) for t in range(8)]
    for g in range(NG):
        x = off[0, g] - r * BX
        y = off[1, g] - c * BY
        across = (lane >= y) & (lane < y + PC)
        edge = lane == y + PC - 1
        for t in range(8):
            last[t] = jnp.where((row + 8 * t == x + PC - 1) & across, 1.0, last[t])
            east[t] = jnp.where((row + 8 * t >= x) & (row + 8 * t < x + PC) & edge, 1.0, east[t])
    norm[...] = nv[0:1, 0:1]
    flat = ri.reshape(128 * PITCH, 128)
    got[0].wait()
    for k in range(PARTS):
        for copy in had[k]:
            copy.wait()
        for l in range(levels * k, levels * k + levels):
            ends = []
            turn = []
            for side in range(2):
                at = (2 * l + side) * 8 * PITCH + 16
                ends.append(flat[pl.ds(at, 8, stride=PITCH), :])
                turn.append([pltpu.roll(flat[pl.ds(at + 1 + w, 8, stride=PITCH), :], 128 - 8 * r, 1) for w in range(2)])
            for t in range(8):
                tile = slice(8 * t, 8 * t + 8)
                e0 = jnp.where(last[t] > 0.5, ends[1], ends[0])
                e1 = [
                    jnp.where(lane < 64, *[jnp.broadcast_to(turn[side][w][:, t : t + 1], (8, 128)) for w in range(2)])
                    for side in range(2)
                ]
                e1 = jnp.where(east[t] > 0.5, e1[1], e1[0])
                for f in range(4):
                    p = 8 * f + l
                    new = flat[pl.ds((p // 2) * 8 * PITCH + (p % 2) * 8 + t, 8, stride=PITCH), :]
                    edge = e0 * d0[p, tile, :] + e1 * d1[p, tile, :]
                    tend[p, tile, :] = tend[p, tile, :] + new + (0.15 / 9) * edge
        for copy in give[k]:
            copy.start()
        take[k].wait()
        put[k].start()
    for k in range(PARTS):
        for copy in give[k]:
            copy.wait()
        put[k].wait()


def merge(off, tend, d0, d1, ri, fout, nv):
    hbm = pl.BlockSpec(memory_space=pl.ANY)
    return pl.pallas_call(
        merge_kernel,
        out_shape=(shape(32, BX, BY), shape(32, FR, 1, FC), shape(1, 1)),
        in_specs=[sspec()] + [hbm] * 5 + [vspec()],
        out_specs=(hbm, hbm, vspec()),
        scratch_shapes=[
            VM((32, BX, BY), F32),
            VM((32, BX, BY), F32),
            VM((32, BX, BY), F32),
            VM((NG * NM, PITCH, 128), F32),
            VM((32, FR, FC), F32),
            pltpu.SemaphoreType.DMA((1 + 4 * PARTS,)),
        ],
    )(off, tend, d0, d1, ri.reshape(NG * NM, PITCH, 128), fout, nv)


def local(base_state, base_old, fine_state, fine_old, coupling, patch_offsets, patch_group):
    base = base_state.reshape(32, BX, BY)
    old = base_old.reshape(32, BX, BY)
    fine = fine_state.reshape(32, FR, 1, FC)
    fold = fine_old.reshape(32, FR, 1, FC)
    off = patch_offsets.T
    tend, d0, d1, fout, nv, r2 = main(off, patch_group, coupling, base, old, fine, fold)
    bout, fres, norm = merge(off, tend, d0, d1, r2, fout, nv)
    return (
        bout.reshape(4, 8, BX, BY),
        fres.reshape(4, 8, 1, FR, FC),
        norm.reshape(()),
    )


def solution(mesh):
    placed = (
        P(None, None, "gx", "gy"),
        P(None, None, "gx", "gy"),
        P(None, None, "gx", "gy", None),
        P(None, None, "gx", "gy", None),
        P(),
        P(),
        P(),
    )
    return jax.shard_map(
        local,
        mesh=mesh,
        in_specs=placed,
        out_specs=(P(None, None, "gx", "gy"), P(None, None, "gx", "gy", None), P()),
        check_vma=False,
    )
```

```python
import functools

import jax
import jax.numpy as jnp
from jax import lax
from jax.experimental import pallas as pl
from jax.experimental.pallas import tpu as pltpu
from jax.sharding import PartitionSpec as P

PC = 88
NG, NM = 16, 8
BX, BY = 64, 128
FR, FC = 33, 264
MESH = pl.DeviceIdType.MESH
VM = pltpu.VMEM
F32 = jnp.float32
HI = lax.Precision.HIGHEST


def vspec():
    return pl.BlockSpec(memory_space=pltpu.VMEM)


def sspec():
    return pl.BlockSpec(memory_space=pltpu.SMEM)


def shape(*dims):
    return jax.ShapeDtypeStruct(dims, F32)


def iota(dims, axis):
    return lax.broadcasted_iota(jnp.int32, dims, axis)


def wrap(v, n):
    return jnp.where(v >= n, v - n, v)


def gx_peers(gx):
    x = gx // 4
    z = gx - 4 * x
    out = []
    for dx, dz in GX_OFFSETS:
        out.append(wrap(x + dx, 4) * 4 + wrap(z + dz, 4))
    return out


GX_OFFSETS = (
    (2, 2), (1, 2), (2, 1), (3, 2), (2, 3), (1, 1), (3, 3), (1, 3), (3, 1), (2, 0), (0, 2), (1, 0), (0, 1), (3, 0), (0, 3),
)


def gy_peers(gy):
    return [wrap(gy + d, NM) for d in range(1, NM)]


def all_peers(gx, gy):
    x = gx // 4
    z = gx - 4 * x
    y = gy // 2
    c = gy - 2 * y
    offs = [(a, b, d, e) for a in range(4) for b in range(4) for d in range(4) for e in range(2)][1:]
    offs.sort(key=lambda o: -sum(min(v, 4 - v) for v in o[:3]))
    xs = [wrap(x + d, 4) for d in range(4)]
    ys = [wrap(y + d, 4) for d in range(4)]
    zs = [wrap(z + d, 4) for d in range(4)]
    cs = [c, 1 - c]
    return [(xs[a] * 4 + zs[d], ys[b] * 2 + cs[e]) for a, b, d, e in offs]


def remote(src, dst, send, recv, a, b):
    return pltpu.make_async_remote_copy(
        src_ref=src, dst_ref=dst, send_sem=send, recv_sem=recv, device_id=(a, b), device_id_type=MESH
    )


def wait_bytes(ref, sem):
    pltpu.make_async_copy(ref, ref, sem).wait()


def slot(d, n, size=None):
    return pl.ds(pl.multiple_of(d * n, n), size or n)


def stencil(q, north, south, east, west, above, below, old, cpl, a0m, a0p, a1m, a1p, own, f):
    total = own * q[f] - old
    total += north * a0m - south * a0p
    total += east * a1m - west * a1p
    total -= 0.05 * (above + below)
    for g in range(4):
        total += cpl[f][g] * q[g]
    return total


def couplings(cp):
    return [[0.1 * cp[f, g] for g in range(4)] for f in range(4)]


PITCH = 24
USED = 18
EARLY = 0
HALF = 4
KB = 0.02
KF = 0.02 * 9


def place_patches(off, pg, pxy):
    for g in range(NG):
        x = jnp.int32(0)
        y = jnp.int32(0)
        for p in range(NG):
            hit = pg[p] == g
            x = x + jnp.where(hit, off[0, p], 0)
            y = y + jnp.where(hit, off[1, p], 0)
        pxy[0, g] = x
        pxy[1, g] = y


def extract_base(r, c, pxy, base, trans, hr, hc, s1):
    flat = trans.reshape(2048, 128)
    for q in range(16):
        flat[pl.ds(q, 128, stride=16), :] = base[2 * q : 2 * q + 2].reshape(128, 128).T
    hr[0] = base[:, 0, :]
    hr[1] = base[:, BX - 1, :]
    hc[0] = trans[0]
    hc[1] = trans[127]

    def body(g, _):
        x = pxy[0, g]
        y = pxy[1, g]
        lo = x - 1 - r * BX
        hi = x + PC - r * BX
        loc = jnp.where((lo >= 0) & (lo < BX), lo, jnp.clip(hi, 0, BX - 1))
        s1[g, 0:32, :] = base[:, loc, :]
        y0 = jnp.clip(y - 1 - c * BY, 0, BY - 1)
        s1[g, 32:48, :] = trans[y0]
        y1 = jnp.clip(y + PC - c * BY, 0, BY - 1)
        s1[g, 48:64, :] = trans[y1]
        return 0

    lax.fori_loop(0, NG, body, 0)


def base_tendency(r, c, pxy, cpl, base, old, hrn, hcn, hz, ring, tend, d0, d1):
    keep = [
        jnp.where(r > 0, 1.0, 0.0),
        jnp.where(r < NG - 1, 1.0, 0.0),
        jnp.where(c > 0, 1.0, 0.0),
        jnp.where(c < NM - 1, 1.0, 0.0),
    ]
    hz[0] = hrn[0] * keep[0]
    hz[1] = hrn[1] * keep[1]
    zeros = jnp.zeros((112, 128), F32)
    westc = jnp.concatenate([hcn[0] * keep[2], zeros], axis=0).T
    eastc = jnp.concatenate([hcn[1] * keep[3], zeros], axis=0).T
    row = iota((BX, BY), 0)
    lane = iota((BX, BY), 1)
    open_ = ring_masks(r, c, pxy, ring)
    own = 1.0 + 4 * KB + 0.1
    acc = jnp.zeros((BX, BY), F32)
    for l in range(8):
        q = [base[f * 8 + l] for f in range(4)]
        a0 = 0.05 * q[0]
        a1 = 0.05 * q[1]
        for f in range(4):
            p = f * 8 + l
            pair, par = p // 2, p % 2
            north = jnp.where(row == BX - 1, hz[1, p : p + 1, :], pltpu.roll(q[f], BX - 1, 0))
            south = jnp.where(row == 0, hz[0, p : p + 1, :], pltpu.roll(q[f], 1, 0))
            ecol = pltpu.roll(eastc[par * 64 : par * 64 + 64], 127 - pair, 1)
            wcol = pltpu.roll(westc[par * 64 : par * 64 + 64], (128 - pair) % 128, 1)
            east = jnp.where(lane == BY - 1, ecol, pltpu.roll(q[f], BY - 1, 1))
            west = jnp.where(lane == 0, wcol, pltpu.roll(q[f], 1, 1))
            none = jnp.zeros((BX, BY), F32)
            above = base[p + 1] if l < 7 else none
            below = base[p - 1] if l > 0 else none
            total = stencil(
                q, north, south, east, west, above, below, old[p], cpl,
                a0 - KB, a0 + KB, a1 - KB, a1 + KB, own, f,
            )
            after = ring[1] * north
            before = ring[0] * south
            d0[p] = after - before
            both = after + before
            after = ring[3] * east
            before = ring[2] * west
            d1[p] = after - before
            tend[p] = open_ * total - (3 * KF / 9) * (both + after + before)
            acc = acc + open_ * (total * total)
    return acc.reshape(8, 8, 128).sum(axis=0)


def ring_masks(r, c, pxy, ring):
    row = iota((BX, BY), 0)
    lane = iota((BX, BY), 1)
    cells = jnp.ones((BX, BY), F32)
    sides = [jnp.zeros((BX, BY), F32)] * 4
    for g in range(NG):
        x = pxy[0, g] - r * BX
        y = pxy[1, g] - c * BY
        inside = (row >= x) & (row < x + PC) & (lane >= y) & (lane < y + PC)
        cells = jnp.where(inside, 0.0, cells)
        lines = (row == x, row == x + PC - 1, lane == y, lane == y + PC - 1)
        sides = [jnp.where(inside & line, 1.0, side) for line, side in zip(lines, sides)]
    for k in range(4):
        ring[k] = sides[k]
    return cells


def fine_fill(fine, pad):
    for f in range(4):
        pad[f * 10] = jnp.zeros((56, 384), F32)
        pad[f * 10 + 9] = jnp.zeros((56, 384), F32)

    def fill(p, _):
        dst = p + 2 * (p // 8) + 1
        pad[dst, 0:8, :] = jnp.zeros((8, 384), F32)
        pad[dst, 8 : 8 + FR, 0:256] = fine[p, :, 0:256]
        pad[dst, 8 : 8 + FR, 256:384] = jnp.concatenate([fine[p, :, 256:FC], jnp.zeros((FR, 120), F32)], axis=1)
        pad[dst, 8 + FR : 9 + FR, :] = jnp.zeros((1, 384), F32)
        return 0

    lax.fori_loop(0, 32, fill, 0)


def fine_levels(first, stop, acc, cpl, old, pad, res):
    own = 1.0 + 4 * KF + 0.1

    def level(l, acc):
        for start, n in ((0, 8), (8, 8), (16, 8), (24, 8), (32, 1)):
            s = 8 + start
            q = [pad[f * 10 + 1 + l, s : s + n, :] for f in range(4)]
            a0 = 0.15 * q[0]
            a1 = 0.15 * q[1]
            keep = iota((n, 384), 1) < FC
            for f in range(4):
                z = f * 10 + 1 + l
                north = pad[z, s + 1 : s + 1 + n, :]
                south = pad[z, s - 1 : s - 1 + n, :]
                east = pltpu.roll(q[f], 383, 1)
                west = pltpu.roll(q[f], 1, 1)
                p = f * 8 + l
                before = old[p, start : start + n, :]
                before = jnp.concatenate([before, jnp.zeros((n, 384 - FC), F32)], axis=1)
                total = stencil(
                    q, north, south, east, west, pad[z + 1, s : s + n, :], pad[z - 1, s : s + n, :],
                    before, cpl, a0 - KF, a0 + KF, a1 - KF, a1 + KF, own, f,
                )
                total = jnp.where(keep, total, 0.0)
                for t in range(3):
                    part = total[:, 128 * t : 128 * t + 128]
                    res[pl.ds((t * 32 + p) * 40 + start, n), :] = part
                    sq = part * part
                    if n == 1:
                        sq = jnp.where(iota((8, 128), 0) == 0, jnp.broadcast_to(sq, (8, 128)), 0.0)
                    acc = acc + sq
        return acc

    return lax.fori_loop(first, stop, level, acc)


def edge_columns(x, y, j, gr):
    first = lax.rem(x + 11 * j, BX)
    cl = jnp.maximum(y - 1, 0) // BY
    cr = (y + PC) // BY
    blank = jnp.zeros((96, 128), F32)
    va = jnp.concatenate([gr[cl, 0:16, :], gr[cr, 16:32, :], blank], axis=0)
    vb = jnp.concatenate([gr[cl, 32:48, :], gr[cr, 48:64, :], blank], axis=0)
    want = first + iota((40, 128), 0) // 3
    lane40 = iota((40, 128), 1)
    cols = []
    for par in range(2):
        at = lane40 - 64 * par
        good = (at >= 0) & (at < 64)
        pa = jnp.where(good & (at == want), 1.0, 0.0)
        pb = jnp.where(good & (at + 64 == want), 1.0, 0.0)
        dims = (((1,), (1,)), ((), ()))
        cols.append(
            lax.dot_general(pa, va, dims, precision=HI, preferred_element_type=F32)
            + lax.dot_general(pb, vb, dims, precision=HI, preferred_element_type=F32)
        )
    return cols


def edge_row(y, cells):
    c0 = y // BY
    c1 = jnp.minimum(c0 + 1, NM - 1)
    b = iota((128, 384), 0)
    jf = iota((128, 384), 1)
    cell = y + jf // 3 - c0 * BY
    good = jf < FC
    p0 = jnp.where(good & (b == cell), 1.0, 0.0)
    p1 = jnp.where(good & (b + BY == cell), 1.0, 0.0)
    return jnp.dot(cells[c0], p0, precision=HI, preferred_element_type=F32) + jnp.dot(
        cells[c1], p1, precision=HI, preferred_element_type=F32
    )


def fine_rows(hrow, fh, res):
    change = jnp.zeros((8, 128), F32)
    for t in range(3):
        for row, side in ((0, 0), (FR - 1, 1)):
            a0 = 0.15 * fh[side, 0:8, 128 * t : 128 * t + 128]
            factor = a0 - KF if side else -(a0 + KF)
            factor = jnp.concatenate([factor] * 4, axis=0)
            at = pl.ds(t * 32 * 40 + row, 32, stride=40)
            was = res[at, :]
            now = was + hrow[side, :, 128 * t : 128 * t + 128] * factor
            res[at, :] = now
            for f in range(4):
                change = change + (now[8 * f : 8 * f + 8] * now[8 * f : 8 * f + 8])
                change = change - (was[8 * f : 8 * f + 8] * was[8 * f : 8 * f + 8])
    return change


def fine_columns(cols, fine, res):
    change = jnp.zeros((8, 128), F32)
    lane = iota((FR, 128), 1)
    for l in range(8):
        q1 = fine[8 + l, :, 0:128]
        lo = -(0.15 * q1 + KF)
        q1 = jnp.concatenate([fine[8 + l, :, 256:FC], jnp.zeros((FR, 120), F32)], axis=1)
        hi = 0.15 * q1 - KF
        for f in range(4):
            p = f * 8 + l
            pair, par = p // 2, p % 2
            cv = cols[par][:FR]
            for t, factor, spot, turn in ((0, lo, 0, (128 - pair) % 128), (2, hi, 7, 119 - pair)):
                at = pl.ds((t * 32 + p) * 40, FR)
                was = res[at, :]
                now = jnp.where(lane == spot, was + pltpu.roll(cv, turn, 1) * factor, was)
                res[at, :] = now
                delta = now * now - was * was
                change = change + delta[0:8] + delta[8:16] + delta[16:24] + delta[24:32]
                change = change + jnp.where(iota((8, 128), 0) == 0, jnp.broadcast_to(delta[32:33], (8, 128)), 0.0)
    return change


def restrict(x, j, fine, fh, qs, res, mm, cells, ss):
    for t in range(3):
        mm[t, :, 8:16, :] = jnp.zeros((32, 8, 128), F32)

    def rows(pair, _):
        for par in range(2):
            for t in range(3):
                at = (t * 32 + 2 * pair + par) * 40
                part = [res[pl.ds(at + d, 11, stride=3), :] for d in range(3)]
                mm[t, par * 16 + pair, 0:11, :] = part[0] + part[1] + part[2]
        return 0

    lax.fori_loop(0, 16, rows, 0, unroll=2)
    total = 0.0
    ends = [0.0, 0.0]
    for t in range(3):
        comb = jnp.where((iota((128, 128), 0) + 128 * t) // 3 == iota((128, 128), 1), 1.0, 0.0)
        total = total + jnp.dot(mm[t].reshape(512, 128), comb, precision=HI, preferred_element_type=F32)
        for side in range(2):
            row = fh[side, 0:8, 128 * t : 128 * t + 128]
            ends[side] = ends[side] + jnp.dot(row, comb, precision=HI, preferred_element_type=F32)
    cells[...] = (total * (1.0 / 9.0)).reshape(32, 16, 128)
    for l in range(8):
        qs[pl.ds(l * 40, FR), :] = fine[8 + l, :, 0:128]
        qs[pl.ds((8 + l) * 40, FR), :] = jnp.concatenate([fine[8 + l, :, 256:FC], jnp.zeros((FR, 120), F32)], axis=1)
    lane = iota((11, 128), 1)
    for l in range(8):
        for side, turn in ((0, 88), (1, 81)):
            at = (side * 8 + l) * 40
            part = [qs[pl.ds(at + d, 11, stride=3), :] for d in range(3)]
            edge = pltpu.roll(part[0] + part[1] + part[2], turn, 1)
            cells[2 * l + side, 0:11, :] = jnp.where(lane == 88, edge, cells[2 * l + side, 0:11, :])
    for k in range(NM):
        first = lax.rem(k - x - 11 * j + 2048, 8)
        for par in range(2):
            for h in range(2):
                v = cells[pl.ds(par * 16, 16), first + 8 * h, :]
                ss[pl.ds(k * 8 + par * 2 + h, 16, stride=64), :] = v
        for side in range(2):
            ss[pl.ds((side * 8 + k) * 8 + 4, 8, stride=128), :] = ends[side]


def split3(v):
    hi = v.astype(jnp.bfloat16)
    rest = v - hi.astype(F32)
    mid = rest.astype(jnp.bfloat16)
    return hi, mid, (rest - mid.astype(F32)).astype(jnp.bfloat16)


def compose_rows(gy, pxy, take):
    n = iota((1, 256), 1)
    h = n // 128
    g = (n - h * 128) // 8
    k = n - (n // 8) * 8
    x = jnp.zeros((1, 256), jnp.int32)
    for i in range(NG):
        x = jnp.where(g == i, pxy[0, i], x)
    start = x + 11 * k
    away = gy - start + 2048
    row = away - (away // 8) * 8 + 8 * h
    octet = jnp.where(row <= 10, (start + row - gy) // 8, -1)
    take[...] = jnp.where(iota((128, 256), 0) == octet, 1.0, 0.0).astype(jnp.bfloat16)


def compose_prepare(gx, pxy, rs, rolled, take, turned, lines):
    for i in range(NG):
        v = [rs[pl.ds(i * 64 + q, 8, stride=8), :] for q in range(4)]
        shift = jnp.broadcast_to(lax.rem(pxy[1, i], BY), (8, 128))
        for bit in range(7):
            shift, odd = shift // 2, shift - 2 * (shift // 2) == 1
            v = [jnp.where(odd, pltpu.roll(u, 1 << bit, 1), u) for u in v]
        for q in range(4):
            rolled[q, 8 * i : 8 * i + 8, :] = v[q]
    lane = iota((8, 128), 1)
    side = gx - 2 * (gx // 2)
    rank = iota((NG, 128), 0)
    yy = jnp.zeros((NG, 128), jnp.int32)
    for i in range(NG):
        yy = jnp.where(rank == i, pxy[1, i], yy)
    ends = rs[pl.ds(side * (NM - 1) * 8 + 4, NG, stride=64), :]
    shift = yy - (yy // BY) * BY
    for bit in range(7):
        shift, odd = shift // 2, shift - 2 * (shift // 2) == 1
        ends = jnp.where(odd, pltpu.roll(ends, 1 << bit, 1), ends)
    lines[...] = ends
    spots = []
    for i in range(NG):
        spots.append(jnp.where(lane == (pxy[1, i] + side * (PC - 1)) // 64, 1.0, 0.0))
    spots = jnp.concatenate(spots, axis=0)
    sums = []
    for h_ in range(2):
        v = rs[pl.ds(h_, 128, stride=8), :]
        sums.append(jnp.broadcast_to(v[:, 88:89], (128, 128)) * spots)
    b = jnp.concatenate(split3(jnp.concatenate(sums, axis=0)), axis=1)
    b = jnp.dot(take[...], b, preferred_element_type=F32)
    turned[...] = (b[:, 0:128] + (b[:, 128:256] + b[:, 256:384])).T


def compose_send(first, stop, gx, gy, pxy, so, rolled, take, turned, lines, r2, sems):
    lane = iota((8, 128), 1)
    side = gx - 2 * (gx // 2)
    rank = iota((NG, 128), 0)
    yy = jnp.zeros((NG, 128), jnp.int32)
    for i in range(NG):
        yy = jnp.where(rank == i, pxy[1, i], yy)
    ends = lines[...]
    x4 = gx // 4
    z4 = gx - 4 * x4
    def column(step, _):
        c = wrap(gy + step, NM)
        inside = []
        for i in range(NG):
            at = lane + c * BY - pxy[1, i]
            inside.append((at >= 0) & (at < PC))
        for par in range(2):
            rows = []
            for q in (2 * par, 2 * par + 1):
                for i in range(NG):
                    rows.append(jnp.where(inside[i], rolled[q, 8 * i : 8 * i + 8, :], 0.0))
            b = jnp.concatenate(split3(jnp.concatenate(rows, axis=0)), axis=1)
            got = jnp.dot(take[...], b, preferred_element_type=F32)
            got = got[:, 0:128] + (got[:, 128:256] + got[:, 256:384])
            for r in range(NG):
                at = pl.multiple_of((r * NM + c) * PITCH + 8 * par, 8)
                so[pl.ds(at, 8), :] = got[8 * r : 8 * r + 8]
        across = iota((NG, 128), 1) + c * BY - yy
        mine = jnp.where((across >= 0) & (across < PC), ends, 0.0)
        out = jnp.zeros((NG, 128), F32)
        for i in range(NG):
            line = pxy[0, i] + side * (PC - 1)
            hit = (rank == line // BX) & (line - (line // 8) * 8 == gy)
            out = jnp.where(hit, out + jnp.broadcast_to(mine[i : i + 1], (NG, 128)), out)
        so[pl.ds(c * PITCH + 16, NG, stride=NM * PITCH), :] = out
        octet = iota((NG, 128), 1) // 8
        low = jnp.broadcast_to(turned[pl.ds(2 * c, 1), :], (NG, 128))
        high = jnp.broadcast_to(pltpu.roll(turned[pl.ds(2 * c + 1, 1), :], 64, 1), (NG, 128))
        so[pl.ds(c * PITCH + 17, NG, stride=NM * PITCH), :] = jnp.where(octet == rank, low, high)

        for dx, dz in GX_OFFSETS + ((0, 0),):
            a = wrap(x4 + dx, 4) * 4 + wrap(z4 + dz, 4)
            send = remote(
                so.at[slot(a * NM + c, PITCH, USED), :], r2.at[slot(gx * NM + gy, PITCH, USED), :],
                sems.at[0], sems.at[1], a, c,
            )
            if (dx, dz) == (0, 0):
                pl.when(step > 0)(send.start)
            else:
                send.start()
        return 0

    lax.fori_loop(first, stop, column, 0)


def main_kernel(
    off, pg, cp, base_h, old_h, fine_h, fold_h,
    tend_h, d0_h, d1_h, fout_h, norm_h, r2,
    pxy, base, old, fine, fold, tend, d0, d1, ring, trans, s1, hr, hc, fh, r1, hrn, hcn, fhn, gs, tb, gr, tr, br, hz,
    pad, hrow, res, mm, qs, cells, ss, rs, so, rolled, take, turned, lines, nv, nr, fout,
    la, sa, sb, sc, sd, se, sf, lb, known,
):
    gx = lax.axis_index("gx")
    gy = lax.axis_index("gy")
    me = gx * NM + gy
    ga = gx_peers(gx)
    gb = gy_peers(gy)
    peers = all_peers(gx, gy)
    n = NG * NM - 1
    loads = [
        pltpu.make_async_copy(base_h, base, la.at[0]),
        pltpu.make_async_copy(fine_h.at[:, :, 0, :], fine, la.at[1]),
        pltpu.make_async_copy(fold_h.at[:, :, 0, :], fold, la.at[2]),
        pltpu.make_async_copy(old_h, old, la.at[3]),
    ]
    for load in loads:
        load.start()
    bar = pltpu.get_barrier_semaphore()
    for a in ga:
        pl.semaphore_signal(bar, inc=1, device_id=(a, gy), device_id_type=MESH)
    for b in gb:
        pl.semaphore_signal(bar, inc=1, device_id=(gx, b), device_id_type=MESH)
    cpl = couplings(cp)
    place_patches(off, pg, pxy)
    loads[0].wait()
    extract_base(gx, gy, pxy, base, trans, hr, hc, s1)
    loads[1].wait()
    blank = jnp.zeros((32, 384 - FC), F32)
    fh[0] = jnp.concatenate([fine[:, 0, :], blank], axis=1)
    fh[1] = jnp.concatenate([fine[:, FR - 1, :], blank], axis=1)
    own = pltpu.make_async_copy(s1.at[gx], r1.at[gx], lb.at[0])
    own.start()
    fine_fill(fine, pad)
    loads[2].wait()
    acc = fine_levels(0, EARLY, jnp.zeros((8, 128), F32), cpl, fold, pad, res)
    pl.semaphore_wait(bar, len(ga) + len(gb))
    for a in ga:
        pl.semaphore_signal(known, inc=1, device_id=(a, gy), device_id_type=MESH)

    up, down = wrap(gx + 1, NG), wrap(gx + NG - 1, NG)
    right, left = wrap(gy + 1, NM), wrap(gy + NM - 1, NM)
    halos = [
        remote(fh.at[1], fhn.at[0], sb.at[8], sb.at[9], gx, right),
        remote(fh.at[0], fhn.at[1], sb.at[10], sb.at[11], gx, left),
        remote(hr.at[1], hrn.at[0], sb.at[0], sb.at[1], up, gy),
        remote(hr.at[0], hrn.at[1], sb.at[2], sb.at[3], down, gy),
        remote(hc.at[1], hcn.at[0], sb.at[4], sb.at[5], gx, right),
        remote(hc.at[0], hcn.at[1], sb.at[6], sb.at[7], gx, left),
    ]
    for h in halos:
        h.start()
    for a in ga:
        remote(s1.at[a], r1.at[gx], sa.at[0], sa.at[1], a, gy).start()

    acc = fine_levels(EARLY, 8, acc, cpl, fold, pad, res)
    halos[0].wait()
    halos[1].wait()
    hrow[0] = fhn[0] * jnp.where(gy > 0, 1.0, 0.0)
    hrow[1] = fhn[1] * jnp.where(gy < NM - 1, 1.0, 0.0)
    acc = acc + fine_rows(hrow, fh, res)
    x = pxy[0, gx]
    y = pxy[1, gx]
    restrict(x, gy, fine, fh, qs, res, mm, cells, ss)
    rs[slot(me, 8), :] = ss[slot(me, 8), :]
    pl.semaphore_wait(known, len(ga))
    for a, b in peers:
        remote(ss.at[slot(a * NM + b, 8, 5), :], rs.at[slot(me, 8, 5), :], sd.at[0], sd.at[1], a, b).start()

    for h in halos[2:]:
        h.wait()
    loads[3].wait()
    bsum = base_tendency(gx, gy, pxy, cpl, base, old, hrn, hcn, hz, ring, tend, d0, d1)
    puts = [
        pltpu.make_async_copy(tend, tend_h, lb.at[3]),
        pltpu.make_async_copy(d0, d0_h, lb.at[4]),
        pltpu.make_async_copy(d1, d1_h, lb.at[5]),
        pltpu.make_async_copy(fout, fout_h, lb.at[6]),
        pltpu.make_async_copy(so.at[slot(me, PITCH), :], r2.at[slot(me, PITCH), :], lb.at[7]),
        pltpu.make_async_copy(nv, norm_h, lb.at[8]),
    ]
    for k in range(3):
        puts[k].start()

    own.wait()
    wait_bytes(r1.at[pl.ds(0, NG - 1)], sa.at[1])
    tb[0] = r1[jnp.maximum(x - 1, 0) // BX, 0:32, :]
    tb[1] = r1[(x + PC) // BX, 0:32, :]
    for j in range(NM):
        a = (x + 11 * j) // BX
        b = jnp.minimum(a + 1, NG - 1)
        gs[j, 0:32, :] = r1[a, 32:64, :]
        gs[j, 32:64, :] = r1[b, 32:64, :]
    for b in gb:
        remote(gs.at[b], gr.at[gy], sc.at[0], sc.at[1], gx, b).start()
    mine = pltpu.make_async_copy(gs.at[gy], gr.at[gy], lb.at[1])
    mine.start()
    ends = ((tr, 0, 0), (br, NM - 1, 1))
    for ref, target, k in ends:
        far = remote(tb.at[k], ref.at[gy], sc.at[2 + 2 * k], sc.at[3 + 2 * k], gx, target)
        near = pltpu.make_async_copy(tb.at[k], ref.at[gy], lb.at[2])

        @pl.when(gy != target)
        def _():
            far.start()

        @pl.when(gy == target)
        def _():
            near.start()

    compose_rows(gy, pxy, take)
    wait_bytes(rs.at[pl.ds(0, 5 * n), :], sd.at[1])
    compose_prepare(gx, pxy, rs, rolled, take, turned, lines)
    compose_send(0, HALF, gx, gy, pxy, so, rolled, take, turned, lines, r2, se)
    puts[4].start()

    mine.wait()
    wait_bytes(gr.at[pl.ds(0, NM - 1)], sc.at[1])
    hrow[...] = jnp.zeros((2, 32, 384), F32)
    for ref, target, k in ends:
        far = remote(tb.at[k], ref.at[gy], sc.at[2 + 2 * k], sc.at[3 + 2 * k], gx, target)
        near = pltpu.make_async_copy(tb.at[k], ref.at[gy], lb.at[2])

        @pl.when(gy != target)
        def _():
            far.wait_send()

        @pl.when(gy == target)
        def _():
            near.wait()
            wait_bytes(ref.at[pl.ds(0, NM - 1)], sc.at[3 + 2 * k])
            hrow[k] = edge_row(y, ref)

    cols = edge_columns(x, y, gy, gr)
    acc = acc + fine_rows(hrow, fh, res)
    acc = acc + fine_columns(cols, fine, res)
    norm = jnp.sum(bsum + acc * (1.0 / 9.0), axis=(0, 1), keepdims=True)
    nv[...] = jnp.broadcast_to(norm, (8, 128))
    nr[slot(me, 8), :] = jnp.broadcast_to(norm, (8, 128))
    for a, b in peers:
        remote(nv.at[pl.ds(0, 1), :], nr.at[slot(me, 8, 1), :], sf.at[0], sf.at[1], a, b).start()

    compose_send(HALF, NM, gx, gy, pxy, so, rolled, take, turned, lines, r2, se)

    def write(p, _):
        for t in range(2):
            fout[p, :, 128 * t : 128 * t + 128] = res[pl.ds((t * 32 + p) * 40, FR), :]
        fout[p, :, 256:FC] = res[pl.ds((64 + p) * 40, FR), :][:, 0 : FC - 256]
        return 0

    lax.fori_loop(0, 32, write, 0)
    puts[3].start()
    wait_bytes(nr.at[pl.ds(0, n), :], sf.at[1])
    wait_bytes(nr.at[pl.ds(0, n), :], sf.at[0])
    total = jnp.sum(nr[pl.ds(0, 128, stride=8), :], axis=0, keepdims=True)
    nv[...] = jnp.broadcast_to(jnp.sqrt(total), (8, 128))
    puts[5].start()
    for put in puts:
        put.wait()
    wait_bytes(r1.at[pl.ds(0, NG - 1)], sa.at[0])
    wait_bytes(gr.at[pl.ds(0, NM - 1)], sc.at[0])
    wait_bytes(rs.at[pl.ds(0, 5 * n), :], sd.at[0])
    wait_bytes(so.at[pl.ds(0, USED * n), :], se.at[0])
    wait_bytes(so.at[pl.ds(0, USED * n), :], se.at[1])


def main(off, pg, cp, base, old, fine, fold):
    hbm = pl.BlockSpec(memory_space=pl.ANY)
    dma = pltpu.SemaphoreType.DMA
    return pl.pallas_call(
        main_kernel,
        out_shape=(shape(32, BX, BY),) * 3 + (shape(32, FR, FC), shape(8, 128), shape(NG * NM * PITCH, 128)),
        in_specs=[sspec()] * 3 + [hbm] * 4,
        out_specs=(hbm,) * 6,
        scratch_shapes=[
            pltpu.SMEM((2, NG), jnp.int32),
            VM((32, BX, BY), F32),
            VM((32, BX, BY), F32),
            VM((32, FR, FC), F32),
            VM((32, FR, FC), F32),
            VM((32, BX, BY), F32),
            VM((32, BX, BY), F32),
            VM((32, BX, BY), F32),
            VM((4, BX, BY), F32),
            VM((128, 16, 128), F32),
            VM((NG, 64, 128), F32),
            VM((2, 32, 128), F32),
            VM((2, 16, 128), F32),
            VM((2, 32, 384), F32),
            VM((NG, 64, 128), F32),
            VM((2, 32, 128), F32),
            VM((2, 16, 128), F32),
            VM((2, 32, 384), F32),
            VM((NM, 64, 128), F32),
            VM((2, 32, 128), F32),
            VM((NM, 64, 128), F32),
            VM((NM, 32, 128), F32),
            VM((NM, 32, 128), F32),
            VM((2, 32, 128), F32),
            VM((40, 56, 384), F32),
            VM((2, 32, 384), F32),
            VM((3 * 32 * 40, 128), F32),
            VM((3, 32, 16, 128), F32),
            VM((16 * 40, 128), F32),
            VM((32, 16, 128), F32),
            VM((1024, 128), F32),
            VM((1024, 128), F32),
            VM((NG * NM * PITCH, 128), F32),
            VM((4, 128, 128), F32),
            VM((128, 256), jnp.bfloat16),
            VM((128, 128), F32),
            VM((NG, 128), F32),
            VM((8, 128), F32),
            VM((1024, 128), F32),
            VM((32, FR, FC), F32),
            dma((4,)),
            dma((2,)),
            dma((12,)),
            dma((6,)),
            dma((2,)),
            dma((2,)),
            dma((2,)),
            dma((9,)),
            pltpu.SemaphoreType.REGULAR,
        ],
        compiler_params=pltpu.CompilerParams(collective_id=0, has_side_effects=True),
    )(off, pg, cp, base, old, fine, fold)


PARTS = 4


def merge_kernel(off, tend_h, d0_h, d1_h, r2, fout, nv, out_h, fres, norm, tend, d0, d1, ri, fine, sem):
    r = lax.axis_index("gx")
    c = lax.axis_index("gy")
    slots = [pl.ds(128 // PARTS * k, 128 // PARTS) for k in range(PARTS)]
    levels = 8 // PARTS

    def copies(pairs, at):
        return [[pltpu.make_async_copy(a, b, sem.at[at + k]) for a, b in pairs(k)] for k in range(PARTS)]

    def planes(k):
        return [pl.ds(8 * f + levels * k, levels) for f in range(4)]

    piece = 32 // PARTS
    here = [pl.ds(piece * k, piece) for k in range(PARTS)]
    got = [pltpu.make_async_copy(r2.at[:, 0:USED, :], ri.at[:, 0:USED, :], sem.at[0])]
    had = [
        [pltpu.make_async_copy(a.at[s], b.at[s], sem.at[1 + k]) for a, b in ((tend_h, tend), (d0_h, d0), (d1_h, d1)) for s in planes(k)]
        for k in range(PARTS)
    ]
    give = [[pltpu.make_async_copy(tend.at[s], out_h.at[s], sem.at[1 + PARTS + k]) for s in planes(k)] for k in range(PARTS)]
    take = [pltpu.make_async_copy(fout.at[here[k]], fine.at[here[k]], sem.at[1 + 2 * PARTS + k]) for k in range(PARTS)]
    put = [pltpu.make_async_copy(fine.at[here[k]], fres.at[here[k], :, 0, :], sem.at[1 + 3 * PARTS + k]) for k in range(PARTS)]
    got[0].start()
    for k in range(PARTS):
        for copy in had[k]:
            copy.start()
    for k in range(PARTS):
        take[k].start()
    row = iota((8, BY), 0)
    lane = iota((8, BY), 1)
    last = [jnp.zeros((8, BY), F32) for t in range(8)]
    east = [jnp.zeros((8, BY), F32) for t in range(8)]
    for g in range(NG):
        x = off[0, g] - r * BX
        y = off[1, g] - c * BY
        across = (lane >= y) & (lane < y + PC)
        edge = lane == y + PC - 1
        for t in range(8):
            last[t] = jnp.where((row + 8 * t == x + PC - 1) & across, 1.0, last[t])
            east[t] = jnp.where((row + 8 * t >= x) & (row + 8 * t < x + PC) & edge, 1.0, east[t])
    norm[...] = nv[0:1, 0:1]
    flat = ri.reshape(128 * PITCH, 128)
    got[0].wait()
    for k in range(PARTS):
        for copy in had[k]:
            copy.wait()
        for l in range(levels * k, levels * k + levels):
            ends = []
            turn = []
            for side in range(2):
                at = (2 * l + side) * 8 * PITCH + 16
                ends.append(flat[pl.ds(at, 8, stride=PITCH), :])
                row17 = flat[pl.ds(at + 1, 8, stride=PITCH), :]
                turn.append([pltpu.roll(row17, lax.rem(256 - 8 * r - 64 * w, 128), 1) for w in range(2)])
            for t in range(8):
                tile = slice(8 * t, 8 * t + 8)
                e0 = jnp.where(last[t] > 0.5, ends[1], ends[0])
                e1 = [
                    jnp.where(lane < 64, *[jnp.broadcast_to(turn[side][w][:, t : t + 1], (8, 128)) for w in range(2)])
                    for side in range(2)
                ]
                e1 = jnp.where(east[t] > 0.5, e1[1], e1[0])
                for f in range(4):
                    p = 8 * f + l
                    new = flat[pl.ds((p // 2) * 8 * PITCH + (p % 2) * 8 + t, 8, stride=PITCH), :]
                    edge = e0 * d0[p, tile, :] + e1 * d1[p, tile, :]
                    tend[p, tile, :] = tend[p, tile, :] + new + (0.15 / 9) * edge
        for copy in give[k]:
            copy.start()
        take[k].wait()
        put[k].start()
    for k in range(PARTS):
        for copy in give[k]:
            copy.wait()
        put[k].wait()


def merge(off, tend, d0, d1, ri, fout, nv):
    hbm = pl.BlockSpec(memory_space=pl.ANY)
    return pl.pallas_call(
        merge_kernel,
        out_shape=(shape(32, BX, BY), shape(32, FR, 1, FC), shape(1, 1)),
        in_specs=[sspec()] + [hbm] * 5 + [vspec()],
        out_specs=(hbm, hbm, vspec()),
        scratch_shapes=[
            VM((32, BX, BY), F32),
            VM((32, BX, BY), F32),
            VM((32, BX, BY), F32),
            VM((NG * NM, PITCH, 128), F32),
            VM((32, FR, FC), F32),
            pltpu.SemaphoreType.DMA((1 + 4 * PARTS,)),
        ],
    )(off, tend, d0, d1, ri.reshape(NG * NM, PITCH, 128), fout, nv)


def local(base_state, base_old, fine_state, fine_old, coupling, patch_offsets, patch_group):
    base = base_state.reshape(32, BX, BY)
    old = base_old.reshape(32, BX, BY)
    fine = fine_state.reshape(32, FR, 1, FC)
    fold = fine_old.reshape(32, FR, 1, FC)
    off = patch_offsets.T
    tend, d0, d1, fout, nv, r2 = main(off, patch_group, coupling, base, old, fine, fold)
    bout, fres, norm = merge(off, tend, d0, d1, r2, fout, nv)
    return (
        bout.reshape(4, 8, BX, BY),
        fres.reshape(4, 8, 1, FR, FC),
        norm.reshape(()),
    )


def solution(mesh):
    placed = (
        P(None, None, "gx", "gy"),
        P(None, None, "gx", "gy"),
        P(None, None, "gx", "gy", None),
        P(None, None, "gx", "gy", None),
        P(),
        P(),
        P(),
    )
    return jax.shard_map(
        local,
        mesh=mesh,
        in_specs=placed,
        out_specs=(P(None, None, "gx", "gy"), P(None, None, "gx", "gy", None), P()),
        check_vma=False,
    )
```

```python
import functools

import jax
import jax.numpy as jnp
from jax import lax
from jax.experimental import pallas as pl
from jax.experimental.pallas import tpu as pltpu
from jax.sharding import PartitionSpec as P

PC = 88
NG, NM = 16, 8
BX, BY = 64, 128
FR, FC = 33, 264
MESH = pl.DeviceIdType.MESH
VM = pltpu.VMEM
F32 = jnp.float32
HI = lax.Precision.HIGHEST


def vspec():
    return pl.BlockSpec(memory_space=pltpu.VMEM)


def sspec():
    return pl.BlockSpec(memory_space=pltpu.SMEM)


def shape(*dims):
    return jax.ShapeDtypeStruct(dims, F32)


def iota(dims, axis):
    return lax.broadcasted_iota(jnp.int32, dims, axis)


def wrap(v, n):
    return jnp.where(v >= n, v - n, v)


def gx_peers(gx):
    x = gx // 4
    z = gx - 4 * x
    out = []
    for dx, dz in GX_OFFSETS:
        out.append(wrap(x + dx, 4) * 4 + wrap(z + dz, 4))
    return out


GX_OFFSETS = (
    (2, 2), (1, 2), (2, 1), (3, 2), (2, 3), (1, 1), (3, 3), (1, 3), (3, 1), (2, 0), (0, 2), (1, 0), (0, 1), (3, 0), (0, 3),
)


def gy_peers(gy):
    return [wrap(gy + d, NM) for d in range(1, NM)]


def all_peers(gx, gy):
    x = gx // 4
    z = gx - 4 * x
    y = gy // 2
    c = gy - 2 * y
    offs = [(a, b, d, e) for a in range(4) for b in range(4) for d in range(4) for e in range(2)][1:]
    offs.sort(key=lambda o: -sum(min(v, 4 - v) for v in o[:3]))
    xs = [wrap(x + d, 4) for d in range(4)]
    ys = [wrap(y + d, 4) for d in range(4)]
    zs = [wrap(z + d, 4) for d in range(4)]
    cs = [c, 1 - c]
    return [(xs[a] * 4 + zs[d], ys[b] * 2 + cs[e]) for a, b, d, e in offs]


def remote(src, dst, send, recv, a, b):
    return pltpu.make_async_remote_copy(
        src_ref=src, dst_ref=dst, send_sem=send, recv_sem=recv, device_id=(a, b), device_id_type=MESH
    )


def wait_bytes(ref, sem):
    pltpu.make_async_copy(ref, ref, sem).wait()


def slot(d, n, size=None):
    return pl.ds(pl.multiple_of(d * n, n), size or n)


def stencil(q, north, south, east, west, above, below, old, cpl, a0m, a0p, a1m, a1p, own, f):
    total = own * q[f] - old
    total += north * a0m - south * a0p
    total += east * a1m - west * a1p
    total -= 0.05 * (above + below)
    for g in range(4):
        total += cpl[f][g] * q[g]
    return total


def couplings(cp):
    return [[0.1 * cp[f, g] for g in range(4)] for f in range(4)]


PITCH = 24
USED = 18
EARLY = 0
HALF = 5
KB = 0.02
KF = 0.02 * 9


def place_patches(off, pg, pxy):
    for g in range(NG):
        x = jnp.int32(0)
        y = jnp.int32(0)
        for p in range(NG):
            hit = pg[p] == g
            x = x + jnp.where(hit, off[0, p], 0)
            y = y + jnp.where(hit, off[1, p], 0)
        pxy[0, g] = x
        pxy[1, g] = y


def extract_base(r, c, pxy, base, trans, hr, hc, s1):
    flat = trans.reshape(2048, 128)
    for q in range(16):
        flat[pl.ds(q, 128, stride=16), :] = base[2 * q : 2 * q + 2].reshape(128, 128).T
    hr[0] = base[:, 0, :]
    hr[1] = base[:, BX - 1, :]
    hc[0] = trans[0]
    hc[1] = trans[127]

    def body(g, _):
        x = pxy[0, g]
        y = pxy[1, g]
        lo = x - 1 - r * BX
        hi = x + PC - r * BX
        loc = jnp.where((lo >= 0) & (lo < BX), lo, jnp.clip(hi, 0, BX - 1))
        s1[g, 0:32, :] = base[:, loc, :]
        y0 = jnp.clip(y - 1 - c * BY, 0, BY - 1)
        s1[g, 32:48, :] = trans[y0]
        y1 = jnp.clip(y + PC - c * BY, 0, BY - 1)
        s1[g, 48:64, :] = trans[y1]
        return 0

    lax.fori_loop(0, NG, body, 0)


def base_tendency(r, c, pxy, cpl, base, old, hrn, hcn, hz, ring, tend, d0, d1):
    keep = [
        jnp.where(r > 0, 1.0, 0.0),
        jnp.where(r < NG - 1, 1.0, 0.0),
        jnp.where(c > 0, 1.0, 0.0),
        jnp.where(c < NM - 1, 1.0, 0.0),
    ]
    hz[0] = hrn[0] * keep[0]
    hz[1] = hrn[1] * keep[1]
    zeros = jnp.zeros((112, 128), F32)
    westc = jnp.concatenate([hcn[0] * keep[2], zeros], axis=0).T
    eastc = jnp.concatenate([hcn[1] * keep[3], zeros], axis=0).T
    row = iota((BX, BY), 0)
    lane = iota((BX, BY), 1)
    open_ = ring_masks(r, c, pxy, ring)
    own = 1.0 + 4 * KB + 0.1
    acc = jnp.zeros((BX, BY), F32)
    for l in range(8):
        q = [base[f * 8 + l] for f in range(4)]
        a0 = 0.05 * q[0]
        a1 = 0.05 * q[1]
        for f in range(4):
            p = f * 8 + l
            pair, par = p // 2, p % 2
            north = jnp.where(row == BX - 1, hz[1, p : p + 1, :], pltpu.roll(q[f], BX - 1, 0))
            south = jnp.where(row == 0, hz[0, p : p + 1, :], pltpu.roll(q[f], 1, 0))
            ecol = pltpu.roll(eastc[par * 64 : par * 64 + 64], 127 - pair, 1)
            wcol = pltpu.roll(westc[par * 64 : par * 64 + 64], (128 - pair) % 128, 1)
            east = jnp.where(lane == BY - 1, ecol, pltpu.roll(q[f], BY - 1, 1))
            west = jnp.where(lane == 0, wcol, pltpu.roll(q[f], 1, 1))
            none = jnp.zeros((BX, BY), F32)
            above = base[p + 1] if l < 7 else none
            below = base[p - 1] if l > 0 else none
            total = stencil(
                q, north, south, east, west, above, below, old[p], cpl,
                a0 - KB, a0 + KB, a1 - KB, a1 + KB, own, f,
            )
            after = ring[1] * north
            before = ring[0] * south
            d0[0, p : p + 1, :] = jnp.sum(before, axis=0, keepdims=True)
            d0[1, p : p + 1, :] = jnp.sum(after, axis=0, keepdims=True)
            both = after + before
            after = ring[3] * east
            before = ring[2] * west
            d1[p] = after - before
            tend[p] = open_ * total - (3 * KF / 9) * (both + after + before)
            acc = acc + open_ * (total * total)
    return acc.reshape(8, 8, 128).sum(axis=0)


def ring_masks(r, c, pxy, ring):
    row = iota((BX, BY), 0)
    lane = iota((BX, BY), 1)
    cells = jnp.ones((BX, BY), F32)
    sides = [jnp.zeros((BX, BY), F32)] * 4
    for g in range(NG):
        x = pxy[0, g] - r * BX
        y = pxy[1, g] - c * BY
        inside = (row >= x) & (row < x + PC) & (lane >= y) & (lane < y + PC)
        cells = jnp.where(inside, 0.0, cells)
        lines = (row == x, row == x + PC - 1, lane == y, lane == y + PC - 1)
        sides = [jnp.where(inside & line, 1.0, side) for line, side in zip(lines, sides)]
    for k in range(4):
        ring[k] = sides[k]
    return cells


def fine_fill(fine, pad):
    for f in range(4):
        pad[f * 10] = jnp.zeros((56, 384), F32)
        pad[f * 10 + 9] = jnp.zeros((56, 384), F32)

    def fill(p, _):
        dst = p + 2 * (p // 8) + 1
        pad[dst, 0:8, :] = jnp.zeros((8, 384), F32)
        pad[dst, 8 : 8 + FR, 0:256] = fine[p, :, 0:256]
        pad[dst, 8 : 8 + FR, 256:384] = jnp.concatenate([fine[p, :, 256:FC], jnp.zeros((FR, 120), F32)], axis=1)
        pad[dst, 8 + FR : 9 + FR, :] = jnp.zeros((1, 384), F32)
        return 0

    lax.fori_loop(0, 32, fill, 0)


def fine_levels(first, stop, acc, cpl, old, pad, res):
    own = 1.0 + 4 * KF + 0.1

    def level(l, acc):
        for start, n in ((0, 8), (8, 8), (16, 8), (24, 8), (32, 1)):
            s = 8 + start
            q = [pad[f * 10 + 1 + l, s : s + n, :] for f in range(4)]
            a0 = 0.15 * q[0]
            a1 = 0.15 * q[1]
            keep = iota((n, 384), 1) < FC
            for f in range(4):
                z = f * 10 + 1 + l
                north = pad[z, s + 1 : s + 1 + n, :]
                south = pad[z, s - 1 : s - 1 + n, :]
                east = pltpu.roll(q[f], 383, 1)
                west = pltpu.roll(q[f], 1, 1)
                p = f * 8 + l
                before = old[p, start : start + n, :]
                before = jnp.concatenate([before, jnp.zeros((n, 384 - FC), F32)], axis=1)
                total = stencil(
                    q, north, south, east, west, pad[z + 1, s : s + n, :], pad[z - 1, s : s + n, :],
                    before, cpl, a0 - KF, a0 + KF, a1 - KF, a1 + KF, own, f,
                )
                total = jnp.where(keep, total, 0.0)
                for t in range(3):
                    part = total[:, 128 * t : 128 * t + 128]
                    res[pl.ds((t * 32 + p) * 40 + start, n), :] = part
                    sq = part * part
                    if n == 1:
                        sq = jnp.where(iota((8, 128), 0) == 0, jnp.broadcast_to(sq, (8, 128)), 0.0)
                    acc = acc + sq
        return acc

    return lax.fori_loop(first, stop, level, acc)


def edge_columns(x, y, j, gr):
    first = lax.rem(x + 11 * j, BX)
    cl = jnp.maximum(y - 1, 0) // BY
    cr = (y + PC) // BY
    blank = jnp.zeros((96, 128), F32)
    va = jnp.concatenate([gr[cl, 0:16, :], gr[cr, 16:32, :], blank], axis=0)
    vb = jnp.concatenate([gr[cl, 32:48, :], gr[cr, 48:64, :], blank], axis=0)
    want = first + iota((40, 128), 0) // 3
    lane40 = iota((40, 128), 1)
    cols = []
    for par in range(2):
        at = lane40 - 64 * par
        good = (at >= 0) & (at < 64)
        pa = jnp.where(good & (at == want), 1.0, 0.0)
        pb = jnp.where(good & (at + 64 == want), 1.0, 0.0)
        dims = (((1,), (1,)), ((), ()))
        cols.append(
            lax.dot_general(pa, va, dims, precision=HI, preferred_element_type=F32)
            + lax.dot_general(pb, vb, dims, precision=HI, preferred_element_type=F32)
        )
    return cols


def edge_row(y, cells):
    c0 = y // BY
    c1 = jnp.minimum(c0 + 1, NM - 1)
    b = iota((128, 384), 0)
    jf = iota((128, 384), 1)
    cell = y + jf // 3 - c0 * BY
    good = jf < FC
    p0 = jnp.where(good & (b == cell), 1.0, 0.0)
    p1 = jnp.where(good & (b + BY == cell), 1.0, 0.0)
    return jnp.dot(cells[c0], p0, precision=HI, preferred_element_type=F32) + jnp.dot(
        cells[c1], p1, precision=HI, preferred_element_type=F32
    )


def fine_rows(hrow, fh, res):
    change = jnp.zeros((8, 128), F32)
    for t in range(3):
        for row, side in ((0, 0), (FR - 1, 1)):
            a0 = 0.15 * fh[side, 0:8, 128 * t : 128 * t + 128]
            factor = a0 - KF if side else -(a0 + KF)
            factor = jnp.concatenate([factor] * 4, axis=0)
            at = pl.ds(t * 32 * 40 + row, 32, stride=40)
            was = res[at, :]
            now = was + hrow[side, :, 128 * t : 128 * t + 128] * factor
            res[at, :] = now
            for f in range(4):
                change = change + (now[8 * f : 8 * f + 8] * now[8 * f : 8 * f + 8])
                change = change - (was[8 * f : 8 * f + 8] * was[8 * f : 8 * f + 8])
    return change


def fine_columns(cols, fine, res):
    change = jnp.zeros((8, 128), F32)
    lane = iota((FR, 128), 1)
    for l in range(8):
        q1 = fine[8 + l, :, 0:128]
        lo = -(0.15 * q1 + KF)
        q1 = jnp.concatenate([fine[8 + l, :, 256:FC], jnp.zeros((FR, 120), F32)], axis=1)
        hi = 0.15 * q1 - KF
        for f in range(4):
            p = f * 8 + l
            pair, par = p // 2, p % 2
            cv = cols[par][:FR]
            for t, factor, spot, turn in ((0, lo, 0, (128 - pair) % 128), (2, hi, 7, 119 - pair)):
                at = pl.ds((t * 32 + p) * 40, FR)
                was = res[at, :]
                now = jnp.where(lane == spot, was + pltpu.roll(cv, turn, 1) * factor, was)
                res[at, :] = now
                delta = now * now - was * was
                change = change + delta[0:8] + delta[8:16] + delta[16:24] + delta[24:32]
                change = change + jnp.where(iota((8, 128), 0) == 0, jnp.broadcast_to(delta[32:33], (8, 128)), 0.0)
    return change


def restrict(x, j, fine, fh, qs, res, mm, cells, ss):
    for t in range(3):
        mm[t, :, 8:16, :] = jnp.zeros((32, 8, 128), F32)

    def rows(pair, _):
        for par in range(2):
            for t in range(3):
                at = (t * 32 + 2 * pair + par) * 40
                part = [res[pl.ds(at + d, 11, stride=3), :] for d in range(3)]
                mm[t, par * 16 + pair, 0:11, :] = part[0] + part[1] + part[2]
        return 0

    lax.fori_loop(0, 16, rows, 0, unroll=2)
    total = 0.0
    ends = [0.0, 0.0]
    for t in range(3):
        comb = jnp.where((iota((128, 128), 0) + 128 * t) // 3 == iota((128, 128), 1), 1.0, 0.0)
        total = total + jnp.dot(mm[t].reshape(512, 128), comb, precision=HI, preferred_element_type=F32)
        for side in range(2):
            row = fh[side, 0:8, 128 * t : 128 * t + 128]
            ends[side] = ends[side] + jnp.dot(row, comb, precision=HI, preferred_element_type=F32)
    cells[...] = (total * (1.0 / 9.0)).reshape(32, 16, 128)
    for l in range(8):
        qs[pl.ds(l * 40, FR), :] = fine[8 + l, :, 0:128]
        qs[pl.ds((8 + l) * 40, FR), :] = jnp.concatenate([fine[8 + l, :, 256:FC], jnp.zeros((FR, 120), F32)], axis=1)
    lane = iota((11, 128), 1)
    for l in range(8):
        for side, turn in ((0, 88), (1, 81)):
            at = (side * 8 + l) * 40
            part = [qs[pl.ds(at + d, 11, stride=3), :] for d in range(3)]
            edge = pltpu.roll(part[0] + part[1] + part[2], turn, 1)
            cells[2 * l + side, 0:11, :] = jnp.where(lane == 88, edge, cells[2 * l + side, 0:11, :])
    for k in range(NM):
        first = lax.rem(k - x - 11 * j + 2048, 8)
        for par in range(2):
            for h in range(2):
                v = cells[pl.ds(par * 16, 16), first + 8 * h, :]
                ss[pl.ds(k * 8 + par * 2 + h, 16, stride=64), :] = v
        for side in range(2):
            ss[pl.ds((side * 8 + k) * 8 + 4, 8, stride=128), :] = ends[side]


def split3(v):
    hi = v.astype(jnp.bfloat16)
    rest = v - hi.astype(F32)
    mid = rest.astype(jnp.bfloat16)
    return hi, mid, (rest - mid.astype(F32)).astype(jnp.bfloat16)


def compose_rows(gy, pxy, take):
    n = iota((1, 256), 1)
    h = n // 128
    g = (n - h * 128) // 8
    k = n - (n // 8) * 8
    x = jnp.zeros((1, 256), jnp.int32)
    for i in range(NG):
        x = jnp.where(g == i, pxy[0, i], x)
    start = x + 11 * k
    away = gy - start + 2048
    row = away - (away // 8) * 8 + 8 * h
    octet = jnp.where(row <= 10, (start + row - gy) // 8, -1)
    take[...] = jnp.where(iota((128, 256), 0) == octet, 1.0, 0.0).astype(jnp.bfloat16)


def compose_prepare(gx, pxy, rs, rolled, take, turned, lines):
    for i in range(NG):
        v = [rs[pl.ds(i * 64 + q, 8, stride=8), :] for q in range(4)]
        shift = jnp.broadcast_to(lax.rem(pxy[1, i], BY), (8, 128))
        for bit in range(7):
            shift, odd = shift // 2, shift - 2 * (shift // 2) == 1
            v = [jnp.where(odd, pltpu.roll(u, 1 << bit, 1), u) for u in v]
        for q in range(4):
            rolled[q, 8 * i : 8 * i + 8, :] = v[q]
    lane = iota((8, 128), 1)
    side = gx - 2 * (gx // 2)
    rank = iota((NG, 128), 0)
    yy = jnp.zeros((NG, 128), jnp.int32)
    for i in range(NG):
        yy = jnp.where(rank == i, pxy[1, i], yy)
    ends = rs[pl.ds(side * (NM - 1) * 8 + 4, NG, stride=64), :]
    shift = yy - (yy // BY) * BY
    for bit in range(7):
        shift, odd = shift // 2, shift - 2 * (shift // 2) == 1
        ends = jnp.where(odd, pltpu.roll(ends, 1 << bit, 1), ends)
    lines[...] = ends
    spots = []
    for i in range(NG):
        spots.append(jnp.where(lane == (pxy[1, i] + side * (PC - 1)) // 64, 1.0, 0.0))
    spots = jnp.concatenate(spots, axis=0)
    sums = []
    for h_ in range(2):
        v = rs[pl.ds(h_, 128, stride=8), :]
        sums.append(jnp.broadcast_to(v[:, 88:89], (128, 128)) * spots)
    b = jnp.concatenate(split3(jnp.concatenate(sums, axis=0)), axis=1)
    b = jnp.dot(take[...], b, preferred_element_type=F32)
    turned[...] = (b[:, 0:128] + (b[:, 128:256] + b[:, 256:384])).T


def compose_send(first, stop, gx, gy, pxy, so, rolled, take, turned, lines, r2, sems):
    lane = iota((8, 128), 1)
    side = gx - 2 * (gx // 2)
    rank = iota((NG, 128), 0)
    yy = jnp.zeros((NG, 128), jnp.int32)
    for i in range(NG):
        yy = jnp.where(rank == i, pxy[1, i], yy)
    ends = lines[...]
    x4 = gx // 4
    z4 = gx - 4 * x4
    def column(step, _):
        half = (step + 1) // 2
        away = 4 + jnp.where(step - 2 * (step // 2) == 0, half, -half)
        c = wrap(gy + away, NM)
        inside = []
        for i in range(NG):
            at = lane + c * BY - pxy[1, i]
            inside.append((at >= 0) & (at < PC))
        for par in range(2):
            rows = []
            for q in (2 * par, 2 * par + 1):
                for i in range(NG):
                    rows.append(jnp.where(inside[i], rolled[q, 8 * i : 8 * i + 8, :], 0.0))
            b = jnp.concatenate(split3(jnp.concatenate(rows, axis=0)), axis=1)
            got = jnp.dot(take[...], b, preferred_element_type=F32)
            got = got[:, 0:128] + (got[:, 128:256] + got[:, 256:384])
            for r in range(NG):
                at = pl.multiple_of((r * NM + c) * PITCH + 8 * par, 8)
                so[pl.ds(at, 8), :] = got[8 * r : 8 * r + 8]
        across = iota((NG, 128), 1) + c * BY - yy
        mine = jnp.where((across >= 0) & (across < PC), ends, 0.0)
        out = jnp.zeros((NG, 128), F32)
        for i in range(NG):
            line = pxy[0, i] + side * (PC - 1)
            hit = (rank == line // BX) & (line - (line // 8) * 8 == gy)
            out = jnp.where(hit, out + jnp.broadcast_to(mine[i : i + 1], (NG, 128)), out)
        so[pl.ds(c * PITCH + 16, NG, stride=NM * PITCH), :] = out
        octet = iota((NG, 128), 1) // 8
        low = jnp.broadcast_to(turned[pl.ds(2 * c, 1), :], (NG, 128))
        high = jnp.broadcast_to(pltpu.roll(turned[pl.ds(2 * c + 1, 1), :], 64, 1), (NG, 128))
        so[pl.ds(c * PITCH + 17, NG, stride=NM * PITCH), :] = jnp.where(octet == rank, low, high)

        for dx, dz in GX_OFFSETS + ((0, 0),):
            a = wrap(x4 + dx, 4) * 4 + wrap(z4 + dz, 4)
            send = remote(
                so.at[slot(a * NM + c, PITCH, USED), :], r2.at[slot(gx * NM + gy, PITCH, USED), :],
                sems.at[0], sems.at[1], a, c,
            )
            if (dx, dz) == (0, 0):
                pl.when(away > 0)(send.start)
            else:
                send.start()
        return 0

    lax.fori_loop(first, stop, column, 0)


def main_kernel(
    off, pg, cp, base_h, old_h, fine_h, fold_h,
    tend_h, d0_h, d1_h, fout_h, norm_h, r2,
    pxy, base, old, fine, fold, tend, d0, d1, ring, trans, s1, hr, hc, fh, r1, hrn, hcn, fhn, gs, tb, gr, tr, br, hz,
    pad, hrow, res, mm, qs, cells, ss, rs, so, rolled, take, turned, lines, nv, nr, fout,
    la, sa, sb, sc, sd, se, sf, lb, known,
):
    gx = lax.axis_index("gx")
    gy = lax.axis_index("gy")
    me = gx * NM + gy
    ga = gx_peers(gx)
    gb = gy_peers(gy)
    peers = all_peers(gx, gy)
    n = NG * NM - 1
    loads = [
        pltpu.make_async_copy(base_h, base, la.at[0]),
        pltpu.make_async_copy(fine_h.at[:, :, 0, :], fine, la.at[1]),
        pltpu.make_async_copy(fold_h.at[:, :, 0, :], fold, la.at[2]),
        pltpu.make_async_copy(old_h, old, la.at[3]),
    ]
    for load in loads:
        load.start()
    bar = pltpu.get_barrier_semaphore()
    for a in ga:
        pl.semaphore_signal(bar, inc=1, device_id=(a, gy), device_id_type=MESH)
    for b in gb:
        pl.semaphore_signal(bar, inc=1, device_id=(gx, b), device_id_type=MESH)
    cpl = couplings(cp)
    place_patches(off, pg, pxy)
    loads[0].wait()
    extract_base(gx, gy, pxy, base, trans, hr, hc, s1)
    loads[1].wait()
    blank = jnp.zeros((32, 384 - FC), F32)
    fh[0] = jnp.concatenate([fine[:, 0, :], blank], axis=1)
    fh[1] = jnp.concatenate([fine[:, FR - 1, :], blank], axis=1)
    own = pltpu.make_async_copy(s1.at[gx], r1.at[gx], lb.at[0])
    own.start()
    fine_fill(fine, pad)
    loads[2].wait()
    acc = fine_levels(0, EARLY, jnp.zeros((8, 128), F32), cpl, fold, pad, res)
    pl.semaphore_wait(bar, len(ga) + len(gb))
    for a in ga:
        pl.semaphore_signal(known, inc=1, device_id=(a, gy), device_id_type=MESH)

    up, down = wrap(gx + 1, NG), wrap(gx + NG - 1, NG)
    right, left = wrap(gy + 1, NM), wrap(gy + NM - 1, NM)
    halos = [
        remote(fh.at[1], fhn.at[0], sb.at[8], sb.at[9], gx, right),
        remote(fh.at[0], fhn.at[1], sb.at[10], sb.at[11], gx, left),
        remote(hr.at[1], hrn.at[0], sb.at[0], sb.at[1], up, gy),
        remote(hr.at[0], hrn.at[1], sb.at[2], sb.at[3], down, gy),
        remote(hc.at[1], hcn.at[0], sb.at[4], sb.at[5], gx, right),
        remote(hc.at[0], hcn.at[1], sb.at[6], sb.at[7], gx, left),
    ]
    for h in halos:
        h.start()
    for a in ga:
        remote(s1.at[a], r1.at[gx], sa.at[0], sa.at[1], a, gy).start()

    acc = fine_levels(EARLY, 8, acc, cpl, fold, pad, res)
    halos[0].wait()
    halos[1].wait()
    hrow[0] = fhn[0] * jnp.where(gy > 0, 1.0, 0.0)
    hrow[1] = fhn[1] * jnp.where(gy < NM - 1, 1.0, 0.0)
    acc = acc + fine_rows(hrow, fh, res)
    x = pxy[0, gx]
    y = pxy[1, gx]
    restrict(x, gy, fine, fh, qs, res, mm, cells, ss)
    rs[slot(me, 8), :] = ss[slot(me, 8), :]
    pl.semaphore_wait(known, len(ga))
    for a, b in peers:
        remote(ss.at[slot(a * NM + b, 8, 5), :], rs.at[slot(me, 8, 5), :], sd.at[0], sd.at[1], a, b).start()

    for h in halos[2:]:
        h.wait()
    loads[3].wait()
    bsum = base_tendency(gx, gy, pxy, cpl, base, old, hrn, hcn, hz, ring, tend, d0, d1)
    puts = [
        pltpu.make_async_copy(tend, tend_h, lb.at[3]),
        pltpu.make_async_copy(d0, d0_h, lb.at[4]),
        pltpu.make_async_copy(d1, d1_h, lb.at[5]),
        pltpu.make_async_copy(fout, fout_h, lb.at[6]),
        pltpu.make_async_copy(so.at[slot(me, PITCH), :], r2.at[slot(me, PITCH), :], lb.at[7]),
        pltpu.make_async_copy(nv, norm_h, lb.at[8]),
    ]
    for k in range(3):
        puts[k].start()

    own.wait()
    wait_bytes(r1.at[pl.ds(0, NG - 1)], sa.at[1])
    tb[0] = r1[jnp.maximum(x - 1, 0) // BX, 0:32, :]
    tb[1] = r1[(x + PC) // BX, 0:32, :]
    for j in range(NM):
        a = (x + 11 * j) // BX
        b = jnp.minimum(a + 1, NG - 1)
        gs[j, 0:32, :] = r1[a, 32:64, :]
        gs[j, 32:64, :] = r1[b, 32:64, :]
    for b in gb:
        remote(gs.at[b], gr.at[gy], sc.at[0], sc.at[1], gx, b).start()
    mine = pltpu.make_async_copy(gs.at[gy], gr.at[gy], lb.at[1])
    mine.start()
    ends = ((tr, 0, 0), (br, NM - 1, 1))
    for ref, target, k in ends:
        far = remote(tb.at[k], ref.at[gy], sc.at[2 + 2 * k], sc.at[3 + 2 * k], gx, target)
        near = pltpu.make_async_copy(tb.at[k], ref.at[gy], lb.at[2])

        @pl.when(gy != target)
        def _():
            far.start()

        @pl.when(gy == target)
        def _():
            near.start()

    compose_rows(gy, pxy, take)
    wait_bytes(rs.at[pl.ds(0, 5 * n), :], sd.at[1])
    compose_prepare(gx, pxy, rs, rolled, take, turned, lines)
    compose_send(0, HALF, gx, gy, pxy, so, rolled, take, turned, lines, r2, se)

    mine.wait()
    wait_bytes(gr.at[pl.ds(0, NM - 1)], sc.at[1])
    hrow[...] = jnp.zeros((2, 32, 384), F32)
    for ref, target, k in ends:
        far = remote(tb.at[k], ref.at[gy], sc.at[2 + 2 * k], sc.at[3 + 2 * k], gx, target)
        near = pltpu.make_async_copy(tb.at[k], ref.at[gy], lb.at[2])

        @pl.when(gy != target)
        def _():
            far.wait_send()

        @pl.when(gy == target)
        def _():
            near.wait()
            wait_bytes(ref.at[pl.ds(0, NM - 1)], sc.at[3 + 2 * k])
            hrow[k] = edge_row(y, ref)

    cols = edge_columns(x, y, gy, gr)
    acc = acc + fine_rows(hrow, fh, res)
    acc = acc + fine_columns(cols, fine, res)
    norm = jnp.sum(bsum + acc * (1.0 / 9.0), axis=(0, 1), keepdims=True)
    nv[...] = jnp.broadcast_to(norm, (8, 128))
    nr[slot(me, 8), :] = jnp.broadcast_to(norm, (8, 128))
    for a, b in peers:
        remote(nv.at[pl.ds(0, 1), :], nr.at[slot(me, 8, 1), :], sf.at[0], sf.at[1], a, b).start()

    compose_send(HALF, NM, gx, gy, pxy, so, rolled, take, turned, lines, r2, se)
    puts[4].start()

    def write(p, _):
        for t in range(2):
            fout[p, :, 128 * t : 128 * t + 128] = res[pl.ds((t * 32 + p) * 40, FR), :]
        fout[p, :, 256:FC] = res[pl.ds((64 + p) * 40, FR), :][:, 0 : FC - 256]
        return 0

    lax.fori_loop(0, 32, write, 0)
    puts[3].start()
    wait_bytes(nr.at[pl.ds(0, n), :], sf.at[1])
    wait_bytes(nr.at[pl.ds(0, n), :], sf.at[0])
    total = jnp.sum(nr[pl.ds(0, 128, stride=8), :], axis=0, keepdims=True)
    nv[...] = jnp.broadcast_to(jnp.sqrt(total), (8, 128))
    puts[5].start()
    for put in puts:
        put.wait()
    wait_bytes(r1.at[pl.ds(0, NG - 1)], sa.at[0])
    wait_bytes(gr.at[pl.ds(0, NM - 1)], sc.at[0])
    wait_bytes(rs.at[pl.ds(0, 5 * n), :], sd.at[0])
    wait_bytes(so.at[pl.ds(0, USED * n), :], se.at[0])
    wait_bytes(so.at[pl.ds(0, USED * n), :], se.at[1])


def main(off, pg, cp, base, old, fine, fold):
    hbm = pl.BlockSpec(memory_space=pl.ANY)
    dma = pltpu.SemaphoreType.DMA
    return pl.pallas_call(
        main_kernel,
        out_shape=(shape(32, BX, BY), shape(2, 32, BY), shape(32, BX, BY)) + (shape(32, FR, FC), shape(8, 128), shape(NG * NM * PITCH, 128)),
        in_specs=[sspec()] * 3 + [hbm] * 4,
        out_specs=(hbm,) * 6,
        scratch_shapes=[
            pltpu.SMEM((2, NG), jnp.int32),
            VM((32, BX, BY), F32),
            VM((32, BX, BY), F32),
            VM((32, FR, FC), F32),
            VM((32, FR, FC), F32),
            VM((32, BX, BY), F32),
            VM((2, 32, BY), F32),
            VM((32, BX, BY), F32),
            VM((4, BX, BY), F32),
            VM((128, 16, 128), F32),
            VM((NG, 64, 128), F32),
            VM((2, 32, 128), F32),
            VM((2, 16, 128), F32),
            VM((2, 32, 384), F32),
            VM((NG, 64, 128), F32),
            VM((2, 32, 128), F32),
            VM((2, 16, 128), F32),
            VM((2, 32, 384), F32),
            VM((NM, 64, 128), F32),
            VM((2, 32, 128), F32),
            VM((NM, 64, 128), F32),
            VM((NM, 32, 128), F32),
            VM((NM, 32, 128), F32),
            VM((2, 32, 128), F32),
            VM((40, 56, 384), F32),
            VM((2, 32, 384), F32),
            VM((3 * 32 * 40, 128), F32),
            VM((3, 32, 16, 128), F32),
            VM((16 * 40, 128), F32),
            VM((32, 16, 128), F32),
            VM((1024, 128), F32),
            VM((1024, 128), F32),
            VM((NG * NM * PITCH, 128), F32),
            VM((4, 128, 128), F32),
            VM((128, 256), jnp.bfloat16),
            VM((128, 128), F32),
            VM((NG, 128), F32),
            VM((8, 128), F32),
            VM((1024, 128), F32),
            VM((32, FR, FC), F32),
            dma((4,)),
            dma((2,)),
            dma((12,)),
            dma((6,)),
            dma((2,)),
            dma((2,)),
            dma((2,)),
            dma((9,)),
            pltpu.SemaphoreType.REGULAR,
        ],
        compiler_params=pltpu.CompilerParams(collective_id=0, has_side_effects=True),
    )(off, pg, cp, base, old, fine, fold)


PARTS = 4


def merge_kernel(off, tend_h, d0, d1_h, r2, fout, nv, out_h, fres, norm, tend, d1, ri, fine, sem):
    r = lax.axis_index("gx")
    c = lax.axis_index("gy")
    slots = [pl.ds(128 // PARTS * k, 128 // PARTS) for k in range(PARTS)]
    levels = 8 // PARTS

    def copies(pairs, at):
        return [[pltpu.make_async_copy(a, b, sem.at[at + k]) for a, b in pairs(k)] for k in range(PARTS)]

    def planes(k):
        return [pl.ds(8 * f + levels * k, levels) for f in range(4)]

    piece = 32 // PARTS
    here = [pl.ds(piece * k, piece) for k in range(PARTS)]
    got = [pltpu.make_async_copy(r2.at[:, 0:USED, :], ri.at[:, 0:USED, :], sem.at[0])]
    had = [
        [pltpu.make_async_copy(a.at[s], b.at[s], sem.at[1 + k]) for a, b in ((tend_h, tend), (d1_h, d1)) for s in planes(k)]
        for k in range(PARTS)
    ]
    give = [[pltpu.make_async_copy(tend.at[s], out_h.at[s], sem.at[1 + PARTS + k]) for s in planes(k)] for k in range(PARTS)]
    take = [pltpu.make_async_copy(fout.at[here[k]], fine.at[here[k]], sem.at[1 + 2 * PARTS + k]) for k in range(PARTS)]
    put = [pltpu.make_async_copy(fine.at[here[k]], fres.at[here[k], :, 0, :], sem.at[1 + 3 * PARTS + k]) for k in range(PARTS)]
    got[0].start()
    for k in range(PARTS):
        for copy in had[k]:
            copy.start()
    for k in range(PARTS):
        take[k].start()
    row = iota((8, BY), 0)
    lane = iota((8, BY), 1)
    first = [jnp.zeros((8, BY), F32) for t in range(8)]
    last = [jnp.zeros((8, BY), F32) for t in range(8)]
    east = [jnp.zeros((8, BY), F32) for t in range(8)]
    for g in range(NG):
        x = off[0, g] - r * BX
        y = off[1, g] - c * BY
        across = (lane >= y) & (lane < y + PC)
        edge = lane == y + PC - 1
        for t in range(8):
            first[t] = jnp.where((row + 8 * t == x) & across, 1.0, first[t])
            last[t] = jnp.where((row + 8 * t == x + PC - 1) & across, 1.0, last[t])
            east[t] = jnp.where((row + 8 * t >= x) & (row + 8 * t < x + PC) & edge, 1.0, east[t])
    norm[...] = nv[0:1, 0:1]
    flat = ri.reshape(128 * PITCH, 128)
    got[0].wait()
    for k in range(PARTS):
        for copy in had[k]:
            copy.wait()
        for l in range(levels * k, levels * k + levels):
            ends = []
            turn = []
            for side in range(2):
                at = (2 * l + side) * 8 * PITCH + 16
                ends.append(flat[pl.ds(at, 8, stride=PITCH), :])
                row17 = flat[pl.ds(at + 1, 8, stride=PITCH), :]
                turn.append([pltpu.roll(row17, lax.rem(256 - 8 * r - 64 * w, 128), 1) for w in range(2)])
            for t in range(8):
                tile = slice(8 * t, 8 * t + 8)
                top = first[t] * ends[0]
                bottom = last[t] * ends[1]
                e1 = [
                    jnp.where(lane < 64, *[jnp.broadcast_to(turn[side][w][:, t : t + 1], (8, 128)) for w in range(2)])
                    for side in range(2)
                ]
                e1 = jnp.where(east[t] > 0.5, e1[1], e1[0])
                for f in range(4):
                    p = 8 * f + l
                    new = flat[pl.ds((p // 2) * 8 * PITCH + (p % 2) * 8 + t, 8, stride=PITCH), :]
                    edge = bottom * d0[1, p : p + 1, :] - top * d0[0, p : p + 1, :] + e1 * d1[p, tile, :]
                    tend[p, tile, :] = tend[p, tile, :] + new + (0.15 / 9) * edge
        for copy in give[k]:
            copy.start()
        take[k].wait()
        put[k].start()
    for k in range(PARTS):
        for copy in give[k]:
            copy.wait()
        put[k].wait()


def merge(off, tend, d0, d1, ri, fout, nv):
    hbm = pl.BlockSpec(memory_space=pl.ANY)
    return pl.pallas_call(
        merge_kernel,
        out_shape=(shape(32, BX, BY), shape(32, FR, 1, FC), shape(1, 1)),
        in_specs=[sspec(), hbm, vspec()] + [hbm] * 3 + [vspec()],
        out_specs=(hbm, hbm, vspec()),
        scratch_shapes=[
            VM((32, BX, BY), F32),
            VM((32, BX, BY), F32),
            VM((NG * NM, PITCH, 128), F32),
            VM((32, FR, FC), F32),
            pltpu.SemaphoreType.DMA((1 + 4 * PARTS,)),
        ],
    )(off, tend, d0, d1, ri.reshape(NG * NM, PITCH, 128), fout, nv)


def local(base_state, base_old, fine_state, fine_old, coupling, patch_offsets, patch_group):
    base = base_state.reshape(32, BX, BY)
    old = base_old.reshape(32, BX, BY)
    fine = fine_state.reshape(32, FR, 1, FC)
    fold = fine_old.reshape(32, FR, 1, FC)
    off = patch_offsets.T
    tend, d0, d1, fout, nv, r2 = main(off, patch_group, coupling, base, old, fine, fold)
    bout, fres, norm = merge(off, tend, d0, d1, r2, fout, nv)
    return (
        bout.reshape(4, 8, BX, BY),
        fres.reshape(4, 8, 1, FR, FC),
        norm.reshape(()),
    )


def solution(mesh):
    placed = (
        P(None, None, "gx", "gy"),
        P(None, None, "gx", "gy"),
        P(None, None, "gx", "gy", None),
        P(None, None, "gx", "gy", None),
        P(),
        P(),
        P(),
    )
    return jax.shard_map(
        local,
        mesh=mesh,
        in_specs=placed,
        out_specs=(P(None, None, "gx", "gy"), P(None, None, "gx", "gy", None), P()),
        check_vma=False,
    )
```
